8 devices in a mesh: dp: 2 (over z, y), tp: 4 (over x, core).
Axes of the slice: x: 2, y: 2, z: 1, core: 2. Of those that a mesh axis runs over, the one named last changes fastest.
Arguments:
- x: bfloat16 [448, 5120], P('dp'), parts along dimension 0
- lengths: int32 [194], P('dp'), parts along dimension 0
- attn_gain: bfloat16 [2, 5120], replicated
- w_q: bfloat16 [2, 5120, 4096], P(None, None, 'tp')
- w_k: bfloat16 [2, 5120, 1024], P(None, None, 'tp')
- w_v: bfloat16 [2, 5120, 1024], P(None, None, 'tp')
- w_o: bfloat16 [2, 4096, 5120], P(None, 'tp')
- mlp_gain: bfloat16 [2, 5120], replicated
- w_gate: bfloat16 [2, 5120, 14336], P(None, None, 'tp')
- w_up: bfloat16 [2, 5120, 14336], P(None, None, 'tp')
- w_down: bfloat16 [2, 14336, 5120], P(None, 'tp')
- k_cache: bfloat16 [2, 194, 8, 256, 128], P(None, 'dp', 'tp'), parts along dimension 1
- v_cache: bfloat16 [2, 194, 8, 256, 128], P(None, 'dp', 'tp'), parts along dimension 1
Outputs:
- output: bfloat16 [448, 5120], P('dp'), parts along dimension 0
There are 2 independent parts. The reference program is written for one: setup_inputs(seed, part) draws one part's arguments, and reference() takes and returns one part's arrays. A program takes and returns all parts, laid end to end along the dimension named above; an argument that names none is the same for every part.
All inputs are finite; a program needn't handle non-finite values.
Results may differ from the reference program's by a relative error of at most 0.0199313.
Values are sent between devices in bfloat16 or wider.
A program may use at most 1.25 GiB of HBM per device.

```python
import jax
import jax.numpy as jnp
from jax import lax

D = 5120
HEADS = 32
KV_HEADS = 8
HEAD = 128
FF = 14336
BATCH = 96
CHUNK = 128
SEQ = 256
LAYERS = 2

GROUP = HEADS // KV_HEADS
TOKENS = BATCH + CHUNK
ATTN_SCALE = HEAD ** -0.5
ROPE_BASE = 500000.0
EPSILON = 1e-5


def setup_inputs(seed: int = 0, part: int = 0) -> dict:
    root_key = jax.random.key(seed)
    shared_keys = jax.random.split(root_key, 9)
    part_keys = jax.random.split(jax.random.fold_in(root_key, part), 8)

    def gaussian(sub_key, arr_shape, factor):
        return jax.random.normal(sub_key, arr_shape, jnp.float32) * factor

    lengths = jax.random.randint(part_keys[1], (BATCH + 1,), 1, SEQ)
    longest = jax.random.randint(part_keys[2], (), 0, BATCH + 1)
    lengths = jnp.where(jnp.arange(BATCH + 1) == longest, SEQ - 1, lengths).astype(jnp.int32)
    pos_ramp = (jnp.arange(SEQ, dtype=jnp.float32) * (2.0 / SEQ) - 1.0)[:, None]
    cache_shape = (LAYERS, BATCH + 1, KV_HEADS, SEQ, HEAD)
    row_shape = (LAYERS, BATCH + 1, KV_HEADS, 1, HEAD)
    k_cache = gaussian(part_keys[3], cache_shape, 1.0) + pos_ramp * gaussian(part_keys[4], row_shape, 1.0)
    v_cache = gaussian(part_keys[5], row_shape, 1.0) + pos_ramp * gaussian(part_keys[6], row_shape, 1.0) + gaussian(part_keys[7], cache_shape, 0.5)
    return {
        'x': gaussian(part_keys[0], (TOKENS, D), 1.0).astype(jnp.bfloat16),
        'lengths': lengths,
        'attn_gain': jax.random.uniform(shared_keys[0], (LAYERS, D), jnp.float32, 0.5, 1.5).astype(jnp.bfloat16),
        'w_q': gaussian(shared_keys[1], (LAYERS, D, HEADS * HEAD), D ** -0.5).astype(jnp.bfloat16),
        'w_k': gaussian(shared_keys[2], (LAYERS, D, KV_HEADS * HEAD), D ** -0.5).astype(jnp.bfloat16),
        'w_v': gaussian(shared_keys[3], (LAYERS, D, KV_HEADS * HEAD), D ** -0.5).astype(jnp.bfloat16),
        'w_o': gaussian(shared_keys[4], (LAYERS, HEADS * HEAD, D), (HEADS * HEAD) ** -0.5).astype(jnp.bfloat16),
        'mlp_gain': jax.random.uniform(shared_keys[5], (LAYERS, D), jnp.float32, 0.5, 1.5).astype(jnp.bfloat16),
        'w_gate': gaussian(shared_keys[6], (LAYERS, D, FF), D ** -0.5).astype(jnp.bfloat16),
        'w_up': gaussian(shared_keys[7], (LAYERS, D, FF), D ** -0.5).astype(jnp.bfloat16),
        'w_down': gaussian(shared_keys[8], (LAYERS, FF, D), 1.5 * FF ** -0.5).astype(jnp.bfloat16),
        'k_cache': k_cache.astype(jnp.bfloat16),
        'v_cache': v_cache.astype(jnp.bfloat16),
    }


def rms_norm(x, norm_gain):
    x_f32 = x.astype(jnp.float32)
    inv_rms = lax.rsqrt(jnp.mean(x_f32 * x_f32, axis=-1, keepdims=True) + EPSILON)
    return (x_f32 * inv_rms * norm_gain.astype(jnp.float32)).astype(jnp.bfloat16)


def rope_tables(positions):
    freq_exps = jnp.arange(0, HEAD, 2, dtype=jnp.float32) / HEAD
    angles = positions.astype(jnp.float32)[:, None] * jnp.power(ROPE_BASE, -freq_exps)[None, :]
    return jnp.cos(angles)[:, None, :], jnp.sin(angles)[:, None, :]


def apply_rope(vectors, cos_tab, sin_tab):
    half_dim = HEAD // 2
    vec_f32 = vectors.astype(jnp.float32)
    first = vec_f32[..., :half_dim]
    second = vec_f32[..., half_dim:]
    return jnp.concatenate([first * cos_tab - second * sin_tab, second * cos_tab + first * sin_tab], axis=-1).astype(jnp.bfloat16)


def decode_row(row_args):
    q_row, k_row, v_row, kc_row, vc_row, length = row_args
    q_f32 = q_row.reshape(KV_HEADS, GROUP, HEAD).astype(jnp.float32)
    logits_cache = jnp.einsum('grd,gsd->grs', q_f32, kc_row.astype(jnp.float32)) * ATTN_SCALE
    logits_cache = jnp.where(jnp.arange(SEQ)[None, None, :] < length, logits_cache, -jnp.inf)
    logits_self = jnp.einsum('grd,gd->gr', q_f32, k_row.astype(jnp.float32))[:, :, None] * ATTN_SCALE
    prob_all = jax.nn.softmax(jnp.concatenate([logits_cache, logits_self], axis=-1), axis=-1)
    prob_all = prob_all.astype(jnp.bfloat16).astype(jnp.float32)
    result = jnp.einsum('grs,gsd->grd', prob_all[..., :SEQ], vc_row.astype(jnp.float32)) + prob_all[..., SEQ:] * v_row.astype(jnp.float32)[:, None, :]
    return result.astype(jnp.bfloat16).reshape(HEADS * HEAD)


def chunk_attention(q_chk, k_chk, v_chk, kc_row, vc_row, prefix_len):
    q_heads = q_chk.reshape(CHUNK, KV_HEADS, GROUP, HEAD).transpose(1, 0, 2, 3)
    k_heads = k_chk.transpose(1, 0, 2)
    v_heads = v_chk.transpose(1, 0, 2)
    cache_mask = jnp.arange(SEQ)[None, None, :] < prefix_len
    tok_ids = jnp.arange(CHUNK)
    causal_mask = (tok_ids[None, :] <= tok_ids[:, None])[:, None, :]

    def one_head(head_args):
        q_head, k_head, v_head, kc_head, vc_head = head_args
        q_f32 = q_head.astype(jnp.float32)
        logits_cache = jnp.einsum('crd,sd->crs', q_f32, kc_head.astype(jnp.float32)) * ATTN_SCALE
        logits_cache = jnp.where(cache_mask, logits_cache, -jnp.inf)
        logits_new = jnp.einsum('crd,jd->crj', q_f32, k_head.astype(jnp.float32)) * ATTN_SCALE
        logits_new = jnp.where(causal_mask, logits_new, -jnp.inf)
        prob_all = jax.nn.softmax(jnp.concatenate([logits_cache, logits_new], axis=-1), axis=-1)
        prob_all = prob_all.astype(jnp.bfloat16).astype(jnp.float32)
        result = jnp.einsum('crs,sd->crd', prob_all[..., :SEQ], vc_head.astype(jnp.float32)) + jnp.einsum('crj,jd->crd', prob_all[..., SEQ:], v_head.astype(jnp.float32))
        return result.astype(jnp.bfloat16)

    heads_out = lax.map(one_head, (q_heads, k_heads, v_heads, kc_row, vc_row))
    return heads_out.transpose(1, 0, 2, 3).reshape(CHUNK, HEADS * HEAD)


def decoder_layer(x, lengths, cos_tab, sin_tab, params):
    attn_gain, w_q, w_k, w_v, w_o, mlp_gain, w_gate, w_up, w_down, k_cache, v_cache = params
    normed = rms_norm(x, attn_gain)
    q_all = apply_rope(jnp.dot(normed, w_q, preferred_element_type=jnp.float32).astype(jnp.bfloat16).reshape(TOKENS, HEADS, HEAD), cos_tab, sin_tab)
    k_all = apply_rope(jnp.dot(normed, w_k, preferred_element_type=jnp.float32).astype(jnp.bfloat16).reshape(TOKENS, KV_HEADS, HEAD), cos_tab, sin_tab)
    v_all = jnp.dot(normed, w_v, preferred_element_type=jnp.float32).astype(jnp.bfloat16).reshape(TOKENS, KV_HEADS, HEAD)
    dec_out = lax.map(decode_row, (q_all[:BATCH], k_all[:BATCH], v_all[:BATCH], k_cache[:BATCH], v_cache[:BATCH], lengths[:BATCH]))
    chk_out = chunk_attention(q_all[BATCH:], k_all[BATCH:], v_all[BATCH:], k_cache[BATCH], v_cache[BATCH], lengths[BATCH])
    attended = jnp.concatenate([dec_out, chk_out], axis=0)
    hidden = (x.astype(jnp.float32) + jnp.dot(attended, w_o, preferred_element_type=jnp.float32)).astype(jnp.bfloat16)
    mlp_in = rms_norm(hidden, mlp_gain)
    gate_proj = jnp.dot(mlp_in, w_gate, preferred_element_type=jnp.float32)
    up_proj = jnp.dot(mlp_in, w_up, preferred_element_type=jnp.float32)
    activated = (jax.nn.silu(gate_proj) * up_proj).astype(jnp.bfloat16)
    down_proj = jnp.dot(activated, w_down, preferred_element_type=jnp.float32)
    return (hidden.astype(jnp.float32) + down_proj).astype(jnp.bfloat16)


def reference(x, lengths, attn_gain, w_q, w_k, w_v, w_o, mlp_gain, w_gate, w_up, w_down, k_cache, v_cache):
    positions = jnp.concatenate([lengths[:BATCH], lengths[BATCH] + jnp.arange(CHUNK, dtype=jnp.int32)])
    cos_tab, sin_tab = rope_tables(positions)

    def layer_step(hidden, params):
        return decoder_layer(hidden, lengths, cos_tab, sin_tab, params), None

    result, unused = lax.scan(layer_step, x, (attn_gain, w_q, w_k, w_v, w_o, mlp_gain, w_gate, w_up, w_down, k_cache, v_cache))
    return result
```

```python
import functools

import jax
import jax.numpy as jnp
from jax import lax
from jax.experimental import pallas as pl
from jax.experimental.pallas import tpu as pltpu
from jax.sharding import PartitionSpec as P

ROPE_BASE = 500000.0
EPSILON = 1e-5
MESH = pl.DeviceIdType.MESH
F32 = jnp.float32
BF16 = jnp.bfloat16
CW = 512
G_SLOTS = 3
D_SLOTS = 4


def rms_norm(x, norm_gain):
    x_f32 = x.astype(jnp.float32)
    inv_rms = lax.rsqrt(jnp.mean(x_f32 * x_f32, axis=-1, keepdims=True) + EPSILON)
    return (x_f32 * inv_rms * norm_gain.astype(jnp.float32)).astype(jnp.bfloat16)


def rope_tables(positions, head_dim):
    freq_exps = jnp.arange(0, head_dim, 2, dtype=jnp.float32) / head_dim
    angles = positions.astype(jnp.float32)[:, None] * jnp.power(ROPE_BASE, -freq_exps)[None, :]
    return jnp.cos(angles)[:, None, :], jnp.sin(angles)[:, None, :]


def apply_rope(vectors, cos_tab, sin_tab):
    half_dim = vectors.shape[-1] // 2
    vec_f32 = vectors.astype(jnp.float32)
    first = vec_f32[..., :half_dim]
    second = vec_f32[..., half_dim:]
    return jnp.concatenate([first * cos_tab - second * sin_tab, second * cos_tab + first * sin_tab], axis=-1).astype(jnp.bfloat16)


def attention(q_rot, k_rot, v_new, k_cache, v_cache, lengths):
    dec_rows = lengths.shape[0] - 1
    kv_local = k_cache.shape[1]
    seq_len = k_cache.shape[2]
    head_dim = k_cache.shape[3]
    tok_count = q_rot.shape[0]
    chunk_len = tok_count - dec_rows
    attn_scale = head_dim ** -0.5
    q_grouped = q_rot.reshape(tok_count, kv_local, -1, head_dim)
    q_dec = q_grouped[:dec_rows]
    q_chk = q_grouped[dec_rows:]
    seq_ids = jnp.arange(seq_len)
    dec_cache = jnp.einsum('bgrd,bgsd->bgrs', q_dec, k_cache[:dec_rows], preferred_element_type=jnp.float32) * attn_scale
    dec_cache = jnp.where(seq_ids[None, None, None, :] < lengths[:dec_rows, None, None, None], dec_cache, -jnp.inf)
    dec_self = jnp.einsum('bgrd,bgd->bgr', q_dec, k_rot[:dec_rows], preferred_element_type=jnp.float32)[..., None] * attn_scale
    dec_prob = jax.nn.softmax(jnp.concatenate([dec_cache, dec_self], axis=-1), axis=-1).astype(jnp.bfloat16)
    dec_out = jnp.einsum('bgrs,bgsd->bgrd', dec_prob[..., :seq_len], v_cache[:dec_rows], preferred_element_type=jnp.float32) + dec_prob[..., seq_len:].astype(jnp.float32) * v_new[:dec_rows, :, None, :].astype(jnp.float32)
    chk_cache = jnp.einsum('cgrd,gsd->cgrs', q_chk, k_cache[dec_rows], preferred_element_type=jnp.float32) * attn_scale
    chk_cache = jnp.where(seq_ids[None, None, None, :] < lengths[dec_rows], chk_cache, -jnp.inf)
    chk_self = jnp.einsum('cgrd,jgd->cgrj', q_chk, k_rot[dec_rows:], preferred_element_type=jnp.float32) * attn_scale
    tok_ids = jnp.arange(chunk_len)
    causal_mask = tok_ids[None, :] <= tok_ids[:, None]
    chk_self = jnp.where(causal_mask[:, None, None, :], chk_self, -jnp.inf)
    chk_prob = jax.nn.softmax(jnp.concatenate([chk_cache, chk_self], axis=-1), axis=-1).astype(jnp.bfloat16)
    chk_out = jnp.einsum('cgrs,gsd->cgrd', chk_prob[..., :seq_len], v_cache[dec_rows], preferred_element_type=jnp.float32) + jnp.einsum('cgrj,jgd->cgrd', chk_prob[..., seq_len:], v_new[dec_rows:], preferred_element_type=jnp.float32)
    return jnp.concatenate([dec_out.reshape(dec_rows, -1), chk_out.reshape(chunk_len, -1)], axis=0).astype(jnp.bfloat16)


def layer_kernel(layer, fuse_next, att, x, gain_mlp, gain_next, wo, wg, wu, wd, wq, wk, wv, *rest):
    if fuse_next:
        y, qkv = rest[:2]
        rest = rest[2:]
    else:
        y = rest[0]
        rest = rest[1:]
    gbuf, dbuf, acc, act, pbuf, rbuf, sbuf, xb1, xb2, h1, h2, ssq, pre, wo_sem, g_sem, d_sem, y_sem, p_ss, p_rs, x_ss, x_rs, h_ss, h_rs = rest
    rows, width = x.shape
    half = rows // 2
    ff = wg.shape[2]
    n_chunks = width // CW
    o_depth = wo.shape[1]
    o_per_slot = ff // o_depth
    dp_me = lax.axis_index('dp')
    me = lax.axis_index('tp')
    core = lax.rem(me, 2)
    core_peer = (dp_me, me + 1 - 2 * core)
    x_peer = (dp_me, lax.rem(me + 2, 4))
    own = pl.ds(pl.multiple_of(core * half, 16), half)
    oth = pl.ds(pl.multiple_of((1 - core) * half, 16), half)
    xbs = (xb1, xb2)
    hs = (h1, h2)

    def cols(j):
        return pl.ds(pl.multiple_of(j * CW, CW), CW)

    def wo_copy(j):
        return pltpu.make_async_copy(wo.at[layer, :, cols(j)], dbuf.at[j // o_per_slot, pl.ds(pl.multiple_of(lax.rem(j, o_per_slot) * o_depth, 16), o_depth), :], wo_sem.at[j])

    def g_copies(j):
        slot = lax.rem(j, G_SLOTS)
        return (pltpu.make_async_copy(wg.at[layer, cols(j), :], gbuf.at[slot, 0], g_sem.at[slot, 0]),
                pltpu.make_async_copy(wu.at[layer, cols(j), :], gbuf.at[slot, 1], g_sem.at[slot, 1]))

    def d_copy(j):
        slot = lax.rem(j, D_SLOTS)
        return pltpu.make_async_copy(wd.at[layer, :, cols(j)], dbuf.at[slot], d_sem.at[slot])

    def p_copy(ar, j):
        return pltpu.make_async_remote_copy(pbuf.at[j, oth, :], rbuf.at[j], p_ss.at[ar, j], p_rs.at[ar, j], device_id=core_peer, device_id_type=MESH)

    def x_copy(ar, j):
        return pltpu.make_async_remote_copy(sbuf.at[j], xbs[ar].at[j], x_ss.at[ar, j], x_rs.at[ar, j], device_id=x_peer, device_id_type=MESH)

    def h_copy(ar, j):
        return pltpu.make_async_remote_copy(hs[ar].at[j, own, :], hs[ar].at[j, own, :], h_ss.at[ar, j], h_rs.at[ar, j], device_id=core_peer, device_id_type=MESH)

    def h_wait(ar, j):
        pltpu.make_async_remote_copy(hs[ar].at[j, oth, :], hs[ar].at[j, oth, :], h_ss.at[ar, j], h_rs.at[ar, j], device_id=core_peer, device_id_type=MESH).wait_recv()

    def send_part(ar, j, part):
        pbuf[j] = part.astype(BF16)
        p_copy(ar, j).start()

    def pair_sum(ar, j):
        p_copy(ar, j).wait_recv()
        sbuf[j] = (pbuf[j, own, :].astype(F32) + rbuf[j].astype(F32)).astype(BF16)
        x_copy(ar, j).start()

    def finish(ar, j):
        x_copy(ar, j).wait_recv()
        total = sbuf[j].astype(F32) + xbs[ar][j].astype(F32)
        resid = x[own, cols(j)] if ar == 0 else h1[j, own, :]
        hs[ar][j, own, :] = (resid.astype(F32) + total).astype(BF16)
        h_copy(ar, j).start()

    def add_squares(vals):
        sq = vals * vals
        ssq[...] += sq[:, :128] + sq[:, 128:256] + sq[:, 256:384] + sq[:, 384:]

    def inv_rms():
        return lax.rsqrt(jnp.sum(ssq[...], axis=-1, keepdims=True) * (1.0 / width) + EPSILON)

    for j in range(n_chunks):
        wo_copy(j).start()
    for j in range(G_SLOTS):
        for c in g_copies(j):
            c.start()
    barrier = pltpu.get_barrier_semaphore()
    for peer in (core_peer, x_peer):
        pl.semaphore_signal(barrier, inc=1, device_id=peer, device_id_type=MESH)

    ssq[...] = jnp.zeros_like(ssq)

    def sq_step(j, c):
        add_squares(x[:, cols(j)].astype(F32))
        return c

    lax.fori_loop(0, n_chunks, sq_step, 0)
    pre[...] = jnp.broadcast_to(jnp.maximum(inv_rms(), 1e-30), pre.shape)
    ssq[...] = jnp.zeros_like(ssq)
    acc[...] = jnp.zeros_like(acc)
    pl.semaphore_wait(barrier, 2)

    def o_step(j, c):
        wo_copy(j).wait()
        w = dbuf[j // o_per_slot, pl.ds(pl.multiple_of(lax.rem(j, o_per_slot) * o_depth, 16), o_depth), :]
        send_part(0, j, jnp.dot(att[...], w, preferred_element_type=F32))

        @pl.when(j >= 1)
        def _():
            pair_sum(0, j - 1)
        return c

    lax.fori_loop(0, n_chunks, o_step, 0)
    pair_sum(0, n_chunks - 1)

    def gu_block(j):
        h_wait(0, j)
        vals = h1[j].astype(F32)
        add_squares(vals)
        a = (vals * pre[:, :1] * gain_mlp[:, cols(j)]).astype(BF16)
        slot = lax.rem(j, G_SLOTS)
        for c in g_copies(j):
            c.wait()

        def mat(m, c):
            for n in range(ff // CW):
                col = pl.ds(pl.multiple_of(m * ff + n * CW, CW), CW)
                acc[:, col] += jnp.dot(a, gbuf[slot, m, :, n * CW:(n + 1) * CW], preferred_element_type=F32)
            return c

        lax.fori_loop(0, 2, mat, 0)

        @pl.when(j + G_SLOTS < n_chunks)
        def _():
            for c in g_copies(j + G_SLOTS):
                c.start()

        @pl.when(j >= n_chunks - D_SLOTS)
        def _():
            d_copy(j - (n_chunks - D_SLOTS)).start()

    def gu_step(j, c):
        finish(0, j)

        @pl.when(j >= 1)
        def _():
            gu_block(j - 1)
        return c

    lax.fori_loop(0, n_chunks, gu_step, 0)
    gu_block(n_chunks - 1)

    q_cols, k_cols = wq.shape[2], wk.shape[2]
    n_qkv = q_cols + 2 * k_cols

    def qkv_copies(j):
        slot, which, side = j // 4, lax.rem(j // 2, 2), lax.rem(j, 2)
        base = side * (ff // 2)
        dst = gbuf.at[slot, which]
        sem = wo_sem.at[j]
        return (pltpu.make_async_copy(wq.at[layer + 1, cols(j), :], dst.at[:, pl.ds(pl.multiple_of(base, 128), q_cols)], sem),
                pltpu.make_async_copy(wk.at[layer + 1, cols(j), :], dst.at[:, pl.ds(pl.multiple_of(base + q_cols, 128), k_cols)], qk_sem.at[0, j]),
                pltpu.make_async_copy(wv.at[layer + 1, cols(j), :], dst.at[:, pl.ds(pl.multiple_of(base + q_cols + k_cols, 128), k_cols)], qk_sem.at[1, j]))

    qk_sem = y_sem

    scale = inv_rms() / pre[:, :1]
    pre[...] = jnp.broadcast_to(jnp.maximum(inv_rms(), 1e-30), pre.shape)

    def act_step(n, c):
        gate = acc[:, cols(n)] * scale
        up = acc[:, pl.ds(pl.multiple_of(ff + n * CW, CW), CW)] * scale
        act[:, cols(n)] = (gate * jax.nn.sigmoid(gate) * up).astype(BF16)
        return c

    lax.fori_loop(0, ff // CW, act_step, 0)

    for j in range(n_chunks):
        p_copy(0, j).wait_send()
        x_copy(0, j).wait_send()

    def d_step(j, c):
        d_copy(j).wait()
        send_part(1, j, jnp.dot(act[...], dbuf[lax.rem(j, D_SLOTS)], preferred_element_type=F32))

        @pl.when(j + D_SLOTS < n_chunks)
        def _():
            d_copy(j + D_SLOTS).start()

        if fuse_next:
            for c2 in qkv_copies(j):
                c2.start()

        @pl.when(j >= 1)
        def _():
            pair_sum(1, j - 1)
        return c

    lax.fori_loop(0, n_chunks, d_step, 0)
    pair_sum(1, n_chunks - 1)

    def out_copy(j):
        return pltpu.make_async_copy(h2.at[j], y.at[:, cols(j)], h_ss.at[2, j])

    if fuse_next:
        ssq[...] = jnp.zeros_like(ssq)
        acc[:, :n_qkv] = jnp.zeros((rows, n_qkv), F32)

    def last_block(j):
        h_wait(1, j)
        out_copy(j).start()
        if fuse_next:
            vals = h2[j].astype(F32)
            add_squares(vals)
            a = (vals * pre[:, :1] * gain_next[:, cols(j)]).astype(BF16)
            for c in qkv_copies(j):
                c.wait()
            slot, which, side = j // 4, lax.rem(j // 2, 2), lax.rem(j, 2)
            base = side * (ff // 2)
            for n in range(n_qkv // CW):
                col = pl.ds(pl.multiple_of(base + n * CW, 128), CW)
                acc[:, n * CW:(n + 1) * CW] += jnp.dot(a, gbuf[slot, which, :, col], preferred_element_type=F32)

    def last_step(j, c):
        finish(1, j)

        @pl.when(j >= 1)
        def _():
            last_block(j - 1)
        return c

    lax.fori_loop(0, n_chunks, last_step, 0)
    last_block(n_chunks - 1)
    if fuse_next:
        scale2 = inv_rms() / pre[:, :1]
        qkv[...] = (acc[:, :n_qkv] * scale2).astype(BF16)
    for j in range(n_chunks):
        out_copy(j).wait()
        h_copy(0, j).wait_send()
        h_copy(1, j).wait_send()
        p_copy(1, j).wait_send()
        x_copy(1, j).wait_send()


def layer_call(layer, fuse_next, att, x, gain_mlp, gain_next, wo, wg, wu, wd, wq, wk, wv):
    rows, width = x.shape
    ff = wg.shape[2]
    n_chunks = width // CW
    half = rows // 2
    n_qkv = wq.shape[2] + 2 * wk.shape[2]
    vmem = pl.BlockSpec(memory_space=pltpu.VMEM)
    hbm = pl.BlockSpec(memory_space=pl.ANY)
    out_shape = [jax.ShapeDtypeStruct((rows, width), BF16)]
    out_specs = [hbm]
    if fuse_next:
        out_shape.append(jax.ShapeDtypeStruct((rows, n_qkv), BF16))
        out_specs.append(vmem)
    sem = pltpu.SemaphoreType.DMA
    return pl.pallas_call(
        functools.partial(layer_kernel, layer, fuse_next),
        out_shape=out_shape,
        in_specs=[vmem] * 4 + [hbm] * 7,
        out_specs=out_specs,
        scratch_shapes=[
            pltpu.VMEM((G_SLOTS, 2, CW, ff), BF16),
            pltpu.VMEM((D_SLOTS, ff, CW), BF16),
            pltpu.VMEM((rows, 2 * ff), F32),
            pltpu.VMEM((rows, ff), BF16),
            pltpu.VMEM((n_chunks, rows, CW), BF16),
            pltpu.VMEM((n_chunks, half, CW), BF16),
            pltpu.VMEM((n_chunks, half, CW), BF16),
            pltpu.VMEM((n_chunks, half, CW), BF16),
            pltpu.VMEM((n_chunks, half, CW), BF16),
            pltpu.VMEM((n_chunks, rows, CW), BF16),
            pltpu.VMEM((n_chunks, rows, CW), BF16),
            pltpu.VMEM((rows, 128), F32),
            pltpu.VMEM((rows, 128), F32),
            sem((n_chunks,)),
            sem((G_SLOTS, 2)),
            sem((D_SLOTS,)),
            sem((2, n_chunks)),
            sem((2, n_chunks)),
            sem((2, n_chunks)),
            sem((2, n_chunks)),
            sem((2, n_chunks)),
            sem((3, n_chunks)),
            sem((2, n_chunks)),
        ],
        compiler_params=pltpu.CompilerParams(collective_id=layer, has_side_effects=True, vmem_limit_bytes=67043328),
        name='layer' + str(layer),
    )(att, x, gain_mlp, gain_next, wo, wg, wu, wd, wq, wk, wv)


def solution(mesh):
    col_spec = P(None, None, 'tp')
    row_spec = P(None, 'tp', None)
    cache_spec = P(None, 'dp', 'tp', None, None)
    in_specs = (P('dp', None), P('dp'), P(), col_spec, col_spec, col_spec, row_spec, P(), col_spec, col_spec, row_spec, cache_spec, cache_spec)

    def body(x, lengths, attn_gain, w_q, w_k, w_v, w_o, mlp_gain, w_gate, w_up, w_down, k_cache, v_cache):
        dec_rows = lengths.shape[0] - 1
        rows = x.shape[0]
        chunk_len = rows - dec_rows
        head_dim = k_cache.shape[-1]
        positions = jnp.concatenate([lengths[:dec_rows], lengths[dec_rows] + jnp.arange(chunk_len, dtype=jnp.int32)])
        cos_tab, sin_tab = rope_tables(positions, head_dim)
        n_layers = w_q.shape[0]
        hidden = x
        normed = rms_norm(x, attn_gain[0])
        q, k, v = (jnp.dot(normed, w[0], preferred_element_type=F32).astype(BF16) for w in (w_q, w_k, w_v))
        for layer in range(n_layers):
            q_rot = apply_rope(q.reshape(rows, -1, head_dim), cos_tab, sin_tab)
            k_rot = apply_rope(k.reshape(rows, -1, head_dim), cos_tab, sin_tab)
            att = attention(q_rot, k_rot, v.reshape(rows, -1, head_dim), k_cache[layer], v_cache[layer], lengths)
            fuse_next = layer + 1 < n_layers
            gain_next = attn_gain[min(layer + 1, n_layers - 1)][None].astype(F32)
            outs = layer_call(layer, fuse_next, att, hidden, mlp_gain[layer][None].astype(F32), gain_next, w_o, w_gate, w_up, w_down, w_q, w_k, w_v)
            hidden = outs[0]
            if fuse_next:
                nq, nk = w_q.shape[2], w_k.shape[2]
                q, k, v = outs[1][:, :nq], outs[1][:, nq:nq + nk], outs[1][:, nq + nk:]
        return hidden

    return jax.shard_map(body, mesh=mesh, in_specs=in_specs, out_specs=P('dp', None), check_vma=False)
```

```python
import functools

import jax
import jax.numpy as jnp
from jax import lax
from jax.experimental import pallas as pl
from jax.experimental.pallas import tpu as pltpu
from jax.sharding import PartitionSpec as P

ROPE_BASE = 500000.0
EPSILON = 1e-5
MESH = pl.DeviceIdType.MESH
F32 = jnp.float32
BF16 = jnp.bfloat16
CW = 512
G_SLOTS = 3
D_SLOTS = 4
KV_SLOTS = 3
KV_ROWS = 8
O, M = 0, 1
DEC, PRE = 0, 1


def step_kernel(dims, lens, x_in, cos, sin, gain_a, gain_m, wq, wk, wv, wo, wg, wu, wd, kc, vc, y,
                gbuf, dbuf, acc, act, pbuf, rbuf, xb_o, xb_m, h_o, h_m, ssq, pre, kbuf, vbuf, kpre, vpre,
                qs, kn, vn, qp, kp, vp, att,
                q_sem, w_sem, k_sem, v_sem, g_sem, d_sem, kv_sem, kvp_sem, y_sem, p_ss, p_rs, x_ss, x_rs, h_ss, h_rs):
    dec, chunk = dims
    rows = dec + chunk
    width = x_in.shape[1]
    layers, o_depth = wo.shape[0], wo.shape[1]
    ff = wg.shape[2]
    q_cols, k_cols = wq.shape[2], wk.shape[2]
    n_qkv = q_cols + 2 * k_cols
    seq, hd = kc.shape[3], kc.shape[4]
    heads, kv_heads = q_cols // hd, k_cols // hd
    group = heads // kv_heads
    n_chunks = width // CW
    o_per_slot = ff // o_depth
    scale_qk = hd ** -0.5
    base = (0, dec)
    size = (dec, chunk)
    half = (dec // 2, chunk // 2)
    rbase = (0, dec // 2)

    dp_me = lax.axis_index('dp')
    me = lax.axis_index('tp')
    core = lax.rem(me, 2)
    core_peer = (dp_me, me + 1 - 2 * core)
    x_peer = (dp_me, lax.rem(me + 2, 4))

    def own(part):
        return pl.ds(pl.multiple_of(base[part] + core * half[part], 16), half[part])

    def oth(part):
        return pl.ds(pl.multiple_of(base[part] + (1 - core) * half[part], 16), half[part])

    def whole(part):
        return pl.ds(base[part], size[part])

    def landed(part):
        return pl.ds(rbase[part], half[part])

    def cols(j):
        return pl.ds(pl.multiple_of(j * CW, CW), CW)

    xbs = (xb_o, xb_m)
    hs = (h_o, h_m)

    def x_load(j):
        return pltpu.make_async_copy(x_in.at[:, cols(j)], h_m.at[j], y_sem.at[0, j])

    def wo_copy(l, j):
        return pltpu.make_async_copy(wo.at[l, :, cols(j)], dbuf.at[j // o_per_slot, pl.ds(pl.multiple_of(lax.rem(j, o_per_slot) * o_depth, 16), o_depth), :], w_sem.at[j])

    def g_copies(l, j):
        slot = lax.rem(j, G_SLOTS)
        return (pltpu.make_async_copy(wg.at[l, cols(j), :], gbuf.at[slot, 0], g_sem.at[slot, 0]),
                pltpu.make_async_copy(wu.at[l, cols(j), :], gbuf.at[slot, 1], g_sem.at[slot, 1]))

    def d_copy(l, j):
        slot = lax.rem(j, D_SLOTS)
        return pltpu.make_async_copy(wd.at[l, :, cols(j)], dbuf.at[slot], d_sem.at[slot])

    def qkv_place(j):
        return j // 4, lax.rem(j // 2, 2), lax.rem(j, 2) * (ff // 2)

    def qkv_copies(l, j):
        slot, which, left = qkv_place(j)
        dst = gbuf.at[slot, which]

        def at(off, n):
            return dst.at[:, pl.ds(pl.multiple_of(left + off, 128), n)]

        return (pltpu.make_async_copy(wq.at[l, cols(j), :], at(0, q_cols), q_sem.at[j]),
                pltpu.make_async_copy(wk.at[l, cols(j), :], at(q_cols, k_cols), k_sem.at[j]),
                pltpu.make_async_copy(wv.at[l, cols(j), :], at(q_cols + k_cols, k_cols), v_sem.at[j]))

    def kv_copies(l, i):
        slot = lax.rem(i, KV_SLOTS)
        src = pl.ds(i * KV_ROWS, KV_ROWS)
        return (pltpu.make_async_copy(kc.at[l, src], kbuf.at[slot], kv_sem.at[slot, 0]),
                pltpu.make_async_copy(vc.at[l, src], vbuf.at[slot], kv_sem.at[slot, 1]))

    def kv_pre_copies(l):
        return (pltpu.make_async_copy(kc.at[l, dec], kpre, kvp_sem.at[0]),
                pltpu.make_async_copy(vc.at[l, dec], vpre, kvp_sem.at[1]))

    def start(copies):
        for c in copies:
            c.start()

    def wait(copies):
        for c in copies:
            c.wait()

    def p_copy(ar, part, j):
        return pltpu.make_async_remote_copy(pbuf.at[j, oth(part), :], rbuf.at[j, landed(part), :], p_ss.at[ar, part, j], p_rs.at[ar, part, j], device_id=core_peer, device_id_type=MESH)

    def x_copy(ar, part, j):
        return pltpu.make_async_remote_copy(pbuf.at[j, own(part), :], xbs[ar].at[j, landed(part), :], x_ss.at[ar, part, j], x_rs.at[ar, part, j], device_id=x_peer, device_id_type=MESH)

    def h_copy(ar, part, j):
        return pltpu.make_async_remote_copy(hs[ar].at[j, own(part), :], hs[ar].at[j, own(part), :], h_ss.at[ar, part, j], h_rs.at[ar, part, j], device_id=core_peer, device_id_type=MESH)

    def h_wait(ar, part, j):
        pltpu.make_async_remote_copy(hs[ar].at[j, oth(part), :], hs[ar].at[j, oth(part), :], h_ss.at[ar, part, j], h_rs.at[ar, part, j], device_id=core_peer, device_id_type=MESH).wait_recv()

    def sent(l, ar, part, j):
        if l > 0 or ar == M:
            p_copy(1 - ar, part, j).wait_send()
            x_copy(1 - ar, part, j).wait_send()

    def pair_sum(ar, part, j):
        p_copy(ar, part, j).wait_recv()
        pbuf[j, own(part), :] = (pbuf[j, own(part), :].astype(F32) + rbuf[j, landed(part), :].astype(F32)).astype(BF16)
        x_copy(ar, part, j).start()

    def finish(l, ar, part, j):
        x_copy(ar, part, j).wait_recv()
        total = pbuf[j, own(part), :].astype(F32) + xbs[ar][j, landed(part), :].astype(F32)
        resid = hs[1 - ar][j, own(part), :].astype(F32)
        if l > 0:
            h_copy(ar, part, j).wait_send()
        hs[ar][j, own(part), :] = (resid + total).astype(BF16)
        h_copy(ar, part, j).start()

    def add_squares(r, vals):
        sq = vals * vals
        ssq[r, :] += sq[:, :128] + sq[:, 128:256] + sq[:, 256:384] + sq[:, 384:]

    def inv_rms(r):
        return lax.rsqrt(jnp.sum(ssq[r, :], axis=-1, keepdims=True) * (1.0 / width) + EPSILON)

    def next_scale(r):
        inv = inv_rms(r)
        scale = inv / pre[r, :1]
        n = ssq[r, :].shape[0]
        pre[r, :] = jnp.broadcast_to(jnp.maximum(inv, 1e-30), (n, 128))
        ssq[r, :] = jnp.zeros((n, 128), F32)
        return scale

    def qkv_block(l, part, j):
        r = whole(part)
        if l > 0:
            h_wait(M, part, j)
        vals = h_m[j, r, :].astype(F32)
        add_squares(r, vals)
        a = (vals * pre[r, :1] * gain_a[l:l + 1, cols(j)]).astype(BF16)
        if part == DEC:
            wait(qkv_copies(l, j))
        slot, which, left = qkv_place(j)
        for n in range(n_qkv // CW):
            acc[r, n * CW:(n + 1) * CW] += jnp.dot(a, gbuf[slot, which, :, pl.ds(pl.multiple_of(left + n * CW, 128), CW)], preferred_element_type=F32)

    def qkv_part(l, part):
        r = whole(part)
        acc[r, :n_qkv] = jnp.zeros((size[part], n_qkv), F32)

        def step(j, c):
            if l > 0:
                finish(l - 1, M, part, j)

                @pl.when(j >= 1)
                def _():
                    qkv_block(l, part, j - 1)
            else:
                qkv_block(l, part, j)
            return c

        lax.fori_loop(0, n_chunks, step, 0)
        if l > 0:
            qkv_block(l, part, n_chunks - 1)
        scale = next_scale(r)
        c_tab, s_tab = cos[r, :], sin[r, :]

        def head(col):
            return (acc[r, col * hd:(col + 1) * hd] * scale).astype(BF16).astype(F32)

        def rope(t):
            return (t * c_tab + pltpu.roll(t, hd // 2, 1) * s_tab).astype(BF16)

        for h in range(heads):
            q = rope(head(h))
            if part == DEC:
                qs[pl.ds(h, dec, stride=heads), :] = q.astype(F32)
            else:
                qp[:, h * hd:(h + 1) * hd] = q
        for g in range(kv_heads):
            k = rope(head(heads + g))
            v = head(heads + kv_heads + g)
            if part == DEC:
                for h in range(g * group, (g + 1) * group):
                    kn[pl.ds(h, dec, stride=heads), :] = k.astype(F32)
                    vn[pl.ds(h, dec, stride=heads), :] = v
            else:
                kp[:, g * hd:(g + 1) * hd] = k
                vp[:, g * hd:(g + 1) * hd] = v.astype(BF16)

    def decode_attention(l):
        first_rows = lax.broadcasted_iota(jnp.int32, (heads, hd), 0) < group
        places = lax.broadcasted_iota(jnp.int32, (heads, seq), 1)
        n_blocks = dec // KV_ROWS

        def block(i, c):
            wait(kv_copies(l, i))
            slot = lax.rem(i, KV_SLOTS)
            for n in range(KV_ROWS):
                b = i * KV_ROWS + n
                r = pl.ds(pl.multiple_of(b * heads, heads), heads)
                q = qs[r, :]
                zero = jnp.zeros_like(q)
                q2 = jnp.concatenate([jnp.where(first_rows, q, zero), jnp.where(first_rows, zero, q)], axis=1).astype(BF16)
                k2 = jnp.concatenate([kbuf[slot, n, 0], kbuf[slot, n, 1]], axis=1)
                v2 = jnp.concatenate([vbuf[slot, n, 0], vbuf[slot, n, 1]], axis=1)
                s = lax.dot_general(q2, k2, (((1,), (1,)), ((), ())), preferred_element_type=F32) * scale_qk
                s = jnp.where(places < lens[b], s, -jnp.inf)
                s_new = jnp.sum(q * kn[r, :], axis=-1, keepdims=True) * scale_qk
                top = jnp.maximum(jnp.max(s, axis=-1, keepdims=True), s_new)
                e = jnp.exp(s - top)
                e_new = jnp.exp(s_new - top)
                inv = 1.0 / (jnp.sum(e, axis=-1, keepdims=True) + e_new)
                o = jnp.dot((e * inv).astype(BF16), v2, preferred_element_type=F32)
                qs[r, :] = jnp.where(first_rows, o[:, :hd], o[:, hd:]) + (e_new * inv).astype(BF16).astype(F32) * vn[r, :]

            @pl.when(i + KV_SLOTS < n_blocks)
            def _():
                start(kv_copies(l, i + KV_SLOTS))
            return c

        lax.fori_loop(0, n_blocks, block, 0)
        for h in range(heads):
            att[:dec, h * hd:(h + 1) * hd] = qs[pl.ds(h, dec, stride=heads), :].astype(BF16)

    def prefill_attention(l):
        wait(kv_pre_copies(l))
        n_old = lens[dec]
        old = lax.broadcasted_iota(jnp.int32, (chunk, seq), 1) < n_old
        causal = lax.broadcasted_iota(jnp.int32, (chunk, chunk), 1) <= lax.broadcasted_iota(jnp.int32, (chunk, chunk), 0)

        def heads_step(i, c):
            for g in range(kv_heads):
                col = pl.ds(pl.multiple_of((g * group + i) * hd, hd), hd)
                q = qp[:, col]
                kv_col = slice(g * hd, (g + 1) * hd)
                s = lax.dot_general(q, kpre[g], (((1,), (1,)), ((), ())), preferred_element_type=F32) * scale_qk
                s = jnp.where(old, s, -jnp.inf)
                t = lax.dot_general(q, kp[:, kv_col], (((1,), (1,)), ((), ())), preferred_element_type=F32) * scale_qk
                t = jnp.where(causal, t, -jnp.inf)
                top = jnp.maximum(jnp.max(s, axis=-1, keepdims=True), jnp.max(t, axis=-1, keepdims=True))
                es = jnp.exp(s - top)
                et = jnp.exp(t - top)
                inv = 1.0 / (jnp.sum(es, axis=-1, keepdims=True) + jnp.sum(et, axis=-1, keepdims=True))
                o = jnp.dot((es * inv).astype(BF16), vpre[g], preferred_element_type=F32)
                o += jnp.dot((et * inv).astype(BF16), vp[:, kv_col], preferred_element_type=F32)
                att[pl.ds(dec, chunk), col] = o.astype(BF16)
            return c

        lax.fori_loop(0, group, heads_step, 0)

    def o_part(l, part):
        r = whole(part)

        def step(j, c):
            if part == DEC:
                wo_copy(l, j).wait()
            w = dbuf[j // o_per_slot, pl.ds(pl.multiple_of(lax.rem(j, o_per_slot) * o_depth, 16), o_depth), :]
            sent(l, O, part, j)
            pbuf[j, r, :] = jnp.dot(att[r, :], w, preferred_element_type=F32).astype(BF16)
            p_copy(O, part, j).start()

            @pl.when(j >= 1)
            def _():
                pair_sum(O, part, j - 1)
            return c

        lax.fori_loop(0, n_chunks, step, 0)
        pair_sum(O, part, n_chunks - 1)

    def gate_up(l):
        def block(j):
            h_wait(O, DEC, j)
            h_wait(O, PRE, j)
            vals = h_o[j].astype(F32)
            add_squares(pl.ds(0, rows), vals)
            a = (vals * pre[:, :1] * gain_m[l:l + 1, cols(j)]).astype(BF16)
            slot = lax.rem(j, G_SLOTS)
            wait(g_copies(l, j))

            def mat(m, c):
                for n in range(ff // CW):
                    col = pl.ds(pl.multiple_of(m * ff + n * CW, CW), CW)
                    acc[:, col] += jnp.dot(a, gbuf[slot, m, :, n * CW:(n + 1) * CW], preferred_element_type=F32)
                return c

            lax.fori_loop(0, 2, mat, 0)

            @pl.when(j + G_SLOTS < n_chunks)
            def _():
                start(g_copies(l, j + G_SLOTS))

            @pl.when(j >= n_chunks - D_SLOTS)
            def _():
                d_copy(l, j - (n_chunks - D_SLOTS)).start()

        def step(j, c):
            finish(l, O, DEC, j)
            finish(l, O, PRE, j)

            @pl.when(j >= 1)
            def _():
                block(j - 1)
            return c

        lax.fori_loop(0, n_chunks, step, 0)
        block(n_chunks - 1)
        scale = next_scale(pl.ds(0, rows))

        def act_step(n, c):
            gate = acc[:, cols(n)] * scale
            up = acc[:, pl.ds(pl.multiple_of(ff + n * CW, CW), CW)] * scale
            act[:, cols(n)] = (gate * jax.nn.sigmoid(gate) * up).astype(BF16)
            return c

        lax.fori_loop(0, ff // CW, act_step, 0)

    def down(l):
        def step(j, c):
            d_copy(l, j).wait()
            for part in (DEC, PRE):
                sent(l, M, part, j)
            pbuf[j] = jnp.dot(act[...], dbuf[lax.rem(j, D_SLOTS)], preferred_element_type=F32).astype(BF16)
            for part in (DEC, PRE):
                p_copy(M, part, j).start()

            @pl.when(j + D_SLOTS < n_chunks)
            def _():
                d_copy(l, j + D_SLOTS).start()

            if l + 1 < layers:
                start(qkv_copies(l + 1, j))

            @pl.when(j >= 1)
            def _():
                pair_sum(M, DEC, j - 1)
            return c

        lax.fori_loop(0, n_chunks, step, 0)
        pair_sum(M, DEC, n_chunks - 1)
        if l + 1 < layers:
            start(kv_pre_copies(l + 1))
            for i in range(KV_SLOTS):
                start(kv_copies(l + 1, i))
            for j in range(n_chunks):
                wo_copy(l + 1, j).start()

        def pre_step(j, c):
            pair_sum(M, PRE, j)
            return c

        lax.fori_loop(0, n_chunks, pre_step, 0)

    for j in range(n_chunks):
        x_load(j).start()
    barrier = pltpu.get_barrier_semaphore()
    for peer in (core_peer, x_peer):
        pl.semaphore_signal(barrier, inc=1, device_id=peer, device_id_type=MESH)
    ssq[...] = jnp.zeros_like(ssq)
    for j in range(n_chunks):
        start(qkv_copies(0, j))
    for i in range(KV_SLOTS):
        start(kv_copies(0, i))
    for j in range(n_chunks):
        wo_copy(0, j).start()
    start(kv_pre_copies(0))
    for j in range(n_chunks):
        x_load(j).wait()

    def sq_step(j, c):
        add_squares(pl.ds(0, rows), h_m[j].astype(F32))
        return c

    lax.fori_loop(0, n_chunks, sq_step, 0)
    pre[...] = jnp.broadcast_to(jnp.maximum(inv_rms(pl.ds(0, rows)), 1e-30), pre.shape)
    ssq[...] = jnp.zeros_like(ssq)
    pl.semaphore_wait(barrier, 2)

    for l in range(layers):
        qkv_part(l, DEC)
        decode_attention(l)
        o_part(l, DEC)
        qkv_part(l, PRE)
        for j in range(G_SLOTS):
            start(g_copies(l, j))
        prefill_attention(l)
        o_part(l, PRE)
        acc[...] = jnp.zeros_like(acc)
        gate_up(l)
        down(l)

    def out_copy(part, j):
        r = whole(part)
        return pltpu.make_async_copy(h_m.at[j, r, :], y.at[r, cols(j)], y_sem.at[part, j])

    for part in (DEC, PRE):
        def out_step(j, c):
            finish(layers - 1, M, part, j)

            @pl.when(j >= 1)
            def _():
                h_wait(M, part, j - 1)
                out_copy(part, j - 1).start()
            return c

        lax.fori_loop(0, n_chunks, out_step, 0)
        h_wait(M, part, n_chunks - 1)
        out_copy(part, n_chunks - 1).start()
    for part in (DEC, PRE):
        for j in range(n_chunks):
            out_copy(part, j).wait()
            h_copy(O, part, j).wait_send()
            h_copy(M, part, j).wait_send()
            p_copy(M, part, j).wait_send()
            x_copy(M, part, j).wait_send()


def step_call(lengths, x, cos_tab, sin_tab, attn_gain, mlp_gain, w_q, w_k, w_v, w_o, w_gate, w_up, w_down, k_cache, v_cache):
    rows, width = x.shape
    dec = lengths.shape[0] - 1
    chunk = rows - dec
    ff = w_gate.shape[2]
    n_chunks = width // CW
    q_cols, k_cols = w_q.shape[2], w_k.shape[2]
    kv_heads, seq, hd = k_cache.shape[2:]
    heads = q_cols // hd
    vmem = pl.BlockSpec(memory_space=pltpu.VMEM)
    hbm = pl.BlockSpec(memory_space=pl.ANY)
    smem = pl.BlockSpec(memory_space=pltpu.SMEM)
    sem = pltpu.SemaphoreType.DMA
    buf = pltpu.VMEM
    return pl.pallas_call(
        functools.partial(step_kernel, (dec, chunk)),
        out_shape=jax.ShapeDtypeStruct((rows, width), BF16),
        in_specs=[smem, hbm, vmem, vmem, vmem, vmem] + [hbm] * 9,
        out_specs=hbm,
        scratch_shapes=[
            buf((G_SLOTS, 2, CW, ff), BF16),
            buf((D_SLOTS, ff, CW), BF16),
            buf((rows, 2 * ff), F32),
            buf((rows, ff), BF16),
            buf((n_chunks, rows, CW), BF16),
            buf((n_chunks, rows // 2, CW), BF16),
            buf((n_chunks, rows // 2, CW), BF16),
            buf((n_chunks, rows // 2, CW), BF16),
            buf((n_chunks, rows, CW), BF16),
            buf((n_chunks, rows, CW), BF16),
            buf((rows, 128), F32),
            buf((rows, 128), F32),
            buf((KV_SLOTS, KV_ROWS, kv_heads, seq, hd), BF16),
            buf((KV_SLOTS, KV_ROWS, kv_heads, seq, hd), BF16),
            buf((kv_heads, seq, hd), BF16),
            buf((kv_heads, seq, hd), BF16),
            buf((dec * heads, hd), F32),
            buf((dec * heads, hd), F32),
            buf((dec * heads, hd), F32),
            buf((chunk, q_cols), BF16),
            buf((chunk, k_cols), BF16),
            buf((chunk, k_cols), BF16),
            buf((rows, q_cols), BF16),
            sem((n_chunks,)),
            sem((n_chunks,)),
            sem((n_chunks,)),
            sem((n_chunks,)),
            sem((G_SLOTS, 2)),
            sem((D_SLOTS,)),
            sem((KV_SLOTS, 2)),
            sem((2,)),
            sem((2, n_chunks)),
            sem((2, 2, n_chunks)),
            sem((2, 2, n_chunks)),
            sem((2, 2, n_chunks)),
            sem((2, 2, n_chunks)),
            sem((2, 2, n_chunks)),
            sem((2, 2, n_chunks)),
        ],
        compiler_params=pltpu.CompilerParams(collective_id=0, has_side_effects=True, vmem_limit_bytes=67043328),
        name='decoder_step',
    )(lengths, x, cos_tab, sin_tab, attn_gain, mlp_gain, w_q, w_k, w_v, w_o, w_gate, w_up, w_down, k_cache, v_cache)


def solution(mesh):
    col_spec = P(None, None, 'tp')
    row_spec = P(None, 'tp', None)
    cache_spec = P(None, 'dp', 'tp', None, None)
    in_specs = (P('dp', None), P('dp'), P(), col_spec, col_spec, col_spec, row_spec, P(), col_spec, col_spec, row_spec, cache_spec, cache_spec)

    def body(x, lengths, attn_gain, w_q, w_k, w_v, w_o, mlp_gain, w_gate, w_up, w_down, k_cache, v_cache):
        dec_rows = lengths.shape[0] - 1
        chunk_len = x.shape[0] - dec_rows
        head_dim = k_cache.shape[-1]
        positions = jnp.concatenate([lengths[:dec_rows], lengths[dec_rows] + jnp.arange(chunk_len, dtype=jnp.int32)])
        freq_exps = jnp.arange(0, head_dim, 2, dtype=F32) / head_dim
        angles = positions.astype(F32)[:, None] * jnp.power(ROPE_BASE, -freq_exps)[None, :]
        cos_tab, sin_tab = jnp.cos(angles), jnp.sin(angles)
        cos_tab = jnp.concatenate([cos_tab, cos_tab], axis=-1)
        sin_tab = jnp.concatenate([-sin_tab, sin_tab], axis=-1)
        return step_call(lengths, x, cos_tab, sin_tab, attn_gain.astype(F32), mlp_gain.astype(F32), w_q, w_k, w_v, w_o, w_gate, w_up, w_down, k_cache, v_cache)

    return jax.shard_map(body, mesh=mesh, in_specs=in_specs, out_specs=P('dp', None), check_vma=False)
```

```python
import functools

import jax
import jax.numpy as jnp
import numpy as np
from jax import lax
from jax.experimental import pallas as pl
from jax.experimental.pallas import tpu as pltpu
from jax.sharding import PartitionSpec as P

ROPE_BASE = 500000.0
EPSILON = 1e-5
MESH = pl.DeviceIdType.MESH
F32 = jnp.float32
BF16 = jnp.bfloat16
CW = 512
G_SLOTS = 5
D_SLOTS = 4
KV_SLOTS = 2
KV_ROWS = 16
O, M = 0, 1
DEC, PRE = 0, 1


def step_kernel(dims, lens, x_in, freq, gain_a, gain_m, wq, wk, wv, wo, wg, wu, wd, kc, vc, y,
                gbuf, dbuf, acc, act, pbuf, rbuf, xb_o, xb_m, h_o, h_m, ssq, pre, cos, sin, kbuf, vbuf, kpre, vpre,
                qs, kn, vn, qp, kp, vp, att,
                q_sem, w_sem, k_sem, v_sem, g_sem, d_sem, kv_sem, kvp_sem, y_sem, p_ss, p_rs, x_ss, x_rs, h_ss, h_rs):
    dec, chunk = dims
    rows = dec + chunk
    width = x_in.shape[1]
    layers, o_depth = wo.shape[0], wo.shape[1]
    ff = wg.shape[2]
    q_cols, k_cols = wq.shape[2], wk.shape[2]
    n_qkv = q_cols + 2 * k_cols
    seq, hd = kc.shape[3], kc.shape[4]
    heads, kv_heads = q_cols // hd, k_cols // hd
    group = heads // kv_heads
    n_chunks = width // CW
    o_per_slot = ff // o_depth
    scale_qk = hd ** -0.5
    base = (0, dec)
    size = (dec, chunk)
    half = (dec // 2, chunk // 2)
    rbase = (0, dec // 2)

    dp_me = lax.axis_index('dp')
    me = lax.axis_index('tp')
    core = lax.rem(me, 2)
    core_peer = (dp_me, me + 1 - 2 * core)
    x_peer = (dp_me, lax.rem(me + 2, 4))

    def own(part):
        return pl.ds(pl.multiple_of(base[part] + core * half[part], 16), half[part])

    def oth(part):
        return pl.ds(pl.multiple_of(base[part] + (1 - core) * half[part], 16), half[part])

    def whole(part):
        return pl.ds(base[part], size[part])

    def landed(part):
        return pl.ds(rbase[part], half[part])

    def cols(j):
        return pl.ds(pl.multiple_of(j * CW, CW), CW)

    xbs = (xb_o, xb_m)
    hs = (h_o, h_m)

    def x_load(j):
        return pltpu.make_async_copy(x_in.at[:, cols(j)], h_m.at[j], y_sem.at[0, j])

    def wo_copy(l, j):
        return pltpu.make_async_copy(wo.at[l, :, cols(j)], dbuf.at[j // o_per_slot, pl.ds(pl.multiple_of(lax.rem(j, o_per_slot) * o_depth, 16), o_depth), :], w_sem.at[j])

    def g_copy(l, j, m):
        slot = lax.rem(2 * j + m, G_SLOTS)
        return pltpu.make_async_copy((wg, wu)[m].at[l, cols(j), :], gbuf.at[slot], g_sem.at[slot])

    def d_copy(l, j):
        slot = lax.rem(j, D_SLOTS)
        return pltpu.make_async_copy(wd.at[l, :, cols(j)], dbuf.at[slot], d_sem.at[slot])

    def qkv_place(j):
        return j // 2, lax.rem(j, 2) * (ff // 2)

    def qkv_copies(l, j):
        slot, left = qkv_place(j)
        dst = gbuf.at[slot]

        def at(off, n):
            return dst.at[:, pl.ds(pl.multiple_of(left + off, 128), n)]

        return (pltpu.make_async_copy(wq.at[l, cols(j), :], at(0, q_cols), q_sem.at[j]),
                pltpu.make_async_copy(wk.at[l, cols(j), :], at(q_cols, k_cols), k_sem.at[j]),
                pltpu.make_async_copy(wv.at[l, cols(j), :], at(q_cols + k_cols, k_cols), v_sem.at[j]))

    def kv_copies(l, i):
        slot = lax.rem(i, KV_SLOTS)
        src = pl.ds(i * KV_ROWS, KV_ROWS)
        return (pltpu.make_async_copy(kc.at[l, src], kbuf.at[slot], kv_sem.at[slot, 0]),
                pltpu.make_async_copy(vc.at[l, src], vbuf.at[slot], kv_sem.at[slot, 1]))

    def kv_pre_copies(l):
        return (pltpu.make_async_copy(kc.at[l, dec], kpre, kvp_sem.at[0]),
                pltpu.make_async_copy(vc.at[l, dec], vpre, kvp_sem.at[1]))

    def start(copies):
        for c in copies:
            c.start()

    def wait(copies):
        for c in copies:
            c.wait()

    def p_copy(ar, part, j):
        return pltpu.make_async_remote_copy(pbuf.at[j, oth(part), :], rbuf.at[j, landed(part), :], p_ss.at[ar, part, j], p_rs.at[ar, part, j], device_id=core_peer, device_id_type=MESH)

    def x_copy(ar, part, j):
        return pltpu.make_async_remote_copy(pbuf.at[j, own(part), :], xbs[ar].at[j, landed(part), :], x_ss.at[ar, part, j], x_rs.at[ar, part, j], device_id=x_peer, device_id_type=MESH)

    def h_copy(ar, part, j):
        return pltpu.make_async_remote_copy(hs[ar].at[j, own(part), :], hs[ar].at[j, own(part), :], h_ss.at[ar, part, j], h_rs.at[ar, part, j], device_id=core_peer, device_id_type=MESH)

    def h_wait(ar, part, j):
        pltpu.make_async_remote_copy(hs[ar].at[j, oth(part), :], hs[ar].at[j, oth(part), :], h_ss.at[ar, part, j], h_rs.at[ar, part, j], device_id=core_peer, device_id_type=MESH).wait_recv()

    def sent(l, ar, part, j):
        if l > 0 or ar == M:
            p_copy(1 - ar, part, j).wait_send()
            x_copy(1 - ar, part, j).wait_send()

    def pair_sum(ar, part, j):
        p_copy(ar, part, j).wait_recv()
        pbuf[j, own(part), :] = (pbuf[j, own(part), :].astype(F32) + rbuf[j, landed(part), :].astype(F32)).astype(BF16)
        x_copy(ar, part, j).start()

    def finish(l, ar, part, j):
        x_copy(ar, part, j).wait_recv()
        total = pbuf[j, own(part), :].astype(F32) + xbs[ar][j, landed(part), :].astype(F32)
        resid = hs[1 - ar][j, own(part), :].astype(F32)
        if l > 0:
            h_copy(ar, part, j).wait_send()
        hs[ar][j, own(part), :] = (resid + total).astype(BF16)
        h_copy(ar, part, j).start()

    def add_squares(r, vals):
        sq = vals * vals
        ssq[r, :] += sq[:, :128] + sq[:, 128:256] + sq[:, 256:384] + sq[:, 384:]

    def inv_rms(r):
        return lax.rsqrt(jnp.sum(ssq[r, :], axis=-1, keepdims=True) * (1.0 / width) + EPSILON)

    def next_scale(r):
        inv = inv_rms(r)
        scale = inv / pre[r, :1]
        n = ssq[r, :].shape[0]
        pre[r, :] = jnp.broadcast_to(jnp.maximum(inv, 1e-30), (n, 128))
        ssq[r, :] = jnp.zeros((n, 128), F32)
        return scale

    def qkv_block(l, part, pair):
        r = whole(part)
        a = []
        for j in pair:
            if l > 0:
                h_wait(M, part, j)
            vals = h_m[j, r, :].astype(F32)
            add_squares(r, vals)
            a.append((vals * pre[r, :1] * gain_a[l:l + 1, cols(j)].astype(F32)).astype(BF16))
            if part == DEC:
                wait(qkv_copies(l, j))
        for n in range(n_qkv // CW):
            total = acc[r, n * CW:(n + 1) * CW]
            for j, a_j in zip(pair, a):
                slot, left = qkv_place(j)
                total += jnp.dot(a_j, gbuf[slot, :, pl.ds(pl.multiple_of(left + n * CW, 128), CW)], preferred_element_type=F32)
            acc[r, n * CW:(n + 1) * CW] = total

    def qkv_part(l, part):
        r = whole(part)
        acc[r, :n_qkv] = jnp.zeros((size[part], n_qkv), F32)
        n_pairs = n_chunks // 2

        def pair_of(i):
            return 2 * i, 2 * i + 1

        def step(i, c):
            if l > 0 and part == DEC:
                for j in pair_of(i):
                    finish(l - 1, M, part, j)

                @pl.when(i >= 1)
                def _():
                    qkv_block(l, part, pair_of(i - 1))
            else:
                qkv_block(l, part, pair_of(i))
            return c

        lax.fori_loop(0, n_pairs, step, 0)
        if l > 0 and part == DEC:
            qkv_block(l, part, pair_of(n_pairs - 1))
        scale = next_scale(r)
        c_tab, s_tab = cos[r, :], sin[r, :]

        def head(col):
            return (acc[r, col * hd:(col + 1) * hd] * scale).astype(BF16).astype(F32)

        def rope(t):
            return (t * c_tab + pltpu.roll(t, hd // 2, 1) * s_tab).astype(BF16)

        for h in range(heads):
            q = rope(head(h))
            if part == DEC:
                qs[pl.ds(h, dec, stride=heads), :] = q.astype(F32)
            else:
                qp[:, h * hd:(h + 1) * hd] = q
        for g in range(kv_heads):
            k = rope(head(heads + g))
            v = head(heads + kv_heads + g)
            if part == DEC:
                for h in range(g * group, (g + 1) * group):
                    kn[pl.ds(h, dec, stride=heads), :] = k.astype(F32)
                    vn[pl.ds(h, dec, stride=heads), :] = v
            else:
                kp[:, g * hd:(g + 1) * hd] = k
                vp[:, g * hd:(g + 1) * hd] = v.astype(BF16)

    def decode_attention(l):
        first_rows = lax.broadcasted_iota(jnp.int32, (heads, hd), 0) < group
        places = lax.broadcasted_iota(jnp.int32, (heads, seq), 1)
        n_blocks = dec // KV_ROWS

        def block(i, c):
            wait(kv_copies(l, i))
            slot = lax.rem(i, KV_SLOTS)
            if l == 0:
                @pl.when(i == n_blocks - KV_SLOTS)
                def _():
                    for j in range(n_chunks):
                        wo_copy(l, j).start()
            scores = []
            for n in range(KV_ROWS):
                b = i * KV_ROWS + n
                q = qs[pl.ds(pl.multiple_of(b * heads, heads), heads), :]
                zero = jnp.zeros_like(q)
                q2 = jnp.concatenate([jnp.where(first_rows, q, zero), jnp.where(first_rows, zero, q)], axis=1).astype(BF16)
                k2 = jnp.concatenate([kbuf[slot, n, 0], kbuf[slot, n, 1]], axis=1)
                s = lax.dot_general(q2, k2, (((1,), (1,)), ((), ())), preferred_element_type=F32) * scale_qk
                scores.append(jnp.where(places < lens[b], s, -jnp.inf))
            r = pl.ds(pl.multiple_of(i * KV_ROWS * heads, KV_ROWS * heads), KV_ROWS * heads)
            s = jnp.concatenate(scores, axis=0)
            s_new = jnp.sum(qs[r, :] * kn[r, :], axis=-1, keepdims=True) * scale_qk
            top = jnp.maximum(jnp.max(s, axis=-1, keepdims=True), s_new)
            e = jnp.exp(s - top)
            e_new = jnp.exp(s_new - top)
            inv = 1.0 / (jnp.sum(e, axis=-1, keepdims=True) + e_new)
            p = (e * inv).astype(BF16)
            p_new = (e_new * inv).astype(BF16).astype(F32)
            outs = []
            for n in range(KV_ROWS):
                v2 = jnp.concatenate([vbuf[slot, n, 0], vbuf[slot, n, 1]], axis=1)
                o = jnp.dot(p[n * heads:(n + 1) * heads], v2, preferred_element_type=F32)
                outs.append(jnp.where(first_rows, o[:, :hd], o[:, hd:]))
            qs[r, :] = jnp.concatenate(outs, axis=0) + p_new * vn[r, :]

            @pl.when(i + KV_SLOTS < n_blocks)
            def _():
                start(kv_copies(l, i + KV_SLOTS))
            return c

        lax.fori_loop(0, n_blocks, block, 0)
        for h in range(heads):
            att[:dec, h * hd:(h + 1) * hd] = qs[pl.ds(h, dec, stride=heads), :].astype(BF16)

    def prefill_attention(l):
        wait(kv_pre_copies(l))
        n_old = lens[dec]
        old = lax.broadcasted_iota(jnp.int32, (chunk, seq), 1) < n_old
        causal = lax.broadcasted_iota(jnp.int32, (chunk, chunk), 1) <= lax.broadcasted_iota(jnp.int32, (chunk, chunk), 0)

        def heads_step(i, c):
            for g in range(kv_heads):
                col = pl.ds(pl.multiple_of((g * group + i) * hd, hd), hd)
                q = qp[:, col]
                kv_col = slice(g * hd, (g + 1) * hd)
                s = lax.dot_general(q, kpre[g], (((1,), (1,)), ((), ())), preferred_element_type=F32) * scale_qk
                s = jnp.where(old, s, -jnp.inf)
                t = lax.dot_general(q, kp[:, kv_col], (((1,), (1,)), ((), ())), preferred_element_type=F32) * scale_qk
                t = jnp.where(causal, t, -jnp.inf)
                top = jnp.maximum(jnp.max(s, axis=-1, keepdims=True), jnp.max(t, axis=-1, keepdims=True))
                es = jnp.exp(s - top)
                et = jnp.exp(t - top)
                inv = 1.0 / (jnp.sum(es, axis=-1, keepdims=True) + jnp.sum(et, axis=-1, keepdims=True))
                o = jnp.dot((es * inv).astype(BF16), vpre[g], preferred_element_type=F32)
                o += jnp.dot((et * inv).astype(BF16), vp[:, kv_col], preferred_element_type=F32)
                att[pl.ds(dec, chunk), col] = o.astype(BF16)
            return c

        lax.fori_loop(0, group, heads_step, 0)

    def o_part(l, part):
        r = whole(part)
        lag = 2

        def step(i, c):
            pair = (2 * i, 2 * i + 1)
            for j in pair:
                if part == DEC:
                    wo_copy(l, j).wait()
                sent(l, O, part, j)
            prods = []
            for j in pair:
                w = dbuf[j // o_per_slot, pl.ds(pl.multiple_of(lax.rem(j, o_per_slot) * o_depth, 16), o_depth), :]
                prods.append(jnp.dot(att[r, :], w, preferred_element_type=F32).astype(BF16))
            for j, prod in zip(pair, prods):
                pbuf[j, r, :] = prod
                p_copy(O, part, j).start()

            @pl.when(i >= lag)
            def _():
                for j in pair:
                    pair_sum(O, part, j - 2 * lag)
            return c

        lax.fori_loop(0, n_chunks // 2, step, 0)
        if l > 0 and part == DEC:
            def pre_step(j, c):
                finish(l - 1, M, PRE, j)
                return c

            lax.fori_loop(0, n_chunks, pre_step, 0)
        for j in range(n_chunks - 2 * lag, n_chunks):
            pair_sum(O, part, j)

    def gate_up(l):
        def block(j):
            h_wait(O, DEC, j)
            h_wait(O, PRE, j)
            vals = h_o[j].astype(F32)
            add_squares(pl.ds(0, rows), vals)
            a = (vals * pre[:, :1] * gain_m[l:l + 1, cols(j)].astype(F32)).astype(BF16)
            for m in range(2):
                g_copy(l, j, m).wait()
                slot = lax.rem(2 * j + m, G_SLOTS)
                for n in range(ff // CW):
                    acc[:, m * ff + n * CW:m * ff + (n + 1) * CW] += jnp.dot(a, gbuf[slot, :, n * CW:(n + 1) * CW], preferred_element_type=F32)
                nxt = j + (G_SLOTS + m) // 2

                @pl.when(nxt < n_chunks)
                def _():
                    g_copy(l, nxt, (G_SLOTS + m) % 2).start()

            @pl.when(j >= n_chunks - D_SLOTS)
            def _():
                d_copy(l, j - (n_chunks - D_SLOTS)).start()

        def step(j, c):
            finish(l, O, DEC, j)
            finish(l, O, PRE, j)

            @pl.when(j >= 1)
            def _():
                block(j - 1)
            return c

        lax.fori_loop(0, n_chunks, step, 0)
        block(n_chunks - 1)
        scale = next_scale(pl.ds(0, rows))

        def act_step(n, c):
            gate = acc[:, cols(n)] * scale
            up = acc[:, pl.ds(pl.multiple_of(ff + n * CW, CW), CW)] * scale
            act[:, cols(n)] = (gate * jax.nn.sigmoid(gate) * up).astype(BF16)
            return c

        lax.fori_loop(0, ff // CW, act_step, 0)

    def down(l):
        def step(j, c):
            d_copy(l, j).wait()
            for part in (DEC, PRE):
                sent(l, M, part, j)
            pbuf[j] = jnp.dot(act[...], dbuf[lax.rem(j, D_SLOTS)], preferred_element_type=F32).astype(BF16)
            for part in (DEC, PRE):
                p_copy(M, part, j).start()

            @pl.when(j + D_SLOTS < n_chunks)
            def _():
                d_copy(l, j + D_SLOTS).start()

            if l + 1 < layers:
                start(qkv_copies(l + 1, j))

            @pl.when(j >= 1)
            def _():
                pair_sum(M, DEC, j - 1)
            return c

        lax.fori_loop(0, n_chunks, step, 0)
        pair_sum(M, DEC, n_chunks - 1)
        if l + 1 < layers:
            start(kv_pre_copies(l + 1))
            for i in range(KV_SLOTS):
                start(kv_copies(l + 1, i))
            for j in range(n_chunks):
                wo_copy(l + 1, j).start()

        def pre_step(j, c):
            pair_sum(M, PRE, j)
            return c

        lax.fori_loop(0, n_chunks, pre_step, 0)

    for j in range(n_chunks):
        x_load(j).start()
    barrier = pltpu.get_barrier_semaphore()
    for peer in (core_peer, x_peer):
        pl.semaphore_signal(barrier, inc=1, device_id=peer, device_id_type=MESH)
    for j in range(n_chunks):
        start(qkv_copies(0, j))
    for i in range(KV_SLOTS):
        start(kv_copies(0, i))
    start(kv_pre_copies(0))
    ssq[...] = jnp.zeros_like(ssq)

    def place(b, c):
        cos[pl.ds(b, 1), :] = jnp.full((1, hd), lens[b], jnp.int32).astype(F32)
        return c

    lax.fori_loop(0, dec, place, 0)
    cos[pl.ds(dec, chunk), :] = (lax.broadcasted_iota(jnp.int32, (chunk, hd), 0) + lens[dec]).astype(F32)
    angles = cos[...] * freq[...]
    low = lax.broadcasted_iota(jnp.int32, (rows, hd), 1) < hd // 2
    sines = jnp.sin(angles)
    sin[...] = jnp.where(low, -sines, sines)
    cos[...] = jnp.cos(angles)
    for j in range(n_chunks):
        x_load(j).wait()

    def sq_step(j, c):
        add_squares(pl.ds(0, rows), h_m[j].astype(F32))
        return c

    lax.fori_loop(0, n_chunks, sq_step, 0)
    pre[...] = jnp.broadcast_to(jnp.maximum(inv_rms(pl.ds(0, rows)), 1e-30), pre.shape)
    ssq[...] = jnp.zeros_like(ssq)
    pl.semaphore_wait(barrier, 2)

    for l in range(layers):
        qkv_part(l, DEC)
        decode_attention(l)
        o_part(l, DEC)
        qkv_part(l, PRE)
        for i in range(G_SLOTS):
            g_copy(l, i // 2, i % 2).start()
        prefill_attention(l)
        o_part(l, PRE)
        acc[...] = jnp.zeros_like(acc)
        gate_up(l)
        down(l)

    def out_copy(part, j):
        r = whole(part)
        return pltpu.make_async_copy(h_m.at[j, r, :], y.at[r, cols(j)], y_sem.at[part, j])

    for part in (DEC, PRE):
        def out_step(j, c):
            finish(layers - 1, M, part, j)

            @pl.when(j >= 1)
            def _():
                h_wait(M, part, j - 1)
                out_copy(part, j - 1).start()
            return c

        lax.fori_loop(0, n_chunks, out_step, 0)
        h_wait(M, part, n_chunks - 1)
        out_copy(part, n_chunks - 1).start()
    for part in (DEC, PRE):
        for j in range(n_chunks):
            out_copy(part, j).wait()
            h_copy(O, part, j).wait_send()
            h_copy(M, part, j).wait_send()
            p_copy(M, part, j).wait_send()
            x_copy(M, part, j).wait_send()


def step_call(lengths, x, freq, attn_gain, mlp_gain, w_q, w_k, w_v, w_o, w_gate, w_up, w_down, k_cache, v_cache):
    rows, width = x.shape
    dec = lengths.shape[0] - 1
    chunk = rows - dec
    ff = w_gate.shape[2]
    n_chunks = width // CW
    q_cols, k_cols = w_q.shape[2], w_k.shape[2]
    kv_heads, seq, hd = k_cache.shape[2:]
    heads = q_cols // hd
    vmem = pl.BlockSpec(memory_space=pltpu.VMEM)
    hbm = pl.BlockSpec(memory_space=pl.ANY)
    smem = pl.BlockSpec(memory_space=pltpu.SMEM)
    sem = pltpu.SemaphoreType.DMA
    buf = pltpu.VMEM
    return pl.pallas_call(
        functools.partial(step_kernel, (dec, chunk)),
        out_shape=jax.ShapeDtypeStruct((rows, width), BF16),
        in_specs=[smem, hbm, vmem, vmem, vmem] + [hbm] * 9,
        out_specs=hbm,
        scratch_shapes=[
            buf((G_SLOTS, CW, ff), BF16),
            buf((D_SLOTS, ff, CW), BF16),
            buf((rows, 2 * ff), F32),
            buf((rows, ff), BF16),
            buf((n_chunks, rows, CW), BF16),
            buf((n_chunks, rows // 2, CW), BF16),
            buf((n_chunks, rows // 2, CW), BF16),
            buf((n_chunks, rows // 2, CW), BF16),
            buf((n_chunks, rows, CW), BF16),
            buf((n_chunks, rows, CW), BF16),
            buf((rows, 128), F32),
            buf((rows, 128), F32),
            buf((rows, hd), F32),
            buf((rows, hd), F32),
            buf((KV_SLOTS, KV_ROWS, kv_heads, seq, hd), BF16),
            buf((KV_SLOTS, KV_ROWS, kv_heads, seq, hd), BF16),
            buf((kv_heads, seq, hd), BF16),
            buf((kv_heads, seq, hd), BF16),
            buf((dec * heads, hd), F32),
            buf((dec * heads, hd), F32),
            buf((dec * heads, hd), F32),
            buf((chunk, q_cols), BF16),
            buf((chunk, k_cols), BF16),
            buf((chunk, k_cols), BF16),
            buf((rows, q_cols), BF16),
            sem((n_chunks,)),
            sem((n_chunks,)),
            sem((n_chunks,)),
            sem((n_chunks,)),
            sem((G_SLOTS,)),
            sem((D_SLOTS,)),
            sem((KV_SLOTS, 2)),
            sem((2,)),
            sem((2, n_chunks)),
            sem((2, 2, n_chunks)),
            sem((2, 2, n_chunks)),
            sem((2, 2, n_chunks)),
            sem((2, 2, n_chunks)),
            sem((2, 2, n_chunks)),
            sem((2, 2, n_chunks)),
        ],
        compiler_params=pltpu.CompilerParams(collective_id=0, has_side_effects=True, vmem_limit_bytes=67043328),
        name='decoder_step',
    )(lengths, x, freq, attn_gain, mlp_gain, w_q, w_k, w_v, w_o, w_gate, w_up, w_down, k_cache, v_cache)


def solution(mesh):
    col_spec = P(None, None, 'tp')
    row_spec = P(None, 'tp', None)
    cache_spec = P(None, 'dp', 'tp', None, None)
    in_specs = (P('dp', None), P('dp'), P(), col_spec, col_spec, col_spec, row_spec, P(), col_spec, col_spec, row_spec, cache_spec, cache_spec)

    def body(x, lengths, attn_gain, w_q, w_k, w_v, w_o, mlp_gain, w_gate, w_up, w_down, k_cache, v_cache):
        head_dim = k_cache.shape[-1]
        exps = np.arange(0, head_dim, 2, dtype=np.float32) / np.float32(head_dim)
        freq = np.power(np.float32(ROPE_BASE), -exps).astype(np.float32)
        freq = jnp.asarray(np.concatenate([freq, freq])[None])
        return step_call(lengths, x, freq, attn_gain, mlp_gain, w_q, w_k, w_v, w_o, w_gate, w_up, w_down, k_cache, v_cache)

    return jax.shard_map(body, mesh=mesh, in_specs=in_specs, out_specs=P('dp', None), check_vma=False)
```

```python
import functools

import jax
import jax.numpy as jnp
import numpy as np
from jax import lax
from jax.experimental import pallas as pl
from jax.experimental.pallas import tpu as pltpu
from jax.sharding import PartitionSpec as P

ROPE_BASE = 500000.0
EPSILON = 1e-5
MESH = pl.DeviceIdType.MESH
F32 = jnp.float32
BF16 = jnp.bfloat16
CW = 512
G_SLOTS = 5
D_SLOTS = 4
KV_SLOTS = 5
KV_ROWS = 8
ATT_SLOTS = 2
GROUP = 5
O, M = 0, 1
DEC, PRE = 0, 1


def step_kernel(dims, lens, x_in, freq, gain_a, gain_m, wq, wk, wv, wo, wg, wu, wd, kc, vc, y,
                gbuf, dbuf, acc, act, pbuf, rbuf, xb_o, xb_m, h_o, h_m, ssq, pre, cos, sin, kbuf, vbuf, kpre, vpre,
                qs, kn, vn, qp, kp, vp, att,
                q_sem, w_sem, k_sem, v_sem, g_sem, d_sem, kv_sem, kvp_sem, y_sem, p_ss, p_rs, x_ss, x_rs, h_ss, h_rs):
    dec, chunk = dims
    rows = dec + chunk
    width = x_in.shape[1]
    layers, o_depth = wo.shape[0], wo.shape[1]
    ff = wg.shape[2]
    q_cols, k_cols = wq.shape[2], wk.shape[2]
    n_qkv = q_cols + 2 * k_cols
    seq, hd = kc.shape[3], kc.shape[4]
    heads, kv_heads = q_cols // hd, k_cols // hd
    group = heads // kv_heads
    n_chunks = width // CW
    o_per_slot = ff // o_depth
    scale_qk = hd ** -0.5
    base = (0, dec)
    size = (dec, chunk)
    half = (dec // 2, chunk // 2)
    rbase = (0, dec // 2)

    dp_me = lax.axis_index('dp')
    me = lax.axis_index('tp')
    core = lax.rem(me, 2)
    core_peer = (dp_me, me + 1 - 2 * core)
    x_peer = (dp_me, lax.rem(me + 2, 4))

    def own(part):
        return pl.ds(pl.multiple_of(base[part] + core * half[part], 16), half[part])

    def oth(part):
        return pl.ds(pl.multiple_of(base[part] + (1 - core) * half[part], 16), half[part])

    def whole(part):
        return pl.ds(base[part], size[part])

    def landed(part):
        return pl.ds(rbase[part], half[part])

    def cols(j):
        return pl.ds(pl.multiple_of(j * CW, CW), CW)

    xbs = (xb_o, xb_m)
    hs = (h_o, h_m)

    def x_load(j):
        return pltpu.make_async_copy(x_in.at[:, cols(j)], h_m.at[j], y_sem.at[0, j])

    def wo_copy(l, j):
        return pltpu.make_async_copy(wo.at[l, :, cols(j)], dbuf.at[j // o_per_slot, pl.ds(pl.multiple_of(lax.rem(j, o_per_slot) * o_depth, 16), o_depth), :], w_sem.at[j])

    def g_copy(l, j, m):
        slot = lax.rem(2 * j + m, G_SLOTS)
        return pltpu.make_async_copy((wg, wu)[m].at[l, cols(j), :], gbuf.at[slot], g_sem.at[slot])

    def d_copy(l, j):
        slot = lax.rem(j, D_SLOTS)
        return pltpu.make_async_copy(wd.at[l, :, cols(j)], dbuf.at[slot], d_sem.at[slot])

    def qkv_place(j):
        return j // 2, lax.rem(j, 2) * (ff // 2)

    def qkv_copies(l, j):
        slot, left = qkv_place(j)
        dst = gbuf.at[slot]

        def at(off, n):
            return dst.at[:, pl.ds(pl.multiple_of(left + off, 128), n)]

        return (pltpu.make_async_copy(wq.at[l, cols(j), :], at(0, q_cols), q_sem.at[j]),
                pltpu.make_async_copy(wk.at[l, cols(j), :], at(q_cols, k_cols), k_sem.at[j]),
                pltpu.make_async_copy(wv.at[l, cols(j), :], at(q_cols + k_cols, k_cols), v_sem.at[j]))

    def kv_copies(l, i):
        slot = lax.rem(i, KV_SLOTS)
        src = pl.ds(i * KV_ROWS, KV_ROWS)
        return (pltpu.make_async_copy(kc.at[l, src], kbuf.at[slot], kv_sem.at[slot, 0]),
                pltpu.make_async_copy(vc.at[l, src], vbuf.at[slot], kv_sem.at[slot, 1]))

    def kv_pre_copies(l):
        return (pltpu.make_async_copy(kc.at[l, dec], kpre, kvp_sem.at[0]),
                pltpu.make_async_copy(vc.at[l, dec], vpre, kvp_sem.at[1]))

    def start(copies):
        for c in copies:
            c.start()

    def wait(copies):
        for c in copies:
            c.wait()

    def p_copy(ar, part, j):
        return pltpu.make_async_remote_copy(pbuf.at[j, oth(part), :], rbuf.at[j, landed(part), :], p_ss.at[ar, part, j], p_rs.at[ar, part, j], device_id=core_peer, device_id_type=MESH)

    def x_copy(ar, part, j):
        return pltpu.make_async_remote_copy(pbuf.at[j, own(part), :], xbs[ar].at[j, landed(part), :], x_ss.at[ar, part, j], x_rs.at[ar, part, j], device_id=x_peer, device_id_type=MESH)

    def h_copy(ar, part, j):
        return pltpu.make_async_remote_copy(hs[ar].at[j, own(part), :], hs[ar].at[j, own(part), :], h_ss.at[ar, part, j], h_rs.at[ar, part, j], device_id=core_peer, device_id_type=MESH)

    def h_wait(ar, part, j):
        pltpu.make_async_remote_copy(hs[ar].at[j, oth(part), :], hs[ar].at[j, oth(part), :], h_ss.at[ar, part, j], h_rs.at[ar, part, j], device_id=core_peer, device_id_type=MESH).wait_recv()

    def sent(l, ar, part, j):
        if l > 0 or ar == M:
            p_copy(1 - ar, part, j).wait_send()
            x_copy(1 - ar, part, j).wait_send()

    def pair_sum(ar, part, j):
        p_copy(ar, part, j).wait_recv()
        pbuf[j, own(part), :] = (pbuf[j, own(part), :].astype(F32) + rbuf[j, landed(part), :].astype(F32)).astype(BF16)
        x_copy(ar, part, j).start()

    def finish(l, ar, part, j):
        x_copy(ar, part, j).wait_recv()
        total = pbuf[j, own(part), :].astype(F32) + xbs[ar][j, landed(part), :].astype(F32)
        resid = hs[1 - ar][j, own(part), :].astype(F32)
        if l > 0:
            h_copy(ar, part, j).wait_send()
        hs[ar][j, own(part), :] = (resid + total).astype(BF16)
        h_copy(ar, part, j).start()

    def add_squares(r, vals):
        sq = vals * vals
        ssq[r, :] += sq[:, :128] + sq[:, 128:256] + sq[:, 256:384] + sq[:, 384:]

    def inv_rms(r):
        return lax.rsqrt(jnp.sum(ssq[r, :], axis=-1, keepdims=True) * (1.0 / width) + EPSILON)

    def next_scale(r):
        inv = inv_rms(r)
        scale = inv / pre[r, :1]
        n = ssq[r, :].shape[0]
        pre[r, :] = jnp.broadcast_to(jnp.maximum(inv, 1e-30), (n, 128))
        ssq[r, :] = jnp.zeros((n, 128), F32)
        return scale

    def qkv_block(l, part, pair):
        r = whole(part)
        a = []
        for j in pair:
            if l > 0:
                h_wait(M, part, j)
            vals = h_m[j, r, :].astype(F32)
            add_squares(r, vals)
            a.append((vals * pre[r, :1] * gain_a[l:l + 1, cols(j)].astype(F32)).astype(BF16))
            if part == DEC:
                wait(qkv_copies(l, j))
        for n in range(n_qkv // CW):
            total = acc[r, n * CW:(n + 1) * CW]
            for j, a_j in zip(pair, a):
                slot, left = qkv_place(j)
                total += jnp.dot(a_j, gbuf[slot, :, pl.ds(pl.multiple_of(left + n * CW, 128), CW)], preferred_element_type=F32)
            acc[r, n * CW:(n + 1) * CW] = total

    def qkv_part(l, part):
        r = whole(part)
        acc[r, :n_qkv] = jnp.zeros((size[part], n_qkv), F32)
        n = GROUP if part == PRE else 2
        steps = n_chunks // n
        arriving = l > 0 and part == DEC

        def chunks_of(i):
            return tuple(n * i + t for t in range(n))

        def step(i, c):
            if arriving:
                for j in chunks_of(i):
                    finish(l - 1, M, part, j)

                @pl.when(i >= 1)
                def _():
                    qkv_block(l, part, chunks_of(i - 1))
            else:
                qkv_block(l, part, chunks_of(i))
            if l == 0 and part == DEC:
                @pl.when(i == 2)
                def _():
                    for j in range(n_chunks):
                        wo_copy(l, j).start()
            return c

        lax.fori_loop(0, steps, step, 0)
        if arriving:
            qkv_block(l, part, chunks_of(steps - 1))
        scale = next_scale(r)
        c_tab, s_tab = cos[r, :], sin[r, :]

        def head(col):
            return (acc[r, col * hd:(col + 1) * hd] * scale).astype(BF16).astype(F32)

        def rope(t):
            return (t * c_tab + pltpu.roll(t, hd // 2, 1) * s_tab).astype(BF16)

        for h in range(heads):
            q = rope(head(h))
            if part == DEC:
                qs[pl.ds(h, dec, stride=heads), :] = q.astype(F32)
            else:
                qp[:, h * hd:(h + 1) * hd] = q
        for g in range(kv_heads):
            k = rope(head(heads + g))
            v = head(heads + kv_heads + g)
            if part == DEC:
                for h in range(g * group, (g + 1) * group):
                    kn[pl.ds(h, dec, stride=heads), :] = k.astype(F32)
                    vn[pl.ds(h, dec, stride=heads), :] = v
            else:
                kp[:, g * hd:(g + 1) * hd] = k
                vp[:, g * hd:(g + 1) * hd] = v.astype(BF16)

    def decode_attention(l):
        first_rows = lax.broadcasted_iota(jnp.int32, (heads, hd), 0) < group
        places = lax.broadcasted_iota(jnp.int32, (heads, seq), 1)
        n_slots = dec // KV_ROWS
        step_rows = ATT_SLOTS * KV_ROWS

        def block(i, c):
            slots = []
            for t in range(ATT_SLOTS):
                wait(kv_copies(l, ATT_SLOTS * i + t))
                slots.append(lax.rem(ATT_SLOTS * i + t, KV_SLOTS))
            scores = []
            for n in range(step_rows):
                b = i * step_rows + n
                slot, m = slots[n // KV_ROWS], n % KV_ROWS
                q = qs[pl.ds(pl.multiple_of(b * heads, heads), heads), :]
                zero = jnp.zeros_like(q)
                q2 = jnp.concatenate([jnp.where(first_rows, q, zero), jnp.where(first_rows, zero, q)], axis=1).astype(BF16)
                k2 = jnp.concatenate([kbuf[slot, m, 0], kbuf[slot, m, 1]], axis=1)
                s = lax.dot_general(q2, k2, (((1,), (1,)), ((), ())), preferred_element_type=F32) * scale_qk
                scores.append(jnp.where(places < lens[b], s, -jnp.inf))
            r = pl.ds(pl.multiple_of(i * step_rows * heads, step_rows * heads), step_rows * heads)
            s = jnp.concatenate(scores, axis=0)
            s_new = jnp.sum(qs[r, :] * kn[r, :], axis=-1, keepdims=True) * scale_qk
            top = jnp.maximum(jnp.max(s, axis=-1, keepdims=True), s_new)
            e = jnp.exp(s - top)
            e_new = jnp.exp(s_new - top)
            inv = 1.0 / (jnp.sum(e, axis=-1, keepdims=True) + e_new)
            p = (e * inv).astype(BF16)
            p_new = (e_new * inv).astype(BF16).astype(F32)
            outs = []
            for n in range(step_rows):
                slot, m = slots[n // KV_ROWS], n % KV_ROWS
                v2 = jnp.concatenate([vbuf[slot, m, 0], vbuf[slot, m, 1]], axis=1)
                o = jnp.dot(p[n * heads:(n + 1) * heads], v2, preferred_element_type=F32)
                outs.append(jnp.where(first_rows, o[:, :hd], o[:, hd:]))
            qs[r, :] = jnp.concatenate(outs, axis=0) + p_new * vn[r, :]

            for t in range(ATT_SLOTS):
                nxt = ATT_SLOTS * i + t + KV_SLOTS

                @pl.when(nxt < n_slots)
                def _():
                    start(kv_copies(l, nxt))
            return c

        lax.fori_loop(0, n_slots // ATT_SLOTS, block, 0)
        for h in range(heads):
            att[:dec, h * hd:(h + 1) * hd] = qs[pl.ds(h, dec, stride=heads), :].astype(BF16)

    def prefill_attention(l):
        wait(kv_pre_copies(l))
        old = jnp.where(lax.broadcasted_iota(jnp.int32, (1, seq), 1) < lens[dec], 0.0, -jnp.inf)
        causal = jnp.where(lax.broadcasted_iota(jnp.int32, (chunk, chunk), 1) <= lax.broadcasted_iota(jnp.int32, (chunk, chunk), 0), 0.0, -jnp.inf)
        causal = jnp.concatenate([causal] * group, axis=0)
        for g in range(kv_heads):
            q = jnp.concatenate([qp[:, (g * group + i) * hd:(g * group + i + 1) * hd] for i in range(group)], axis=0)
            kv_col = slice(g * hd, (g + 1) * hd)
            s = lax.dot_general(q, kpre[g], (((1,), (1,)), ((), ())), preferred_element_type=F32) * scale_qk + old
            t = lax.dot_general(q, kp[:, kv_col], (((1,), (1,)), ((), ())), preferred_element_type=F32) * scale_qk + causal
            top = jnp.maximum(jnp.max(s, axis=-1, keepdims=True), jnp.max(t, axis=-1, keepdims=True))
            es = jnp.exp(s - top)
            et = jnp.exp(t - top)
            inv = 1.0 / (jnp.sum(es, axis=-1, keepdims=True) + jnp.sum(et, axis=-1, keepdims=True))
            o = jnp.dot((es * inv).astype(BF16), vpre[g], preferred_element_type=F32)
            o += jnp.dot((et * inv).astype(BF16), vp[:, kv_col], preferred_element_type=F32)
            for i in range(group):
                att[dec:, (g * group + i) * hd:(g * group + i + 1) * hd] = o[i * chunk:(i + 1) * chunk].astype(BF16)

    def o_part(l, part):
        r = whole(part)

        def step(i, c):
            these = tuple(GROUP * i + t for t in range(GROUP))
            for j in these:
                if part == DEC:
                    wo_copy(l, j).wait()
                sent(l, O, part, j)
            for j in these:
                w = dbuf[j // o_per_slot, pl.ds(pl.multiple_of(lax.rem(j, o_per_slot) * o_depth, 16), o_depth), :]
                pbuf[j, r, :] = jnp.dot(att[r, :], w, preferred_element_type=F32).astype(BF16)
                p_copy(O, part, j).start()

            @pl.when(i >= 1)
            def _():
                for j in these:
                    pair_sum(O, part, j - GROUP)
            return c

        lax.fori_loop(0, n_chunks // GROUP, step, 0)

        def rest():
            for j in range(n_chunks - GROUP, n_chunks):
                pair_sum(O, part, j)

        return rest

    def gate_up(l, rest):
        def operand(r, j):
            vals = h_o[j, r, :].astype(F32)
            add_squares(r, vals)
            return (vals * pre[r, :1] * gain_m[l:l + 1, cols(j)].astype(F32)).astype(BF16)

        def release(j, m):
            nxt = j + (G_SLOTS + m) // 2

            @pl.when(nxt < n_chunks)
            def _():
                g_copy(l, nxt, (G_SLOTS + m) % 2).start()

        def first_block(part):
            r = whole(part)
            a = operand(r, 0)
            for m in range(2):
                if part == DEC:
                    g_copy(l, 0, m).wait()
                for n in range(ff // CW):
                    acc[r, m * ff + n * CW:m * ff + (n + 1) * CW] = jnp.dot(a, gbuf[m, :, n * CW:(n + 1) * CW], preferred_element_type=F32)
                if part == PRE:
                    g_copy(l, (G_SLOTS + m) // 2, (G_SLOTS + m) % 2).start()

        def block(j):
            h_wait(O, DEC, j)
            h_wait(O, PRE, j)
            a = operand(pl.ds(0, rows), j)
            for m in range(2):
                g_copy(l, j, m).wait()
                slot = lax.rem(2 * j + m, G_SLOTS)
                for n in range(ff // CW):
                    acc[:, m * ff + n * CW:m * ff + (n + 1) * CW] += jnp.dot(a, gbuf[slot, :, n * CW:(n + 1) * CW], preferred_element_type=F32)
                release(j, m)

            @pl.when(j >= n_chunks - D_SLOTS)
            def _():
                d_copy(l, j - (n_chunks - D_SLOTS)).start()

        def dec_step(j, c):
            finish(l, O, DEC, j)
            return c

        lax.fori_loop(0, GROUP, dec_step, 0)
        rest()
        lax.fori_loop(GROUP, n_chunks, dec_step, 0)
        finish(l, O, PRE, 0)
        h_wait(O, DEC, 0)
        first_block(DEC)
        finish(l, O, PRE, 1)
        h_wait(O, PRE, 0)
        first_block(PRE)

        def step(j, c):
            @pl.when(j + 1 < n_chunks)
            def _():
                finish(l, O, PRE, j + 1)

            block(j)
            return c

        lax.fori_loop(1, n_chunks, step, 0)
        scale = next_scale(pl.ds(0, rows))

        def act_step(n, c):
            gate = acc[:, cols(n)] * scale
            up = acc[:, pl.ds(pl.multiple_of(ff + n * CW, CW), CW)] * scale
            act[:, cols(n)] = (gate * jax.nn.sigmoid(gate) * up).astype(BF16)
            return c

        lax.fori_loop(0, ff // CW, act_step, 0)

    def down(l):
        def step(j, c):
            d_copy(l, j).wait()
            for part in (DEC, PRE):
                sent(l, M, part, j)
            pbuf[j] = jnp.dot(act[...], dbuf[lax.rem(j, D_SLOTS)], preferred_element_type=F32).astype(BF16)
            for part in (DEC, PRE):
                p_copy(M, part, j).start()

            @pl.when(j + D_SLOTS < n_chunks)
            def _():
                d_copy(l, j + D_SLOTS).start()

            if l + 1 < layers:
                @pl.when(j == n_chunks - D_SLOTS - 1)
                def _():
                    for n in range(n_chunks):
                        start(qkv_copies(l + 1, n))

            @pl.when(j >= 1)
            def _():
                pair_sum(M, DEC, j - 1)
            return c

        lax.fori_loop(0, n_chunks, step, 0)
        pair_sum(M, DEC, n_chunks - 1)
        if l + 1 < layers:
            start(kv_pre_copies(l + 1))
            for i in range(KV_SLOTS):
                start(kv_copies(l + 1, i))
            for j in range(n_chunks):
                wo_copy(l + 1, j).start()

        def pre_step(j, c):
            pair_sum(M, PRE, j)
            return c

        lax.fori_loop(0, n_chunks, pre_step, 0)

    for j in range(n_chunks):
        x_load(j).start()
    barrier = pltpu.get_barrier_semaphore()
    for peer in (core_peer, x_peer):
        pl.semaphore_signal(barrier, inc=1, device_id=peer, device_id_type=MESH)
    for j in range(n_chunks):
        start(qkv_copies(0, j))
    for i in range(KV_SLOTS):
        start(kv_copies(0, i))
    start(kv_pre_copies(0))
    ssq[...] = jnp.zeros_like(ssq)

    def place(b, c):
        cos[pl.ds(b, 1), :] = jnp.full((1, hd), lens[b], jnp.int32).astype(F32)
        return c

    lax.fori_loop(0, dec, place, 0)
    cos[pl.ds(dec, chunk), :] = (lax.broadcasted_iota(jnp.int32, (chunk, hd), 0) + lens[dec]).astype(F32)
    angles = cos[...] * freq[...]
    low = lax.broadcasted_iota(jnp.int32, (rows, hd), 1) < hd // 2
    sines = jnp.sin(angles)
    sin[...] = jnp.where(low, -sines, sines)
    cos[...] = jnp.cos(angles)
    for j in range(n_chunks):
        x_load(j).wait()

    def sq_step(j, c):
        add_squares(pl.ds(0, rows), h_m[j].astype(F32))
        return c

    lax.fori_loop(0, n_chunks, sq_step, 0)
    pre[...] = jnp.broadcast_to(jnp.maximum(inv_rms(pl.ds(0, rows)), 1e-30), pre.shape)
    ssq[...] = jnp.zeros_like(ssq)
    pl.semaphore_wait(barrier, 2)

    for l in range(layers):
        qkv_part(l, DEC)
        decode_attention(l)
        rest = o_part(l, DEC)
        if l > 0:
            def pre_step(j, c):
                finish(l - 1, M, PRE, j)
                return c

            lax.fori_loop(0, n_chunks, pre_step, 0)
            rest()
        qkv_part(l, PRE)
        if l == 0:
            rest()
        for i in range(G_SLOTS):
            g_copy(l, i // 2, i % 2).start()
        prefill_attention(l)
        gate_up(l, o_part(l, PRE))
        down(l)

    def out_copy(part, j):
        r = whole(part)
        return pltpu.make_async_copy(h_m.at[j, r, :], y.at[r, cols(j)], y_sem.at[part, j])

    def out_dec(j, c):
        finish(layers - 1, M, DEC, j)

        @pl.when(j >= 1)
        def _():
            h_wait(M, DEC, j - 1)
            out_copy(DEC, j - 1).start()

        h_copy(O, DEC, j).wait_send()
        h_copy(O, PRE, j).wait_send()
        p_copy(M, DEC, j).wait_send()
        p_copy(M, PRE, j).wait_send()
        return c

    lax.fori_loop(0, n_chunks, out_dec, 0)
    h_wait(M, DEC, n_chunks - 1)
    out_copy(DEC, n_chunks - 1).start()

    def out_pre(j, c):
        finish(layers - 1, M, PRE, j)
        x_copy(M, DEC, j).wait_send()
        h_copy(M, DEC, j).wait_send()

        @pl.when(j >= 1)
        def _():
            h_wait(M, PRE, j - 1)
            out_copy(PRE, j - 1).start()
            out_copy(DEC, j - 1).wait()
            x_copy(M, PRE, j - 1).wait_send()

        @pl.when(j >= 2)
        def _():
            h_copy(M, PRE, j - 2).wait_send()
            out_copy(PRE, j - 2).wait()
        return c

    lax.fori_loop(0, n_chunks, out_pre, 0)
    last = n_chunks - 1
    h_wait(M, PRE, last)
    out_copy(PRE, last).start()
    x_copy(M, PRE, last).wait_send()
    out_copy(DEC, last).wait()
    for j in (last - 1, last):
        h_copy(M, PRE, j).wait_send()
        out_copy(PRE, j).wait()


def step_call(lengths, x, freq, attn_gain, mlp_gain, w_q, w_k, w_v, w_o, w_gate, w_up, w_down, k_cache, v_cache):
    rows, width = x.shape
    dec = lengths.shape[0] - 1
    chunk = rows - dec
    ff = w_gate.shape[2]
    n_chunks = width // CW
    q_cols, k_cols = w_q.shape[2], w_k.shape[2]
    kv_heads, seq, hd = k_cache.shape[2:]
    heads = q_cols // hd
    vmem = pl.BlockSpec(memory_space=pltpu.VMEM)
    hbm = pl.BlockSpec(memory_space=pl.ANY)
    smem = pl.BlockSpec(memory_space=pltpu.SMEM)
    sem = pltpu.SemaphoreType.DMA
    buf = pltpu.VMEM
    return pl.pallas_call(
        functools.partial(step_kernel, (dec, chunk)),
        out_shape=jax.ShapeDtypeStruct((rows, width), BF16),
        in_specs=[smem, hbm, vmem, vmem, vmem] + [hbm] * 9,
        out_specs=hbm,
        scratch_shapes=[
            buf((G_SLOTS, CW, ff), BF16),
            buf((D_SLOTS, ff, CW), BF16),
            buf((rows, 2 * ff), F32),
            buf((rows, ff), BF16),
            buf((n_chunks, rows, CW), BF16),
            buf((n_chunks, rows // 2, CW), BF16),
            buf((n_chunks, rows // 2, CW), BF16),
            buf((n_chunks, rows // 2, CW), BF16),
            buf((n_chunks, rows, CW), BF16),
            buf((n_chunks, rows, CW), BF16),
            buf((rows, 128), F32),
            buf((rows, 128), F32),
            buf((rows, hd), F32),
            buf((rows, hd), F32),
            buf((KV_SLOTS, KV_ROWS, kv_heads, seq, hd), BF16),
            buf((KV_SLOTS, KV_ROWS, kv_heads, seq, hd), BF16),
            buf((kv_heads, seq, hd), BF16),
            buf((kv_heads, seq, hd), BF16),
            buf((dec * heads, hd), F32),
            buf((dec * heads, hd), F32),
            buf((dec * heads, hd), F32),
            buf((chunk, q_cols), BF16),
            buf((chunk, k_cols), BF16),
            buf((chunk, k_cols), BF16),
            buf((rows, q_cols), BF16),
            sem((n_chunks,)),
            sem((n_chunks,)),
            sem((n_chunks,)),
            sem((n_chunks,)),
            sem((G_SLOTS,)),
            sem((D_SLOTS,)),
            sem((KV_SLOTS, 2)),
            sem((2,)),
            sem((2, n_chunks)),
            sem((2, 2, n_chunks)),
            sem((2, 2, n_chunks)),
            sem((2, 2, n_chunks)),
            sem((2, 2, n_chunks)),
            sem((2, 2, n_chunks)),
            sem((2, 2, n_chunks)),
        ],
        compiler_params=pltpu.CompilerParams(collective_id=0, has_side_effects=True, vmem_limit_bytes=67043328),
        name='decoder_step',
    )(lengths, x, freq, attn_gain, mlp_gain, w_q, w_k, w_v, w_o, w_gate, w_up, w_down, k_cache, v_cache)


def solution(mesh):
    col_spec = P(None, None, 'tp')
    row_spec = P(None, 'tp', None)
    cache_spec = P(None, 'dp', 'tp', None, None)
    in_specs = (P('dp', None), P('dp'), P(), col_spec, col_spec, col_spec, row_spec, P(), col_spec, col_spec, row_spec, cache_spec, cache_spec)

    def body(x, lengths, attn_gain, w_q, w_k, w_v, w_o, mlp_gain, w_gate, w_up, w_down, k_cache, v_cache):
        head_dim = k_cache.shape[-1]
        exps = np.arange(0, head_dim, 2, dtype=np.float32) / np.float32(head_dim)
        freq = np.power(np.float32(ROPE_BASE), -exps).astype(np.float32)
        freq = jnp.asarray(np.concatenate([freq, freq])[None])
        return step_call(lengths, x, freq, attn_gain, mlp_gain, w_q, w_k, w_v, w_o, w_gate, w_up, w_down, k_cache, v_cache)

    return jax.shard_map(body, mesh=mesh, in_specs=in_specs, out_specs=P('dp', None), check_vma=False)
```

```python
import functools

import jax
import jax.numpy as jnp
import numpy as np
from jax import lax
from jax.experimental import pallas as pl
from jax.experimental.pallas import tpu as pltpu
from jax.sharding import PartitionSpec as P

ROPE_BASE = 500000.0
EPSILON = 1e-5
MESH = pl.DeviceIdType.MESH
F32 = jnp.float32
BF16 = jnp.bfloat16
CW = 512
G_SLOTS = 5
D_SLOTS = 4
KV_SLOTS = 5
KV_ROWS = 8
ATT_SLOTS = 2
AHEAD = 7
GROUP = 5
O, M = 0, 1
DEC, PRE = 0, 1


def step_kernel(dims, lens, x_in, freq, gain_a, gain_m, wq, wk, wv, wo, wg, wu, wd, kc, vc, y,
                gbuf, dbuf, acc, act, pbuf, rbuf, xb_o, xb_m, h_o, h_m, ssq, pre, cos, sin, kbuf, vbuf, kpre, vpre,
                qs, kn, vn, qp, kp, vp, att,
                q_sem, w_sem, g_sem, d_sem, kv_sem, io_sem, p_ss, p_rs, x_ss, x_rs, h_ss, h_rs):
    dec, chunk = dims
    rows = dec + chunk
    width = x_in.shape[1]
    layers, o_depth = wo.shape[0], wo.shape[1]
    ff = wg.shape[2]
    q_cols, k_cols = wq.shape[2], wk.shape[2]
    n_qkv = q_cols + 2 * k_cols
    seq, hd = kc.shape[3], kc.shape[4]
    heads, kv_heads = q_cols // hd, k_cols // hd
    group = heads // kv_heads
    n_chunks = width // CW
    o_per_slot = ff // o_depth
    scale_qk = hd ** -0.5
    base = (0, dec)
    size = (dec, chunk)
    half = (dec // 2, chunk // 2)
    rbase = (0, dec // 2)

    dp_me = lax.axis_index('dp')
    me = lax.axis_index('tp')
    core = lax.rem(me, 2)
    core_peer = (dp_me, me + 1 - 2 * core)
    x_peer = (dp_me, lax.rem(me + 2, 4))

    def own(part):
        return pl.ds(pl.multiple_of(base[part] + core * half[part], 16), half[part])

    def oth(part):
        return pl.ds(pl.multiple_of(base[part] + (1 - core) * half[part], 16), half[part])

    def whole(part):
        return pl.ds(base[part], size[part])

    def landed(part):
        return pl.ds(rbase[part], half[part])

    def cols(j):
        return pl.ds(pl.multiple_of(j * CW, CW), CW)

    xbs = (xb_o, xb_m)
    hs = (h_o, h_m)

    def x_load(j):
        return pltpu.make_async_copy(x_in.at[:, cols(j)], h_m.at[j], io_sem.at[0])

    def wo_copy(l, j):
        return pltpu.make_async_copy(wo.at[l, :, cols(j)], dbuf.at[j // o_per_slot, pl.ds(pl.multiple_of(lax.rem(j, o_per_slot) * o_depth, 16), o_depth), :], w_sem.at[j])

    def g_copy(l, j, m):
        slot = lax.rem(2 * j + m, G_SLOTS)
        return pltpu.make_async_copy((wg, wu)[m].at[l, cols(j), :], gbuf.at[slot], g_sem.at[slot])

    def d_copy(l, j):
        slot = lax.rem(j, D_SLOTS)
        return pltpu.make_async_copy(wd.at[l, :, cols(j)], dbuf.at[slot], d_sem.at[slot])

    def qkv_place(j):
        return j // 2, lax.rem(j, 2) * (ff // 2)

    def qkv_copies(l, j):
        slot, left = qkv_place(j)
        dst = gbuf.at[slot]

        def at(off, n):
            return dst.at[:, pl.ds(pl.multiple_of(left + off, 128), n)]

        return (pltpu.make_async_copy(wq.at[l, cols(j), :], at(0, q_cols), q_sem.at[j]),
                pltpu.make_async_copy(wk.at[l, cols(j), :], at(q_cols, k_cols), q_sem.at[j]),
                pltpu.make_async_copy(wv.at[l, cols(j), :], at(q_cols + k_cols, k_cols), q_sem.at[j]))

    def qkv_wait(j):
        slot, left = qkv_place(j)
        dst = gbuf.at[slot, :, pl.ds(pl.multiple_of(left, 128), n_qkv)]
        pltpu.make_async_copy(dst, dst, q_sem.at[j]).wait()

    def kv_copies(l, i):
        slot = lax.rem(i, KV_SLOTS)
        src = pl.ds(i * KV_ROWS, KV_ROWS)
        return (pltpu.make_async_copy(kc.at[l, src], kbuf.at[slot], kv_sem.at[slot, 0]),
                pltpu.make_async_copy(vc.at[l, src], vbuf.at[slot], kv_sem.at[slot, 1]))

    def kv_pre_copies(l):
        return (pltpu.make_async_copy(kc.at[l, dec], kpre, io_sem.at[1]),
                pltpu.make_async_copy(vc.at[l, dec], vpre, io_sem.at[2]))

    def start(copies):
        for c in copies:
            c.start()

    def wait(copies):
        for c in copies:
            c.wait()

    def p_copy(ar, part, j):
        return pltpu.make_async_remote_copy(pbuf.at[j, oth(part), :], rbuf.at[j, landed(part), :], p_ss.at[part, j], p_rs.at[part, j], device_id=core_peer, device_id_type=MESH)

    def x_copy(ar, part, j):
        return pltpu.make_async_remote_copy(pbuf.at[j, own(part), :], xbs[ar].at[j, landed(part), :], x_ss.at[part, j], x_rs.at[ar, part, j], device_id=x_peer, device_id_type=MESH)

    def h_copy(ar, part, j):
        return pltpu.make_async_remote_copy(hs[ar].at[j, own(part), :], hs[ar].at[j, own(part), :], h_ss.at[part, j], h_rs.at[part, j], device_id=core_peer, device_id_type=MESH)

    def h_wait(ar, part, j):
        pltpu.make_async_remote_copy(hs[ar].at[j, oth(part), :], hs[ar].at[j, oth(part), :], h_ss.at[part, j], h_rs.at[part, j], device_id=core_peer, device_id_type=MESH).wait_recv()

    def sent(l, ar, part, j):
        if l > 0 or ar == M:
            p_copy(1 - ar, part, j).wait_send()
            x_copy(1 - ar, part, j).wait_send()

    def pair_sum(ar, part, j):
        p_copy(ar, part, j).wait_recv()
        pbuf[j, own(part), :] = (pbuf[j, own(part), :].astype(F32) + rbuf[j, landed(part), :].astype(F32)).astype(BF16)
        x_copy(ar, part, j).start()

    def finish(l, ar, part, j):
        x_copy(ar, part, j).wait_recv()
        total = pbuf[j, own(part), :].astype(F32) + xbs[ar][j, landed(part), :].astype(F32)
        resid = hs[1 - ar][j, own(part), :].astype(F32)
        if l > 0 or ar == M:
            h_copy(1 - ar, part, j).wait_send()
        hs[ar][j, own(part), :] = (resid + total).astype(BF16)
        h_copy(ar, part, j).start()

    def add_squares(r, vals):
        sq = vals * vals
        ssq[r, :] += sq[:, :128] + sq[:, 128:256] + sq[:, 256:384] + sq[:, 384:]

    def inv_rms(r):
        return lax.rsqrt(jnp.sum(ssq[r, :], axis=-1, keepdims=True) * (1.0 / width) + EPSILON)

    def next_scale(r):
        inv = inv_rms(r)
        scale = inv / pre[r, :1]
        n = ssq[r, :].shape[0]
        pre[r, :] = jnp.broadcast_to(jnp.maximum(inv, 1e-30), (n, 128))
        ssq[r, :] = jnp.zeros((n, 128), F32)
        return scale

    def qkv_block(l, part, pair):
        r = whole(part)
        a = []
        for j in pair:
            if l > 0:
                h_wait(M, part, j)
            vals = h_m[j, r, :].astype(F32)
            add_squares(r, vals)
            a.append((vals * pre[r, :1] * gain_a[l:l + 1, cols(j)].astype(F32)).astype(BF16))
            if part == DEC:
                qkv_wait(j)
        for n in range(n_qkv // CW):
            total = acc[r, n * CW:(n + 1) * CW]
            for j, a_j in zip(pair, a):
                slot, left = qkv_place(j)
                total += jnp.dot(a_j, gbuf[slot, :, pl.ds(pl.multiple_of(left + n * CW, 128), CW)], preferred_element_type=F32)
            acc[r, n * CW:(n + 1) * CW] = total

    def qkv_part(l, part):
        r = whole(part)
        acc[r, :n_qkv] = jnp.zeros((size[part], n_qkv), F32)
        n = GROUP if part == PRE else 2
        steps = n_chunks // n
        arriving = l > 0 and part == DEC

        def chunks_of(i):
            return tuple(n * i + t for t in range(n))

        def step(i, c):
            if arriving:
                for j in chunks_of(i):
                    finish(l - 1, M, part, j)

                @pl.when(i >= 1)
                def _():
                    qkv_block(l, part, chunks_of(i - 1))
            else:
                qkv_block(l, part, chunks_of(i))
            return c

        lax.fori_loop(0, steps, step, 0)
        if arriving:
            qkv_block(l, part, chunks_of(steps - 1))
        scale = next_scale(r)
        c_tab, s_tab = cos[r, :], sin[r, :]

        def head(col):
            return (acc[r, col * hd:(col + 1) * hd] * scale).astype(BF16).astype(F32)

        def rope(t):
            return (t * c_tab + pltpu.roll(t, hd // 2, 1) * s_tab).astype(BF16)

        for h in range(heads):
            q = rope(head(h))
            if part == DEC:
                qs[pl.ds(h, dec, stride=heads), :] = q.astype(F32)
            else:
                qp[:, h * hd:(h + 1) * hd] = q
        for g in range(kv_heads):
            k = rope(head(heads + g))
            v = head(heads + kv_heads + g)
            if part == DEC:
                for h in range(g * group, (g + 1) * group):
                    kn[pl.ds(h, dec, stride=heads), :] = k.astype(F32)
                    vn[pl.ds(h, dec, stride=heads), :] = v
            else:
                kp[:, g * hd:(g + 1) * hd] = k
                vp[:, g * hd:(g + 1) * hd] = v.astype(BF16)

    def decode_attention(l):
        first_rows = lax.broadcasted_iota(jnp.int32, (heads, hd), 0) < group
        places = lax.broadcasted_iota(jnp.int32, (heads, seq), 1)
        n_slots = dec // KV_ROWS
        step_rows = ATT_SLOTS * KV_ROWS

        def block(i, c):
            slots = []
            for t in range(ATT_SLOTS):
                wait(kv_copies(l, ATT_SLOTS * i + t))
                slots.append(lax.rem(ATT_SLOTS * i + t, KV_SLOTS))
            if l == 0:
                @pl.when(i == 2)
                def _():
                    for j in range(n_chunks):
                        wo_copy(l, j).start()
            scores = []
            for n in range(step_rows):
                b = i * step_rows + n
                slot, m = slots[n // KV_ROWS], n % KV_ROWS
                q = qs[pl.ds(pl.multiple_of(b * heads, heads), heads), :]
                zero = jnp.zeros_like(q)
                q2 = jnp.concatenate([jnp.where(first_rows, q, zero), jnp.where(first_rows, zero, q)], axis=1).astype(BF16)
                k2 = jnp.concatenate([kbuf[slot, m, 0], kbuf[slot, m, 1]], axis=1)
                s = lax.dot_general(q2, k2, (((1,), (1,)), ((), ())), preferred_element_type=F32) * scale_qk
                scores.append(jnp.where(places < lens[b], s, -jnp.inf))
            r = pl.ds(pl.multiple_of(i * step_rows * heads, step_rows * heads), step_rows * heads)
            s = jnp.concatenate(scores, axis=0)
            s_new = jnp.sum(qs[r, :] * kn[r, :], axis=-1, keepdims=True) * scale_qk
            top = jnp.maximum(jnp.max(s, axis=-1, keepdims=True), s_new)
            e = jnp.exp(s - top)
            e_new = jnp.exp(s_new - top)
            inv = 1.0 / (jnp.sum(e, axis=-1, keepdims=True) + e_new)
            p = (e * inv).astype(BF16)
            p_new = (e_new * inv).astype(BF16).astype(F32)
            outs = []
            for n in range(step_rows):
                slot, m = slots[n // KV_ROWS], n % KV_ROWS
                v2 = jnp.concatenate([vbuf[slot, m, 0], vbuf[slot, m, 1]], axis=1)
                o = jnp.dot(p[n * heads:(n + 1) * heads], v2, preferred_element_type=F32)
                outs.append(jnp.where(first_rows, o[:, :hd], o[:, hd:]))
            qs[r, :] = jnp.concatenate(outs, axis=0) + p_new * vn[r, :]

            for t in range(ATT_SLOTS):
                nxt = ATT_SLOTS * i + t + KV_SLOTS

                @pl.when(nxt < n_slots)
                def _():
                    start(kv_copies(l, nxt))
            return c

        lax.fori_loop(0, n_slots // ATT_SLOTS, block, 0)
        for h in range(heads):
            att[:dec, h * hd:(h + 1) * hd] = qs[pl.ds(h, dec, stride=heads), :].astype(BF16)

    def prefill_attention(l):
        wait(kv_pre_copies(l))
        old = jnp.where(lax.broadcasted_iota(jnp.int32, (1, seq), 1) < lens[dec], 0.0, -jnp.inf)
        causal = jnp.where(lax.broadcasted_iota(jnp.int32, (chunk, chunk), 1) <= lax.broadcasted_iota(jnp.int32, (chunk, chunk), 0), 0.0, -jnp.inf)
        causal = jnp.concatenate([causal] * group, axis=0)
        for g in range(kv_heads):
            q = jnp.concatenate([qp[:, (g * group + i) * hd:(g * group + i + 1) * hd] for i in range(group)], axis=0)
            kv_col = slice(g * hd, (g + 1) * hd)
            s = lax.dot_general(q, kpre[g], (((1,), (1,)), ((), ())), preferred_element_type=F32) * scale_qk + old
            t = lax.dot_general(q, kp[:, kv_col], (((1,), (1,)), ((), ())), preferred_element_type=F32) * scale_qk + causal
            top = jnp.maximum(jnp.max(s, axis=-1, keepdims=True), jnp.max(t, axis=-1, keepdims=True))
            es = jnp.exp(s - top)
            et = jnp.exp(t - top)
            inv = 1.0 / (jnp.sum(es, axis=-1, keepdims=True) + jnp.sum(et, axis=-1, keepdims=True))
            o = jnp.dot((es * inv).astype(BF16), vpre[g], preferred_element_type=F32)
            o += jnp.dot((et * inv).astype(BF16), vp[:, kv_col], preferred_element_type=F32)
            for i in range(group):
                att[dec:, (g * group + i) * hd:(g * group + i + 1) * hd] = o[i * chunk:(i + 1) * chunk].astype(BF16)

    def o_part(l, part):
        r = whole(part)

        def step(i, c):
            these = tuple(GROUP * i + t for t in range(GROUP))
            for j in these:
                if part == DEC:
                    wo_copy(l, j).wait()
                sent(l, O, part, j)
            for j in these:
                w = dbuf[j // o_per_slot, pl.ds(pl.multiple_of(lax.rem(j, o_per_slot) * o_depth, 16), o_depth), :]
                pbuf[j, r, :] = jnp.dot(att[r, :], w, preferred_element_type=F32).astype(BF16)
            for j in these:
                p_copy(O, part, j).start()

            @pl.when(i >= 1)
            def _():
                for j in these:
                    pair_sum(O, part, j - GROUP)
            return c

        lax.fori_loop(0, n_chunks // GROUP, step, 0)

    def gate_up(l):
        def operand(r, j):
            vals = h_o[j, r, :].astype(F32)
            add_squares(r, vals)
            return (vals * pre[r, :1] * gain_m[l:l + 1, cols(j)].astype(F32)).astype(BF16)

        def release(j, m):
            nxt = j + (G_SLOTS + m) // 2

            @pl.when(nxt < n_chunks)
            def _():
                g_copy(l, nxt, (G_SLOTS + m) % 2).start()

        def first_block(part):
            r = whole(part)
            a = operand(r, 0)
            for m in range(2):
                if part == DEC:
                    g_copy(l, 0, m).wait()
                for n in range(ff // CW):
                    acc[r, m * ff + n * CW:m * ff + (n + 1) * CW] = jnp.dot(a, gbuf[m, :, n * CW:(n + 1) * CW], preferred_element_type=F32)
                if part == PRE:
                    g_copy(l, (G_SLOTS + m) // 2, (G_SLOTS + m) % 2).start()

        def block(j):
            h_wait(O, DEC, j)
            h_wait(O, PRE, j)
            a = operand(pl.ds(0, rows), j)
            for m in range(2):
                g_copy(l, j, m).wait()
                slot = lax.rem(2 * j + m, G_SLOTS)
                for n in range(ff // CW):
                    acc[:, m * ff + n * CW:m * ff + (n + 1) * CW] += jnp.dot(a, gbuf[slot, :, n * CW:(n + 1) * CW], preferred_element_type=F32)
                release(j, m)

            @pl.when(j >= n_chunks - D_SLOTS)
            def _():
                d_copy(l, j - (n_chunks - D_SLOTS)).start()

        def dec_step(j, c):
            finish(l, O, DEC, j)
            return c

        lax.fori_loop(0, GROUP, dec_step, 0)
        for j in range(GROUP, n_chunks):
            if j >= AHEAD:
                pair_sum(O, DEC, j)
            pair_sum(O, PRE, j)
        lax.fori_loop(GROUP, AHEAD, dec_step, 0)
        finish(l, O, PRE, 0)
        h_wait(O, DEC, 0)
        first_block(DEC)
        finish(l, O, PRE, 1)
        h_wait(O, PRE, 0)
        first_block(PRE)

        def step(j, c):
            @pl.when(j + 1 < n_chunks)
            def _():
                @pl.when(j + 1 >= AHEAD)
                def _():
                    finish(l, O, DEC, j + 1)

                finish(l, O, PRE, j + 1)

            block(j)
            return c

        lax.fori_loop(1, n_chunks, step, 0)
        scale = next_scale(pl.ds(0, rows))

        def act_step(n, c):
            gate = acc[:, cols(n)] * scale
            up = acc[:, pl.ds(pl.multiple_of(ff + n * CW, CW), CW)] * scale
            act[:, cols(n)] = (gate * jax.nn.sigmoid(gate) * up).astype(BF16)
            return c

        lax.fori_loop(0, ff // CW, act_step, 0)

    def down(l):
        def step(j, c):
            d_copy(l, j).wait()
            for part in (DEC, PRE):
                sent(l, M, part, j)
            pbuf[j] = jnp.dot(act[...], dbuf[lax.rem(j, D_SLOTS)], preferred_element_type=F32).astype(BF16)
            for part in (DEC, PRE):
                p_copy(M, part, j).start()

            @pl.when(j + D_SLOTS < n_chunks)
            def _():
                d_copy(l, j + D_SLOTS).start()

            if l + 1 < layers:
                for n in range(3):
                    nxt = 3 * (j - (n_chunks - D_SLOTS)) + n

                    @pl.when((nxt >= 0) & (nxt < n_chunks))
                    def _():
                        start(qkv_copies(l + 1, nxt))

            @pl.when(j >= 1)
            def _():
                pair_sum(M, DEC, j - 1)
            return c

        lax.fori_loop(0, n_chunks, step, 0)
        pair_sum(M, DEC, n_chunks - 1)
        if l + 1 < layers:
            start(kv_pre_copies(l + 1))
            for i in range(KV_SLOTS):
                start(kv_copies(l + 1, i))
            for j in range(n_chunks):
                wo_copy(l + 1, j).start()

        def pre_step(j, c):
            pair_sum(M, PRE, j)
            return c

        lax.fori_loop(0, n_chunks, pre_step, 0)

    for j in range(n_chunks):
        x_load(j).start()
    barrier = pltpu.get_barrier_semaphore()
    for peer in (core_peer, x_peer):
        pl.semaphore_signal(barrier, inc=1, device_id=peer, device_id_type=MESH)
    for j in range(n_chunks):
        start(qkv_copies(0, j))
    for i in range(KV_SLOTS):
        start(kv_copies(0, i))
    start(kv_pre_copies(0))
    ssq[...] = jnp.zeros_like(ssq)

    def place(b, c):
        cos[pl.ds(b, 1), :] = jnp.full((1, hd), lens[b], jnp.int32).astype(F32)
        return c

    lax.fori_loop(0, dec, place, 0)
    cos[pl.ds(dec, chunk), :] = (lax.broadcasted_iota(jnp.int32, (chunk, hd), 0) + lens[dec]).astype(F32)
    angles = cos[...] * freq[...]
    low = lax.broadcasted_iota(jnp.int32, (rows, hd), 1) < hd // 2
    sines = jnp.sin(angles)
    sin[...] = jnp.where(low, -sines, sines)
    cos[...] = jnp.cos(angles)
    pltpu.make_async_copy(h_m, h_m, io_sem.at[0]).wait()

    def sq_step(j, c):
        add_squares(pl.ds(0, rows), h_m[j].astype(F32))
        return c

    lax.fori_loop(0, n_chunks, sq_step, 0)
    pre[...] = jnp.broadcast_to(jnp.maximum(inv_rms(pl.ds(0, rows)), 1e-30), pre.shape)
    ssq[...] = jnp.zeros_like(ssq)
    pl.semaphore_wait(barrier, 2)

    for l in range(layers):
        qkv_part(l, DEC)
        decode_attention(l)
        o_part(l, DEC)
        if l > 0:
            def pre_step(j, c):
                finish(l - 1, M, PRE, j)
                return c

            lax.fori_loop(0, n_chunks, pre_step, 0)
            for j in range(GROUP, AHEAD):
                pair_sum(O, DEC, j)
        qkv_part(l, PRE)
        if l == 0:
            for j in range(GROUP, AHEAD):
                pair_sum(O, DEC, j)
        for i in range(G_SLOTS):
            g_copy(l, i // 2, i % 2).start()
        prefill_attention(l)
        o_part(l, PRE)
        gate_up(l)
        down(l)

    def out_copy(part, j):
        r = whole(part)
        return pltpu.make_async_copy(h_m.at[j, r, :], y.at[r, cols(j)], io_sem.at[3 + part])

    def out_dec(j, c):
        finish(layers - 1, M, DEC, j)

        @pl.when(j >= 1)
        def _():
            h_wait(M, DEC, j - 1)
            out_copy(DEC, j - 1).start()

        p_copy(M, DEC, j).wait_send()
        p_copy(M, PRE, j).wait_send()
        return c

    lax.fori_loop(0, n_chunks, out_dec, 0)
    h_wait(M, DEC, n_chunks - 1)
    out_copy(DEC, n_chunks - 1).start()

    def out_pre(j, c):
        finish(layers - 1, M, PRE, j)
        x_copy(M, DEC, j).wait_send()
        h_copy(M, DEC, j).wait_send()

        @pl.when(j >= 1)
        def _():
            h_wait(M, PRE, j - 1)
            out_copy(PRE, j - 1).start()
            x_copy(M, PRE, j - 1).wait_send()

        @pl.when(j >= 2)
        def _():
            h_copy(M, PRE, j - 2).wait_send()
        return c

    lax.fori_loop(0, n_chunks, out_pre, 0)
    last = n_chunks - 1
    h_wait(M, PRE, last)
    out_copy(PRE, last).start()
    x_copy(M, PRE, last).wait_send()
    for j in (last - 1, last):
        h_copy(M, PRE, j).wait_send()
    for part in (DEC, PRE):
        done = h_m.at[:, whole(part), :]
        pltpu.make_async_copy(done, done, io_sem.at[3 + part]).wait()


def step_call(lengths, x, freq, attn_gain, mlp_gain, w_q, w_k, w_v, w_o, w_gate, w_up, w_down, k_cache, v_cache):
    rows, width = x.shape
    dec = lengths.shape[0] - 1
    chunk = rows - dec
    ff = w_gate.shape[2]
    n_chunks = width // CW
    q_cols, k_cols = w_q.shape[2], w_k.shape[2]
    kv_heads, seq, hd = k_cache.shape[2:]
    heads = q_cols // hd
    vmem = pl.BlockSpec(memory_space=pltpu.VMEM)
    hbm = pl.BlockSpec(memory_space=pl.ANY)
    smem = pl.BlockSpec(memory_space=pltpu.SMEM)
    sem = pltpu.SemaphoreType.DMA
    buf = pltpu.VMEM
    return pl.pallas_call(
        functools.partial(step_kernel, (dec, chunk)),
        out_shape=jax.ShapeDtypeStruct((rows, width), BF16),
        in_specs=[smem, hbm, vmem, vmem, vmem] + [hbm] * 9,
        out_specs=hbm,
        scratch_shapes=[
            buf((G_SLOTS, CW, ff), BF16),
            buf((D_SLOTS, ff, CW), BF16),
            buf((rows, 2 * ff), F32),
            buf((rows, ff), BF16),
            buf((n_chunks, rows, CW), BF16),
            buf((n_chunks, rows // 2, CW), BF16),
            buf((n_chunks, rows // 2, CW), BF16),
            buf((n_chunks, rows // 2, CW), BF16),
            buf((n_chunks, rows, CW), BF16),
            buf((n_chunks, rows, CW), BF16),
            buf((rows, 128), F32),
            buf((rows, 128), F32),
            buf((rows, hd), F32),
            buf((rows, hd), F32),
            buf((KV_SLOTS, KV_ROWS, kv_heads, seq, hd), BF16),
            buf((KV_SLOTS, KV_ROWS, kv_heads, seq, hd), BF16),
            buf((kv_heads, seq, hd), BF16),
            buf((kv_heads, seq, hd), BF16),
            buf((dec * heads, hd), F32),
            buf((dec * heads, hd), F32),
            buf((dec * heads, hd), F32),
            buf((chunk, q_cols), BF16),
            buf((chunk, k_cols), BF16),
            buf((chunk, k_cols), BF16),
            buf((rows, q_cols), BF16),
            sem((n_chunks,)),
            sem((n_chunks,)),
            sem((G_SLOTS,)),
            sem((D_SLOTS,)),
            sem((KV_SLOTS, 2)),
            sem((5,)),
            sem((2, n_chunks)),
            sem((2, n_chunks)),
            sem((2, n_chunks)),
            sem((2, 2, n_chunks)),
            sem((2, n_chunks)),
            sem((2, n_chunks)),
        ],
        compiler_params=pltpu.CompilerParams(collective_id=0, has_side_effects=True, vmem_limit_bytes=67043328),
        name='decoder_step',
    )(lengths, x, freq, attn_gain, mlp_gain, w_q, w_k, w_v, w_o, w_gate, w_up, w_down, k_cache, v_cache)


def solution(mesh):
    col_spec = P(None, None, 'tp')
    row_spec = P(None, 'tp', None)
    cache_spec = P(None, 'dp', 'tp', None, None)
    in_specs = (P('dp', None), P('dp'), P(), col_spec, col_spec, col_spec, row_spec, P(), col_spec, col_spec, row_spec, cache_spec, cache_spec)

    def body(x, lengths, attn_gain, w_q, w_k, w_v, w_o, mlp_gain, w_gate, w_up, w_down, k_cache, v_cache):
        head_dim = k_cache.shape[-1]
        exps = np.arange(0, head_dim, 2, dtype=np.float32) / np.float32(head_dim)
        freq = np.power(np.float32(ROPE_BASE), -exps).astype(np.float32)
        freq = jnp.asarray(np.concatenate([freq, freq])[None])
        return step_call(lengths, x, freq, attn_gain, mlp_gain, w_q, w_k, w_v, w_o, w_gate, w_up, w_down, k_cache, v_cache)

    return jax.shard_map(body, mesh=mesh, in_specs=in_specs, out_specs=P('dp', None), check_vma=False)
```

```python
import functools

import jax
import jax.numpy as jnp
import numpy as np
from jax import lax
from jax.experimental import pallas as pl
from jax.experimental.pallas import tpu as pltpu
from jax.sharding import PartitionSpec as P

ROPE_BASE = 500000.0
EPSILON = 1e-5
MESH = pl.DeviceIdType.MESH
F32 = jnp.float32
BF16 = jnp.bfloat16
CW = 512
G_SLOTS = 5
D_SLOTS = 4
KV_SLOTS = 5
KV_ROWS = 8
ATT_SLOTS = 2
AHEAD = 7
STACK = 4
GROUP = 5
O, M = 0, 1
DEC, PRE = 0, 1


def step_kernel(dims, lens, x_in, freq, gain_a, gain_m, wq, wk, wv, wo, wg, wu, wd, kc, vc, y,
                gbuf, dbuf, abuf, acc, act, pbuf, rbuf, xb_o, xb_m, h_o, h_m, ssq, pre, cos, sin, kbuf, vbuf, kpre, vpre,
                qs, kn, vn,
                q_sem, w_sem, g_sem, d_sem, kv_sem, io_sem, p_ss, p_rs, x_ss, x_rs, h_ss, h_rs):
    dec, chunk = dims
    rows = dec + chunk
    width = x_in.shape[1]
    layers, o_depth = wo.shape[0], wo.shape[1]
    ff = wg.shape[2]
    q_cols, k_cols = wq.shape[2], wk.shape[2]
    n_qkv = q_cols + 2 * k_cols
    seq, hd = kc.shape[3], kc.shape[4]
    heads, kv_heads = q_cols // hd, k_cols // hd
    group = heads // kv_heads
    n_chunks = width // CW
    o_per_slot = ff // o_depth
    scale_qk = hd ** -0.5
    base = (0, dec)
    size = (dec, chunk)
    half = (dec // 2, chunk // 2)
    rbase = (0, dec // 2)

    dp_me = lax.axis_index('dp')
    me = lax.axis_index('tp')
    core = lax.rem(me, 2)
    core_peer = (dp_me, me + 1 - 2 * core)
    x_peer = (dp_me, lax.rem(me + 2, 4))

    def own(part):
        return pl.ds(pl.multiple_of(base[part] + core * half[part], 16), half[part])

    def oth(part):
        return pl.ds(pl.multiple_of(base[part] + (1 - core) * half[part], 16), half[part])

    def whole(part):
        return pl.ds(base[part], size[part])

    def landed(part):
        return pl.ds(rbase[part], half[part])

    def cols(j):
        return pl.ds(pl.multiple_of(j * CW, CW), CW)

    att = act.at[:, pl.ds(0, q_cols)]
    kp = act.at[pl.ds(0, chunk), pl.ds(q_cols, k_cols)]
    vp = act.at[pl.ds(0, chunk), pl.ds(q_cols + k_cols, k_cols)]

    xbs = (xb_o, xb_m)
    hs = (h_o, h_m)

    def x_load(j):
        return pltpu.make_async_copy(x_in.at[:, cols(j)], h_m.at[j], io_sem.at[0])

    def wo_copy(l, j):
        return pltpu.make_async_copy(wo.at[l, :, cols(j)], dbuf.at[j // o_per_slot, pl.ds(pl.multiple_of(lax.rem(j, o_per_slot) * o_depth, 16), o_depth), :], w_sem.at[j])

    def g_copy(l, j, m):
        slot = lax.rem(2 * j + m, G_SLOTS)
        return pltpu.make_async_copy((wg, wu)[m].at[l, cols(j), :], gbuf.at[slot], g_sem.at[slot])

    def d_copy(l, j):
        slot = lax.rem(j, D_SLOTS)
        return pltpu.make_async_copy(wd.at[l, :, cols(j)], dbuf.at[slot], d_sem.at[slot])

    def qkv_place(j):
        return j // 2, (j % 2) * (ff // 2)

    def qkv_copies(l, j):
        slot, left = qkv_place(j)
        dst = gbuf.at[slot]

        def at(off, n):
            return dst.at[:, pl.ds(pl.multiple_of(left + off, 128), n)]

        return (pltpu.make_async_copy(wq.at[l, cols(j), :], at(0, q_cols), q_sem.at[j]),
                pltpu.make_async_copy(wk.at[l, cols(j), :], at(q_cols, k_cols), q_sem.at[j]),
                pltpu.make_async_copy(wv.at[l, cols(j), :], at(q_cols + k_cols, k_cols), q_sem.at[j]))

    def qkv_wait(j):
        slot, left = qkv_place(j)
        dst = gbuf.at[slot, :, pl.ds(pl.multiple_of(left, 128), n_qkv)]
        pltpu.make_async_copy(dst, dst, q_sem.at[j]).wait()

    def kv_copies(l, i):
        slot = lax.rem(i, KV_SLOTS)
        src = pl.ds(i * KV_ROWS, KV_ROWS)
        return (pltpu.make_async_copy(kc.at[l, src], kbuf.at[slot], kv_sem.at[slot, 0]),
                pltpu.make_async_copy(vc.at[l, src], vbuf.at[slot], kv_sem.at[slot, 1]))

    def kv_pre_copies(l):
        return (pltpu.make_async_copy(kc.at[l, dec], kpre, io_sem.at[1]),
                pltpu.make_async_copy(vc.at[l, dec], vpre, io_sem.at[2]))

    def start(copies):
        for c in copies:
            c.start()

    def wait(copies):
        for c in copies:
            c.wait()

    def p_copy(ar, part, j):
        return pltpu.make_async_remote_copy(pbuf.at[j, oth(part), :], rbuf.at[j, landed(part), :], p_ss.at[part, j], p_rs.at[part, j], device_id=core_peer, device_id_type=MESH)

    def x_copy(ar, part, j):
        return pltpu.make_async_remote_copy(pbuf.at[j, own(part), :], xbs[ar].at[j, landed(part), :], x_ss.at[part, j], x_rs.at[ar, part, j], device_id=x_peer, device_id_type=MESH)

    def h_copy(ar, part, j):
        return pltpu.make_async_remote_copy(hs[ar].at[j, own(part), :], hs[ar].at[j, own(part), :], h_ss.at[part, j], h_rs.at[part, j], device_id=core_peer, device_id_type=MESH)

    def h_wait(ar, part, j):
        pltpu.make_async_remote_copy(hs[ar].at[j, oth(part), :], hs[ar].at[j, oth(part), :], h_ss.at[part, j], h_rs.at[part, j], device_id=core_peer, device_id_type=MESH).wait_recv()

    def sent(l, ar, part, j):
        if l > 0 or ar == M:
            p_copy(1 - ar, part, j).wait_send()
            x_copy(1 - ar, part, j).wait_send()

    def pair_sum(ar, part, j):
        p_copy(ar, part, j).wait_recv()
        pbuf[j, own(part), :] = (pbuf[j, own(part), :].astype(F32) + rbuf[j, landed(part), :].astype(F32)).astype(BF16)
        x_copy(ar, part, j).start()

    def finish(l, ar, part, j):
        x_copy(ar, part, j).wait_recv()
        total = pbuf[j, own(part), :].astype(F32) + xbs[ar][j, landed(part), :].astype(F32)
        resid = hs[1 - ar][j, own(part), :].astype(F32)
        if l > 0 or ar == M:
            h_copy(1 - ar, part, j).wait_send()
        hs[ar][j, own(part), :] = (resid + total).astype(BF16)
        h_copy(ar, part, j).start()

    def add_squares(r, vals):
        sq = vals * vals
        ssq[r, :] += sq[:, :128] + sq[:, 128:256] + sq[:, 256:384] + sq[:, 384:]

    def inv_rms(r):
        return lax.rsqrt(jnp.sum(ssq[r, :], axis=-1, keepdims=True) * (1.0 / width) + EPSILON)

    def next_scale(r):
        inv = inv_rms(r)
        scale = inv / pre[r, :1]
        n = ssq[r, :].shape[0]
        pre[r, :] = jnp.broadcast_to(jnp.maximum(inv, 1e-30), (n, 128))
        ssq[r, :] = jnp.zeros((n, 128), F32)
        return scale

    def qkv_block(l, part, pair):
        r = whole(part)
        a = []
        for j in pair:
            if l > 0:
                h_wait(M, part, j)
            vals = h_m[j, r, :].astype(F32)
            add_squares(r, vals)
            a.append((vals * pre[r, :1] * gain_a[l:l + 1, cols(j)].astype(F32)).astype(BF16))
            if part == DEC:
                qkv_wait(j)
        for n in range(n_qkv // CW):
            total = acc[r, n * CW:(n + 1) * CW]
            for j, a_j in zip(pair, a):
                slot, left = qkv_place(j)
                total += jnp.dot(a_j, gbuf[slot, :, pl.ds(pl.multiple_of(left + n * CW, 128), CW)], preferred_element_type=F32)
            acc[r, n * CW:(n + 1) * CW] = total

    def qkv_begin(part):
        acc[whole(part), :n_qkv] = jnp.zeros((size[part], n_qkv), F32)

    def qkv_decode(l):
        qkv_begin(DEC)
        steps = n_chunks // 2

        def pair(i):
            return 2 * i, 2 * i + 1

        def step(i, c):
            if l > 0:
                for j in pair(i):
                    finish(l - 1, M, DEC, j)

                @pl.when(i >= 1)
                def _():
                    qkv_block(l, DEC, pair(i - 1))
            else:
                qkv_block(l, DEC, pair(i))

                @pl.when(i == 2)
                def _():
                    for j in range(n_chunks):
                        wo_copy(l, j).start()
            return c

        lax.fori_loop(0, steps, step, 0)
        if l > 0:
            qkv_block(l, DEC, pair(steps - 1))
        qkv_end(DEC)

    def qkv_end(part):
        r = whole(part)
        scale = next_scale(r)
        c_tab, s_tab = cos[r, :], sin[r, :]

        def head(col):
            return (acc[r, col * hd:(col + 1) * hd] * scale).astype(BF16).astype(F32)

        def rope(t):
            return (t * c_tab + pltpu.roll(t, hd // 2, 1) * s_tab).astype(BF16)

        for h in range(heads):
            q = rope(head(h))
            if part == DEC:
                qs[pl.ds(h, dec, stride=heads), :] = q.astype(F32)
            else:
                att[dec:, h * hd:(h + 1) * hd] = q
        for g in range(kv_heads):
            k = rope(head(heads + g))
            v = head(heads + kv_heads + g)
            if part == DEC:
                for h in range(g * group, (g + 1) * group):
                    kn[pl.ds(h, dec, stride=heads), :] = k.astype(F32)
                    vn[pl.ds(h, dec, stride=heads), :] = v
            else:
                kp[:, g * hd:(g + 1) * hd] = k
                vp[:, g * hd:(g + 1) * hd] = v.astype(BF16)

    def decode_attention(l):
        first_rows = lax.broadcasted_iota(jnp.int32, (heads, hd), 0) < group
        places = lax.broadcasted_iota(jnp.int32, (heads, seq), 1)
        n_slots = dec // KV_ROWS
        step_rows = ATT_SLOTS * KV_ROWS

        def block(i, c):
            slots = []
            for t in range(ATT_SLOTS):
                wait(kv_copies(l, ATT_SLOTS * i + t))
                slots.append(lax.rem(ATT_SLOTS * i + t, KV_SLOTS))
            scores = []
            for n in range(step_rows):
                b = i * step_rows + n
                slot, m = slots[n // KV_ROWS], n % KV_ROWS
                q = qs[pl.ds(pl.multiple_of(b * heads, heads), heads), :]
                zero = jnp.zeros_like(q)
                q2 = jnp.concatenate([jnp.where(first_rows, q, zero), jnp.where(first_rows, zero, q)], axis=1).astype(BF16)
                k2 = jnp.concatenate([kbuf[slot, m, 0], kbuf[slot, m, 1]], axis=1)
                s = lax.dot_general(q2, k2, (((1,), (1,)), ((), ())), preferred_element_type=F32) * scale_qk
                scores.append(jnp.where(places < lens[b], s, -jnp.inf))
            r = pl.ds(pl.multiple_of(i * step_rows * heads, step_rows * heads), step_rows * heads)
            s = jnp.concatenate(scores, axis=0)
            s_new = jnp.sum(qs[r, :] * kn[r, :], axis=-1, keepdims=True) * scale_qk
            top = jnp.maximum(jnp.max(s, axis=-1, keepdims=True), s_new)
            e = jnp.exp(s - top)
            e_new = jnp.exp(s_new - top)
            inv = 1.0 / (jnp.sum(e, axis=-1, keepdims=True) + e_new)
            p = (e * inv).astype(BF16)
            p_new = (e_new * inv).astype(BF16).astype(F32)
            outs = []
            for n in range(step_rows):
                slot, m = slots[n // KV_ROWS], n % KV_ROWS
                v2 = jnp.concatenate([vbuf[slot, m, 0], vbuf[slot, m, 1]], axis=1)
                o = jnp.dot(p[n * heads:(n + 1) * heads], v2, preferred_element_type=F32)
                outs.append(jnp.where(first_rows, o[:, :hd], o[:, hd:]))
            qs[r, :] = jnp.concatenate(outs, axis=0) + p_new * vn[r, :]

            for t in range(ATT_SLOTS):
                nxt = ATT_SLOTS * i + t + KV_SLOTS

                @pl.when(nxt < n_slots)
                def _():
                    start(kv_copies(l, nxt))
            return c

        lax.fori_loop(0, n_slots // ATT_SLOTS, block, 0)
        for h in range(heads):
            att[:dec, h * hd:(h + 1) * hd] = qs[pl.ds(h, dec, stride=heads), :].astype(BF16)

    def prefill_attention(l):
        wait(kv_pre_copies(l))
        old = jnp.where(lax.broadcasted_iota(jnp.int32, (1, seq), 1) < lens[dec], 0.0, -jnp.inf)
        causal = jnp.where(lax.broadcasted_iota(jnp.int32, (chunk, chunk), 1) <= lax.broadcasted_iota(jnp.int32, (chunk, chunk), 0), 0.0, -jnp.inf)
        causal = jnp.concatenate([causal] * STACK, axis=0)
        for first in range(0, heads, STACK):
            g = first // group
            cut = [slice((first + i) * hd, (first + i + 1) * hd) for i in range(STACK)]
            q = jnp.concatenate([att[dec:, c] for c in cut], axis=0)
            kv_col = slice(g * hd, (g + 1) * hd)
            s = lax.dot_general(q, kpre[g], (((1,), (1,)), ((), ())), preferred_element_type=F32) * scale_qk + old
            t = lax.dot_general(q, kp[:, kv_col], (((1,), (1,)), ((), ())), preferred_element_type=F32) * scale_qk + causal
            top = jnp.maximum(jnp.max(s, axis=-1, keepdims=True), jnp.max(t, axis=-1, keepdims=True))
            es = jnp.exp(s - top)
            et = jnp.exp(t - top)
            inv = 1.0 / (jnp.sum(es, axis=-1, keepdims=True) + jnp.sum(et, axis=-1, keepdims=True))
            o = jnp.dot((es * inv).astype(BF16), vpre[g], preferred_element_type=F32)
            o += jnp.dot((et * inv).astype(BF16), vp[:, kv_col], preferred_element_type=F32)
            for i in range(STACK):
                att[dec:, cut[i]] = o[i * chunk:(i + 1) * chunk].astype(BF16)

    def o_part(l, part):
        r = whole(part)

        def step(i, c):
            these = tuple(GROUP * i + t for t in range(GROUP))
            for j in these:
                if part == DEC:
                    wo_copy(l, j).wait()
                sent(l, O, part, j)
            for j in these:
                w = dbuf[j // o_per_slot, pl.ds(pl.multiple_of(lax.rem(j, o_per_slot) * o_depth, 16), o_depth), :]
                pbuf[j, r, :] = jnp.dot(att[r, :], w, preferred_element_type=F32).astype(BF16)
            for j in these:
                p_copy(O, part, j).start()

            @pl.when(i >= 1)
            def _():
                for j in these:
                    pair_sum(O, part, j - GROUP)
            return c

        lax.fori_loop(0, n_chunks // GROUP, step, 0)

    def gate_up(l):
        def operand(r, j):
            vals = h_o[j, r, :].astype(F32)
            add_squares(r, vals)
            return (vals * pre[r, :1] * gain_m[l:l + 1, cols(j)].astype(F32)).astype(BF16)

        def release(j, m):
            nxt = j + (G_SLOTS + m) // 2

            @pl.when(nxt < n_chunks)
            def _():
                g_copy(l, nxt, (G_SLOTS + m) % 2).start()

        def make_ahead(j):
            abuf[j % 2] = operand(pl.ds(0, rows), j)

        def first_block(part):
            r = whole(part)
            a = operand(r, 0)
            for m in range(2):
                if part == DEC:
                    g_copy(l, 0, m).wait()
                elif m == 1:
                    h_wait(O, DEC, 1)
                    h_wait(O, PRE, 1)
                    make_ahead(1)
                for n in range(ff // CW):
                    acc[r, m * ff + n * CW:m * ff + (n + 1) * CW] = jnp.dot(a, gbuf[m, :, n * CW:(n + 1) * CW], preferred_element_type=F32)
                if part == PRE:
                    g_copy(l, (G_SLOTS + m) // 2, (G_SLOTS + m) % 2).start()

        def block(j, more):
            for m in range(2):
                g_copy(l, j, m).wait()
                slot = lax.rem(2 * j + m, G_SLOTS)
                if m == 1 and more:
                    h_wait(O, DEC, j + 1)
                    h_wait(O, PRE, j + 1)
                    make_ahead(j + 1)
                a = abuf[j % 2]
                for n in range(ff // CW):
                    acc[:, m * ff + n * CW:m * ff + (n + 1) * CW] += jnp.dot(a, gbuf[slot, :, n * CW:(n + 1) * CW], preferred_element_type=F32)
                if more:
                    release(j, m)

            @pl.when(j >= n_chunks - D_SLOTS)
            def _():
                d_copy(l, j - (n_chunks - D_SLOTS)).start()

        def dec_step(j, c):
            finish(l, O, DEC, j)
            return c

        lax.fori_loop(0, GROUP, dec_step, 0)
        for j in range(GROUP, n_chunks):
            if j >= AHEAD:
                pair_sum(O, DEC, j)
            pair_sum(O, PRE, j)
        lax.fori_loop(GROUP, AHEAD, dec_step, 0)
        finish(l, O, PRE, 0)
        h_wait(O, DEC, 0)
        first_block(DEC)
        finish(l, O, PRE, 1)
        h_wait(O, PRE, 0)
        first_block(PRE)

        def step(j, c):
            @pl.when(j + 1 >= AHEAD)
            def _():
                finish(l, O, DEC, j + 1)

            finish(l, O, PRE, j + 1)
            block(j, True)
            return c

        lax.fori_loop(1, n_chunks - 1, step, 0)
        block(n_chunks - 1, False)
        scale = next_scale(pl.ds(0, rows))

        def act_step(n, c):
            gate = acc[:, cols(n)] * scale
            up = acc[:, pl.ds(pl.multiple_of(ff + n * CW, CW), CW)] * scale
            act[:, cols(n)] = (gate * jax.nn.sigmoid(gate) * up).astype(BF16)
            return c

        lax.fori_loop(0, ff // CW, act_step, 0)

    def down(l):
        def step(j, c):
            d_copy(l, j).wait()
            for part in (DEC, PRE):
                sent(l, M, part, j)
            pbuf[j] = jnp.dot(act[...], dbuf[lax.rem(j, D_SLOTS)], preferred_element_type=F32).astype(BF16)
            for part in (DEC, PRE):
                p_copy(M, part, j).start()

            @pl.when(j + D_SLOTS < n_chunks)
            def _():
                d_copy(l, j + D_SLOTS).start()

            if l + 1 < layers:
                for n in range(3):
                    nxt = 3 * (j - (n_chunks - D_SLOTS)) + n

                    @pl.when((nxt >= 0) & (nxt < n_chunks))
                    def _():
                        start(qkv_copies(l + 1, nxt))

            @pl.when(j >= 1)
            def _():
                pair_sum(M, DEC, j - 1)
            return c

        lax.fori_loop(0, n_chunks, step, 0)
        pair_sum(M, DEC, n_chunks - 1)
        if l + 1 < layers:
            start(kv_pre_copies(l + 1))
            for i in range(KV_SLOTS):
                start(kv_copies(l + 1, i))
            for j in range(n_chunks):
                wo_copy(l + 1, j).start()

        def pre_step(j, c):
            pair_sum(M, PRE, j)
            return c

        lax.fori_loop(0, n_chunks, pre_step, 0)

    for j in range(n_chunks):
        x_load(j).start()
    barrier = pltpu.get_barrier_semaphore()
    for peer in (core_peer, x_peer):
        pl.semaphore_signal(barrier, inc=1, device_id=peer, device_id_type=MESH)
    for j in range(n_chunks):
        start(qkv_copies(0, j))
    for i in range(KV_SLOTS):
        start(kv_copies(0, i))
    start(kv_pre_copies(0))
    ssq[...] = jnp.zeros_like(ssq)

    def place(b, c):
        cos[pl.ds(b, 1), :] = jnp.full((1, hd), lens[b], jnp.int32).astype(F32)
        return c

    lax.fori_loop(0, dec, place, 0)
    cos[pl.ds(dec, chunk), :] = (lax.broadcasted_iota(jnp.int32, (chunk, hd), 0) + lens[dec]).astype(F32)
    angles = cos[...] * freq[...]
    low = lax.broadcasted_iota(jnp.int32, (rows, hd), 1) < hd // 2
    sines = jnp.sin(angles)
    sin[...] = jnp.where(low, -sines, sines)
    cos[...] = jnp.cos(angles)
    pltpu.make_async_copy(h_m, h_m, io_sem.at[0]).wait()

    def sq_step(j, c):
        add_squares(pl.ds(0, rows), h_m[j].astype(F32))
        return c

    lax.fori_loop(0, n_chunks, sq_step, 0)
    pre[...] = jnp.broadcast_to(jnp.maximum(inv_rms(pl.ds(0, rows)), 1e-30), pre.shape)
    ssq[...] = jnp.zeros_like(ssq)
    pl.semaphore_wait(barrier, 2)

    def finish_pre(l, first, stop):
        if l > 0:
            def pre_step(j, c):
                finish(l - 1, M, PRE, j)
                return c

            lax.fori_loop(first, stop, pre_step, 0)

    for l in range(layers):
        qkv_decode(l)
        decode_attention(l)
        finish_pre(l, 0, 5)
        o_part(l, DEC)
        finish_pre(l, 5, 8)
        qkv_begin(PRE)
        qkv_block(l, PRE, tuple(range(5)))
        for j in range(GROUP, AHEAD):
            pair_sum(O, DEC, j)
        finish_pre(l, 8, 10)
        qkv_block(l, PRE, (5, 6, 7))
        qkv_block(l, PRE, (8, 9))
        qkv_end(PRE)
        for i in range(G_SLOTS):
            g_copy(l, i // 2, i % 2).start()
        prefill_attention(l)
        o_part(l, PRE)
        gate_up(l)
        down(l)

    def out_copy(part, j):
        r = whole(part)
        return pltpu.make_async_copy(h_m.at[j, r, :], y.at[r, cols(j)], io_sem.at[3 + part])

    def out_dec(j, c):
        finish(layers - 1, M, DEC, j)

        @pl.when(j >= 1)
        def _():
            h_wait(M, DEC, j - 1)
            out_copy(DEC, j - 1).start()

        p_copy(M, DEC, j).wait_send()
        p_copy(M, PRE, j).wait_send()
        return c

    lax.fori_loop(0, n_chunks, out_dec, 0)
    h_wait(M, DEC, n_chunks - 1)
    out_copy(DEC, n_chunks - 1).start()

    def out_pre(j, c):
        finish(layers - 1, M, PRE, j)
        x_copy(M, DEC, j).wait_send()
        h_copy(M, DEC, j).wait_send()

        @pl.when(j >= 1)
        def _():
            h_wait(M, PRE, j - 1)
            out_copy(PRE, j - 1).start()
            x_copy(M, PRE, j - 1).wait_send()

        @pl.when(j >= 2)
        def _():
            h_copy(M, PRE, j - 2).wait_send()
        return c

    lax.fori_loop(0, n_chunks, out_pre, 0)
    last = n_chunks - 1
    h_wait(M, PRE, last)
    out_copy(PRE, last).start()
    x_copy(M, PRE, last).wait_send()
    for j in (last - 1, last):
        h_copy(M, PRE, j).wait_send()
    for part in (DEC, PRE):
        done = h_m.at[:, whole(part), :]
        pltpu.make_async_copy(done, done, io_sem.at[3 + part]).wait()


def step_call(lengths, x, freq, attn_gain, mlp_gain, w_q, w_k, w_v, w_o, w_gate, w_up, w_down, k_cache, v_cache):
    rows, width = x.shape
    dec = lengths.shape[0] - 1
    chunk = rows - dec
    ff = w_gate.shape[2]
    n_chunks = width // CW
    q_cols, k_cols = w_q.shape[2], w_k.shape[2]
    kv_heads, seq, hd = k_cache.shape[2:]
    heads = q_cols // hd
    vmem = pl.BlockSpec(memory_space=pltpu.VMEM)
    hbm = pl.BlockSpec(memory_space=pl.ANY)
    smem = pl.BlockSpec(memory_space=pltpu.SMEM)
    sem = pltpu.SemaphoreType.DMA
    buf = pltpu.VMEM
    return pl.pallas_call(
        functools.partial(step_kernel, (dec, chunk)),
        out_shape=jax.ShapeDtypeStruct((rows, width), BF16),
        in_specs=[smem, hbm, vmem, vmem, vmem] + [hbm] * 9,
        out_specs=hbm,
        scratch_shapes=[
            buf((G_SLOTS, CW, ff), BF16),
            buf((D_SLOTS, ff, CW), BF16),
            buf((2, rows, CW), BF16),
            buf((rows, 2 * ff), F32),
            buf((rows, ff), BF16),
            buf((n_chunks, rows, CW), BF16),
            buf((n_chunks, rows // 2, CW), BF16),
            buf((n_chunks, rows // 2, CW), BF16),
            buf((n_chunks, rows // 2, CW), BF16),
            buf((n_chunks, rows, CW), BF16),
            buf((n_chunks, rows, CW), BF16),
            buf((rows, 128), F32),
            buf((rows, 128), F32),
            buf((rows, hd), F32),
            buf((rows, hd), F32),
            buf((KV_SLOTS, KV_ROWS, kv_heads, seq, hd), BF16),
            buf((KV_SLOTS, KV_ROWS, kv_heads, seq, hd), BF16),
            buf((kv_heads, seq, hd), BF16),
            buf((kv_heads, seq, hd), BF16),
            buf((dec * heads, hd), F32),
            buf((dec * heads, hd), F32),
            buf((dec * heads, hd), F32),
            sem((n_chunks,)),
            sem((n_chunks,)),
            sem((G_SLOTS,)),
            sem((D_SLOTS,)),
            sem((KV_SLOTS, 2)),
            sem((5,)),
            sem((2, n_chunks)),
            sem((2, n_chunks)),
            sem((2, n_chunks)),
            sem((2, 2, n_chunks)),
            sem((2, n_chunks)),
            sem((2, n_chunks)),
        ],
        compiler_params=pltpu.CompilerParams(collective_id=0, has_side_effects=True, vmem_limit_bytes=67043328),
        name='decoder_step',
    )(lengths, x, freq, attn_gain, mlp_gain, w_q, w_k, w_v, w_o, w_gate, w_up, w_down, k_cache, v_cache)


def solution(mesh):
    col_spec = P(None, None, 'tp')
    row_spec = P(None, 'tp', None)
    cache_spec = P(None, 'dp', 'tp', None, None)
    in_specs = (P('dp', None), P('dp'), P(), col_spec, col_spec, col_spec, row_spec, P(), col_spec, col_spec, row_spec, cache_spec, cache_spec)

    def body(x, lengths, attn_gain, w_q, w_k, w_v, w_o, mlp_gain, w_gate, w_up, w_down, k_cache, v_cache):
        head_dim = k_cache.shape[-1]
        exps = np.arange(0, head_dim, 2, dtype=np.float32) / np.float32(head_dim)
        freq = np.power(np.float32(ROPE_BASE), -exps).astype(np.float32)
        freq = jnp.asarray(np.concatenate([freq, freq])[None])
        return step_call(lengths, x, freq, attn_gain, mlp_gain, w_q, w_k, w_v, w_o, w_gate, w_up, w_down, k_cache, v_cache)

    return jax.shard_map(body, mesh=mesh, in_specs=in_specs, out_specs=P('dp', None), check_vma=False)
```

```python
import functools

import jax
import jax.numpy as jnp
import numpy as np
from jax import lax
from jax.experimental import pallas as pl
from jax.experimental.pallas import tpu as pltpu
from jax.sharding import PartitionSpec as P

ROPE_BASE = 500000.0
EPSILON = 1e-5
MESH = pl.DeviceIdType.MESH
F32 = jnp.float32
BF16 = jnp.bfloat16
CW = 512
G_SLOTS = 5
D_SLOTS = 4
KV_SLOTS = 5
KV_ROWS = 8
ATT_SLOTS = 2
AHEAD_FIRST, AHEAD = 8, 6
STACK = 4
GROUP = 5
O, M = 0, 1
DEC, PRE = 0, 1


def step_kernel(dims, lens, x_in, freq, gain_a, gain_m, wq, wk, wv, wo, wg, wu, wd, kc, vc, y,
                gbuf, dbuf, abuf, acc, act, pbuf, rbuf, xb_o, xb_m, h_o, h_m, ssq, pre, cos, sin, kbuf, vbuf, kpre, vpre,
                qs, kn, vn,
                q_sem, w_sem, g_sem, d_sem, kv_sem, io_sem, p_ss, p_rs, x_ss, x_rs, h_ss, h_rs):
    dec, chunk = dims
    rows = dec + chunk
    width = x_in.shape[1]
    layers, o_depth = wo.shape[0], wo.shape[1]
    ff = wg.shape[2]
    q_cols, k_cols = wq.shape[2], wk.shape[2]
    n_qkv = q_cols + 2 * k_cols
    seq, hd = kc.shape[3], kc.shape[4]
    heads, kv_heads = q_cols // hd, k_cols // hd
    group = heads // kv_heads
    n_chunks = width // CW
    o_per_slot = ff // o_depth
    scale_qk = hd ** -0.5
    base = (0, dec)
    size = (dec, chunk)
    half = (dec // 2, chunk // 2)
    rbase = (0, dec // 2)

    dp_me = lax.axis_index('dp')
    me = lax.axis_index('tp')
    core = lax.rem(me, 2)
    core_peer = (dp_me, me + 1 - 2 * core)
    x_peer = (dp_me, lax.rem(me + 2, 4))

    def own(part):
        return pl.ds(pl.multiple_of(base[part] + core * half[part], 16), half[part])

    def oth(part):
        return pl.ds(pl.multiple_of(base[part] + (1 - core) * half[part], 16), half[part])

    def whole(part):
        return pl.ds(base[part], size[part])

    def landed(part):
        return pl.ds(rbase[part], half[part])

    def cols(j):
        return pl.ds(pl.multiple_of(j * CW, CW), CW)

    att = act.at[:, pl.ds(0, q_cols)]
    kp = act.at[pl.ds(0, chunk), pl.ds(q_cols, k_cols)]
    vp = act.at[pl.ds(0, chunk), pl.ds(q_cols + k_cols, k_cols)]

    def order(l):
        return (PRE, DEC, AHEAD_FIRST) if l == 0 else (DEC, PRE, AHEAD)

    xbs = (xb_o, xb_m)
    hs = (h_o, h_m)

    def x_load(j):
        return pltpu.make_async_copy(x_in.at[:, cols(j)], h_m.at[j], io_sem.at[0])

    def wo_copy(l, j):
        return pltpu.make_async_copy(wo.at[l, :, cols(j)], dbuf.at[j // o_per_slot, pl.ds(pl.multiple_of(lax.rem(j, o_per_slot) * o_depth, 16), o_depth), :], w_sem.at[j])

    def g_copy(l, j, m):
        slot = lax.rem(2 * j + m, G_SLOTS)
        return pltpu.make_async_copy((wg, wu)[m].at[l, cols(j), :], gbuf.at[slot], g_sem.at[slot])

    def d_copy(l, j):
        slot = lax.rem(j, D_SLOTS)
        return pltpu.make_async_copy(wd.at[l, :, cols(j)], dbuf.at[slot], d_sem.at[slot])

    def qkv_place(j):
        return j // 2, (j % 2) * (ff // 2)

    def qkv_copies(l, j):
        slot, left = qkv_place(j)
        dst = gbuf.at[slot]

        def at(off, n):
            return dst.at[:, pl.ds(pl.multiple_of(left + off, 128), n)]

        return (pltpu.make_async_copy(wq.at[l, cols(j), :], at(0, q_cols), q_sem.at[j]),
                pltpu.make_async_copy(wk.at[l, cols(j), :], at(q_cols, k_cols), q_sem.at[j]),
                pltpu.make_async_copy(wv.at[l, cols(j), :], at(q_cols + k_cols, k_cols), q_sem.at[j]))

    def qkv_wait(j):
        slot, left = qkv_place(j)
        dst = gbuf.at[slot, :, pl.ds(pl.multiple_of(left, 128), n_qkv)]
        pltpu.make_async_copy(dst, dst, q_sem.at[j]).wait()

    def kv_copies(l, i):
        slot = lax.rem(i, KV_SLOTS)
        src = pl.ds(i * KV_ROWS, KV_ROWS)
        return (pltpu.make_async_copy(kc.at[l, src], kbuf.at[slot], kv_sem.at[slot, 0]),
                pltpu.make_async_copy(vc.at[l, src], vbuf.at[slot], kv_sem.at[slot, 1]))

    def kv_pre_copies(l):
        return (pltpu.make_async_copy(kc.at[l, dec], kpre, io_sem.at[1]),
                pltpu.make_async_copy(vc.at[l, dec], vpre, io_sem.at[2]))

    def start(copies):
        for c in copies:
            c.start()

    def wait(copies):
        for c in copies:
            c.wait()

    def p_copy(ar, part, j):
        return pltpu.make_async_remote_copy(pbuf.at[j, oth(part), :], rbuf.at[j, landed(part), :], p_ss.at[part, j], p_rs.at[part, j], device_id=core_peer, device_id_type=MESH)

    def x_copy(ar, part, j):
        return pltpu.make_async_remote_copy(pbuf.at[j, own(part), :], xbs[ar].at[j, landed(part), :], x_ss.at[part, j], x_rs.at[ar, part, j], device_id=x_peer, device_id_type=MESH)

    def h_copy(ar, part, j):
        return pltpu.make_async_remote_copy(hs[ar].at[j, own(part), :], hs[ar].at[j, own(part), :], h_ss.at[part, j], h_rs.at[part, j], device_id=core_peer, device_id_type=MESH)

    def h_wait(ar, part, j):
        pltpu.make_async_remote_copy(hs[ar].at[j, oth(part), :], hs[ar].at[j, oth(part), :], h_ss.at[part, j], h_rs.at[part, j], device_id=core_peer, device_id_type=MESH).wait_recv()

    def sent(l, ar, part, j):
        if l > 0 or ar == M:
            p_copy(1 - ar, part, j).wait_send()
            x_copy(1 - ar, part, j).wait_send()

    def pair_sum(ar, part, j):
        p_copy(ar, part, j).wait_recv()
        pbuf[j, own(part), :] = (pbuf[j, own(part), :].astype(F32) + rbuf[j, landed(part), :].astype(F32)).astype(BF16)
        x_copy(ar, part, j).start()

    def finish(l, ar, part, j):
        x_copy(ar, part, j).wait_recv()
        total = pbuf[j, own(part), :].astype(F32) + xbs[ar][j, landed(part), :].astype(F32)
        resid = hs[1 - ar][j, own(part), :].astype(F32)
        if l > 0 or ar == M:
            h_copy(1 - ar, part, j).wait_send()
        hs[ar][j, own(part), :] = (resid + total).astype(BF16)
        h_copy(ar, part, j).start()

    def add_squares(r, vals):
        sq = vals * vals
        ssq[r, :] += sq[:, :128] + sq[:, 128:256] + sq[:, 256:384] + sq[:, 384:]

    def inv_rms(r):
        return lax.rsqrt(jnp.sum(ssq[r, :], axis=-1, keepdims=True) * (1.0 / width) + EPSILON)

    def next_scale(r):
        inv = inv_rms(r)
        scale = inv / pre[r, :1]
        n = ssq[r, :].shape[0]
        pre[r, :] = jnp.broadcast_to(jnp.maximum(inv, 1e-30), (n, 128))
        ssq[r, :] = jnp.zeros((n, 128), F32)
        return scale

    def qkv_block(l, part, pair):
        r = whole(part)
        a = []
        for j in pair:
            if l > 0:
                h_wait(M, part, j)
            vals = h_m[j, r, :].astype(F32)
            add_squares(r, vals)
            a.append((vals * pre[r, :1] * gain_a[l:l + 1, cols(j)].astype(F32)).astype(BF16))
            if part == order(l)[0]:
                qkv_wait(j)
        for n in range(n_qkv // CW):
            total = acc[r, n * CW:(n + 1) * CW]
            for j, a_j in zip(pair, a):
                slot, left = qkv_place(j)
                total += jnp.dot(a_j, gbuf[slot, :, pl.ds(pl.multiple_of(left + n * CW, 128), CW)], preferred_element_type=F32)
            acc[r, n * CW:(n + 1) * CW] = total

    def qkv_begin(part):
        acc[whole(part), :n_qkv] = jnp.zeros((size[part], n_qkv), F32)

    def qkv_lead(l):
        part = order(l)[0]
        qkv_begin(part)
        steps = n_chunks // 2

        def pair(i):
            return 2 * i, 2 * i + 1

        def step(i, c):
            if l > 0:
                for j in pair(i):
                    finish(l - 1, M, part, j)

                @pl.when(i >= 1)
                def _():
                    qkv_block(l, part, pair(i - 1))
            else:
                qkv_block(l, part, pair(i))

                @pl.when(i == 1)
                def _():
                    for j in range(n_chunks):
                        wo_copy(l, j).start()

                @pl.when(i == 3)
                def _():
                    for n in range(KV_SLOTS):
                        start(kv_copies(l, n))
            return c

        lax.fori_loop(0, steps, step, 0)
        if l > 0:
            qkv_block(l, part, pair(steps - 1))
        qkv_end(part)

    def qkv_end(part):
        r = whole(part)
        scale = next_scale(r)
        c_tab, s_tab = cos[r, :], sin[r, :]

        def head(col):
            return (acc[r, col * hd:(col + 1) * hd] * scale).astype(BF16).astype(F32)

        def rope(t):
            return (t * c_tab + pltpu.roll(t, hd // 2, 1) * s_tab).astype(BF16)

        for h in range(heads):
            q = rope(head(h))
            if part == DEC:
                qs[pl.ds(h, dec, stride=heads), :] = q.astype(F32)
            else:
                att[dec:, h * hd:(h + 1) * hd] = q
        for g in range(kv_heads):
            k = rope(head(heads + g))
            v = head(heads + kv_heads + g)
            if part == DEC:
                for h in range(g * group, (g + 1) * group):
                    kn[pl.ds(h, dec, stride=heads), :] = k.astype(F32)
                    vn[pl.ds(h, dec, stride=heads), :] = v
            else:
                kp[:, g * hd:(g + 1) * hd] = k
                vp[:, g * hd:(g + 1) * hd] = v.astype(BF16)

    def decode_attention(l):
        first_rows = lax.broadcasted_iota(jnp.int32, (heads, hd), 0) < group
        places = lax.broadcasted_iota(jnp.int32, (heads, seq), 1)
        n_slots = dec // KV_ROWS
        step_rows = ATT_SLOTS * KV_ROWS

        def block(i, c):
            slots = []
            for t in range(ATT_SLOTS):
                wait(kv_copies(l, ATT_SLOTS * i + t))
                slots.append(lax.rem(ATT_SLOTS * i + t, KV_SLOTS))
            scores = []
            for n in range(step_rows):
                b = i * step_rows + n
                slot, m = slots[n // KV_ROWS], n % KV_ROWS
                q = qs[pl.ds(pl.multiple_of(b * heads, heads), heads), :]
                zero = jnp.zeros_like(q)
                q2 = jnp.concatenate([jnp.where(first_rows, q, zero), jnp.where(first_rows, zero, q)], axis=1).astype(BF16)
                k2 = jnp.concatenate([kbuf[slot, m, 0], kbuf[slot, m, 1]], axis=1)
                s = lax.dot_general(q2, k2, (((1,), (1,)), ((), ())), preferred_element_type=F32) * scale_qk
                scores.append(jnp.where(places < lens[b], s, -jnp.inf))
            r = pl.ds(pl.multiple_of(i * step_rows * heads, step_rows * heads), step_rows * heads)
            s = jnp.concatenate(scores, axis=0)
            s_new = jnp.sum(qs[r, :] * kn[r, :], axis=-1, keepdims=True) * scale_qk
            top = jnp.maximum(jnp.max(s, axis=-1, keepdims=True), s_new)
            e = jnp.exp(s - top)
            e_new = jnp.exp(s_new - top)
            inv = 1.0 / (jnp.sum(e, axis=-1, keepdims=True) + e_new)
            p = (e * inv).astype(BF16)
            p_new = (e_new * inv).astype(BF16).astype(F32)
            outs = []
            for n in range(step_rows):
                slot, m = slots[n // KV_ROWS], n % KV_ROWS
                v2 = jnp.concatenate([vbuf[slot, m, 0], vbuf[slot, m, 1]], axis=1)
                o = jnp.dot(p[n * heads:(n + 1) * heads], v2, preferred_element_type=F32)
                outs.append(jnp.where(first_rows, o[:, :hd], o[:, hd:]))
            qs[r, :] = jnp.concatenate(outs, axis=0) + p_new * vn[r, :]

            for t in range(ATT_SLOTS):
                nxt = ATT_SLOTS * i + t + KV_SLOTS

                @pl.when(nxt < n_slots)
                def _():
                    start(kv_copies(l, nxt))
            return c

        lax.fori_loop(0, n_slots // ATT_SLOTS, block, 0)
        for h in range(heads):
            att[:dec, h * hd:(h + 1) * hd] = qs[pl.ds(h, dec, stride=heads), :].astype(BF16)

    def prefill_attention(l):
        wait(kv_pre_copies(l))
        old = jnp.where(lax.broadcasted_iota(jnp.int32, (1, seq), 1) < lens[dec], 0.0, -jnp.inf)
        causal = jnp.where(lax.broadcasted_iota(jnp.int32, (chunk, chunk), 1) <= lax.broadcasted_iota(jnp.int32, (chunk, chunk), 0), 0.0, -jnp.inf)
        causal = jnp.concatenate([causal] * STACK, axis=0)
        for first in range(0, heads, STACK):
            g = first // group
            cut = [slice((first + i) * hd, (first + i + 1) * hd) for i in range(STACK)]
            q = jnp.concatenate([att[dec:, c] for c in cut], axis=0)
            kv_col = slice(g * hd, (g + 1) * hd)
            s = lax.dot_general(q, kpre[g], (((1,), (1,)), ((), ())), preferred_element_type=F32) * scale_qk + old
            t = lax.dot_general(q, kp[:, kv_col], (((1,), (1,)), ((), ())), preferred_element_type=F32) * scale_qk + causal
            top = jnp.maximum(jnp.max(s, axis=-1, keepdims=True), jnp.max(t, axis=-1, keepdims=True))
            es = jnp.exp(s - top)
            et = jnp.exp(t - top)
            inv = 1.0 / (jnp.sum(es, axis=-1, keepdims=True) + jnp.sum(et, axis=-1, keepdims=True))
            o = jnp.dot((es * inv).astype(BF16), vpre[g], preferred_element_type=F32)
            o += jnp.dot((et * inv).astype(BF16), vp[:, kv_col], preferred_element_type=F32)
            for i in range(STACK):
                att[dec:, cut[i]] = o[i * chunk:(i + 1) * chunk].astype(BF16)

    def o_part(l, part):
        r = whole(part)

        def step(i, c):
            these = tuple(GROUP * i + t for t in range(GROUP))
            for j in these:
                if part == order(l)[0]:
                    wo_copy(l, j).wait()
                sent(l, O, part, j)
            for j in these:
                w = dbuf[j // o_per_slot, pl.ds(pl.multiple_of(lax.rem(j, o_per_slot) * o_depth, 16), o_depth), :]
                pbuf[j, r, :] = jnp.dot(att[r, :], w, preferred_element_type=F32).astype(BF16)
            for j in these:
                p_copy(O, part, j).start()

            @pl.when(i >= 1)
            def _():
                for j in these:
                    pair_sum(O, part, j - GROUP)
            return c

        lax.fori_loop(0, n_chunks // GROUP, step, 0)

    def gate_up(l):
        lead, trail, ahead = order(l)

        def operand(r, j):
            vals = h_o[j, r, :].astype(F32)
            add_squares(r, vals)
            return (vals * pre[r, :1] * gain_m[l:l + 1, cols(j)].astype(F32)).astype(BF16)

        def release(j, m):
            nxt = j + (G_SLOTS + m) // 2

            @pl.when(nxt < n_chunks)
            def _():
                g_copy(l, nxt, (G_SLOTS + m) % 2).start()

        def make_ahead(j):
            abuf[j % 2] = operand(pl.ds(0, rows), j)

        def first_block(part):
            r = whole(part)
            a = operand(r, 0)
            for m in range(2):
                if part == lead:
                    g_copy(l, 0, m).wait()
                elif m == 1:
                    h_wait(O, DEC, 1)
                    h_wait(O, PRE, 1)
                    make_ahead(1)
                for n in range(ff // CW):
                    acc[r, m * ff + n * CW:m * ff + (n + 1) * CW] = jnp.dot(a, gbuf[m, :, n * CW:(n + 1) * CW], preferred_element_type=F32)
                if part == trail:
                    g_copy(l, (G_SLOTS + m) // 2, (G_SLOTS + m) % 2).start()

        def block(j, more):
            for m in range(2):
                g_copy(l, j, m).wait()
                slot = lax.rem(2 * j + m, G_SLOTS)
                if m == 1 and more:
                    h_wait(O, DEC, j + 1)
                    h_wait(O, PRE, j + 1)
                    make_ahead(j + 1)
                a = abuf[j % 2]
                for n in range(ff // CW):
                    acc[:, m * ff + n * CW:m * ff + (n + 1) * CW] += jnp.dot(a, gbuf[slot, :, n * CW:(n + 1) * CW], preferred_element_type=F32)
                if more:
                    release(j, m)

            @pl.when(j >= n_chunks - D_SLOTS)
            def _():
                d_copy(l, j - (n_chunks - D_SLOTS)).start()

        def lead_step(j, c):
            finish(l, O, lead, j)
            return c

        lax.fori_loop(0, GROUP, lead_step, 0)
        for j in range(GROUP, n_chunks):
            if j >= ahead:
                pair_sum(O, lead, j)
            pair_sum(O, trail, j)
        lax.fori_loop(GROUP, ahead, lead_step, 0)
        finish(l, O, trail, 0)
        h_wait(O, lead, 0)
        first_block(lead)
        finish(l, O, trail, 1)
        h_wait(O, trail, 0)
        first_block(trail)

        def step(j, c):
            @pl.when(j + 1 >= ahead)
            def _():
                finish(l, O, lead, j + 1)

            finish(l, O, trail, j + 1)
            block(j, True)
            return c

        lax.fori_loop(1, n_chunks - 1, step, 0)
        block(n_chunks - 1, False)
        scale = next_scale(pl.ds(0, rows))

        def act_step(n, c):
            gate = acc[:, cols(n)] * scale
            up = acc[:, pl.ds(pl.multiple_of(ff + n * CW, CW), CW)] * scale
            act[:, cols(n)] = (gate * jax.nn.sigmoid(gate) * up).astype(BF16)
            return c

        lax.fori_loop(0, ff // CW, act_step, 0)

    def down(l):
        def step(j, c):
            d_copy(l, j).wait()
            for part in (DEC, PRE):
                sent(l, M, part, j)
            pbuf[j] = jnp.dot(act[...], dbuf[lax.rem(j, D_SLOTS)], preferred_element_type=F32).astype(BF16)
            for part in (DEC, PRE):
                p_copy(M, part, j).start()

            @pl.when(j + D_SLOTS < n_chunks)
            def _():
                d_copy(l, j + D_SLOTS).start()

            if l + 1 < layers:
                for n in range(3):
                    nxt = 3 * (j - (n_chunks - D_SLOTS)) + n

                    @pl.when((nxt >= 0) & (nxt < n_chunks))
                    def _():
                        start(qkv_copies(l + 1, nxt))

            @pl.when(j >= 1)
            def _():
                pair_sum(M, DEC, j - 1)
            return c

        lax.fori_loop(0, n_chunks, step, 0)
        pair_sum(M, DEC, n_chunks - 1)
        if l + 1 < layers:
            start(kv_pre_copies(l + 1))
            for i in range(KV_SLOTS):
                start(kv_copies(l + 1, i))
            for j in range(n_chunks):
                wo_copy(l + 1, j).start()

        def pre_step(j, c):
            pair_sum(M, PRE, j)
            return c

        lax.fori_loop(0, n_chunks, pre_step, 0)

    for j in range(n_chunks):
        x_load(j).start()
    barrier = pltpu.get_barrier_semaphore()
    for peer in (core_peer, x_peer):
        pl.semaphore_signal(barrier, inc=1, device_id=peer, device_id_type=MESH)
    for j in range(n_chunks):
        start(qkv_copies(0, j))
    start(kv_pre_copies(0))
    ssq[...] = jnp.zeros_like(ssq)

    def place(b, c):
        cos[pl.ds(b, 1), :] = jnp.full((1, hd), lens[b], jnp.int32).astype(F32)
        return c

    lax.fori_loop(0, dec, place, 0)
    cos[pl.ds(dec, chunk), :] = (lax.broadcasted_iota(jnp.int32, (chunk, hd), 0) + lens[dec]).astype(F32)
    angles = cos[...] * freq[...]
    low = lax.broadcasted_iota(jnp.int32, (rows, hd), 1) < hd // 2
    sines = jnp.sin(angles)
    sin[...] = jnp.where(low, -sines, sines)
    cos[...] = jnp.cos(angles)
    pltpu.make_async_copy(h_m, h_m, io_sem.at[0]).wait()

    def sq_step(j, c):
        add_squares(pl.ds(0, rows), h_m[j].astype(F32))
        return c

    lax.fori_loop(0, n_chunks, sq_step, 0)
    pre[...] = jnp.broadcast_to(jnp.maximum(inv_rms(pl.ds(0, rows)), 1e-30), pre.shape)
    ssq[...] = jnp.zeros_like(ssq)
    pl.semaphore_wait(barrier, 2)

    def finish_pre(l, first, stop):
        if l > 0:
            def pre_step(j, c):
                finish(l - 1, M, PRE, j)
                return c

            lax.fori_loop(first, stop, pre_step, 0)

    for l in range(layers):
        lead, trail, ahead = order(l)
        attend = (decode_attention, prefill_attention)
        qkv_lead(l)
        attend[lead](l)
        finish_pre(l, 0, 5)
        o_part(l, lead)
        finish_pre(l, 5, 8)
        qkv_begin(trail)
        qkv_block(l, trail, tuple(range(5)))
        for j in range(GROUP, ahead):
            pair_sum(O, lead, j)
        finish_pre(l, 8, 10)
        qkv_block(l, trail, (5, 6, 7))
        qkv_block(l, trail, (8, 9))
        qkv_end(trail)
        if trail == PRE:
            for i in range(G_SLOTS):
                g_copy(l, i // 2, i % 2).start()
        attend[trail](l)
        if trail == DEC:
            for i in range(G_SLOTS):
                g_copy(l, i // 2, i % 2).start()
        o_part(l, trail)
        gate_up(l)
        down(l)

    def out_copy(part, j):
        r = whole(part)
        return pltpu.make_async_copy(h_m.at[j, r, :], y.at[r, cols(j)], io_sem.at[3 + part])

    def out_dec(j, c):
        finish(layers - 1, M, DEC, j)

        @pl.when(j >= 1)
        def _():
            h_wait(M, DEC, j - 1)
            out_copy(DEC, j - 1).start()

        p_copy(M, DEC, j).wait_send()
        p_copy(M, PRE, j).wait_send()
        return c

    lax.fori_loop(0, n_chunks, out_dec, 0)
    h_wait(M, DEC, n_chunks - 1)
    out_copy(DEC, n_chunks - 1).start()

    def out_pre(j, c):
        finish(layers - 1, M, PRE, j)
        x_copy(M, DEC, j).wait_send()
        h_copy(M, DEC, j).wait_send()

        @pl.when(j >= 1)
        def _():
            h_wait(M, PRE, j - 1)
            out_copy(PRE, j - 1).start()
            x_copy(M, PRE, j - 1).wait_send()

        @pl.when(j >= 2)
        def _():
            h_copy(M, PRE, j - 2).wait_send()
        return c

    lax.fori_loop(0, n_chunks, out_pre, 0)
    last = n_chunks - 1
    h_wait(M, PRE, last)
    out_copy(PRE, last).start()
    x_copy(M, PRE, last).wait_send()
    for j in (last - 1, last):
        h_copy(M, PRE, j).wait_send()
    for part in (DEC, PRE):
        done = h_m.at[:, whole(part), :]
        pltpu.make_async_copy(done, done, io_sem.at[3 + part]).wait()


def step_call(lengths, x, freq, attn_gain, mlp_gain, w_q, w_k, w_v, w_o, w_gate, w_up, w_down, k_cache, v_cache):
    rows, width = x.shape
    dec = lengths.shape[0] - 1
    chunk = rows - dec
    ff = w_gate.shape[2]
    n_chunks = width // CW
    q_cols, k_cols = w_q.shape[2], w_k.shape[2]
    kv_heads, seq, hd = k_cache.shape[2:]
    heads = q_cols // hd
    vmem = pl.BlockSpec(memory_space=pltpu.VMEM)
    hbm = pl.BlockSpec(memory_space=pl.ANY)
    smem = pl.BlockSpec(memory_space=pltpu.SMEM)
    sem = pltpu.SemaphoreType.DMA
    buf = pltpu.VMEM
    return pl.pallas_call(
        functools.partial(step_kernel, (dec, chunk)),
        out_shape=jax.ShapeDtypeStruct((rows, width), BF16),
        in_specs=[smem, hbm, vmem, vmem, vmem] + [hbm] * 9,
        out_specs=hbm,
        scratch_shapes=[
            buf((G_SLOTS, CW, ff), BF16),
            buf((D_SLOTS, ff, CW), BF16),
            buf((2, rows, CW), BF16),
            buf((rows, 2 * ff), F32),
            buf((rows, ff), BF16),
            buf((n_chunks, rows, CW), BF16),
            buf((n_chunks, rows // 2, CW), BF16),
            buf((n_chunks, rows // 2, CW), BF16),
            buf((n_chunks, rows // 2, CW), BF16),
            buf((n_chunks, rows, CW), BF16),
            buf((n_chunks, rows, CW), BF16),
            buf((rows, 128), F32),
            buf((rows, 128), F32),
            buf((rows, hd), F32),
            buf((rows, hd), F32),
            buf((KV_SLOTS, KV_ROWS, kv_heads, seq, hd), BF16),
            buf((KV_SLOTS, KV_ROWS, kv_heads, seq, hd), BF16),
            buf((kv_heads, seq, hd), BF16),
            buf((kv_heads, seq, hd), BF16),
            buf((dec * heads, hd), F32),
            buf((dec * heads, hd), F32),
            buf((dec * heads, hd), F32),
            sem((n_chunks,)),
            sem((n_chunks,)),
            sem((G_SLOTS,)),
            sem((D_SLOTS,)),
            sem((KV_SLOTS, 2)),
            sem((5,)),
            sem((2, n_chunks)),
            sem((2, n_chunks)),
            sem((2, n_chunks)),
            sem((2, 2, n_chunks)),
            sem((2, n_chunks)),
            sem((2, n_chunks)),
        ],
        compiler_params=pltpu.CompilerParams(collective_id=0, has_side_effects=True, vmem_limit_bytes=67043328),
        name='decoder_step',
    )(lengths, x, freq, attn_gain, mlp_gain, w_q, w_k, w_v, w_o, w_gate, w_up, w_down, k_cache, v_cache)


def solution(mesh):
    col_spec = P(None, None, 'tp')
    row_spec = P(None, 'tp', None)
    cache_spec = P(None, 'dp', 'tp', None, None)
    in_specs = (P('dp', None), P('dp'), P(), col_spec, col_spec, col_spec, row_spec, P(), col_spec, col_spec, row_spec, cache_spec, cache_spec)

    def body(x, lengths, attn_gain, w_q, w_k, w_v, w_o, mlp_gain, w_gate, w_up, w_down, k_cache, v_cache):
        head_dim = k_cache.shape[-1]
        exps = np.arange(0, head_dim, 2, dtype=np.float32) / np.float32(head_dim)
        freq = np.power(np.float32(ROPE_BASE), -exps).astype(np.float32)
        freq = jnp.asarray(np.concatenate([freq, freq])[None])
        return step_call(lengths, x, freq, attn_gain, mlp_gain, w_q, w_k, w_v, w_o, w_gate, w_up, w_down, k_cache, v_cache)

    return jax.shard_map(body, mesh=mesh, in_specs=in_specs, out_specs=P('dp', None), check_vma=False)
```

```python
import functools

import jax
import jax.numpy as jnp
import numpy as np
from jax import lax
from jax.experimental import pallas as pl
from jax.experimental.pallas import tpu as pltpu
from jax.sharding import PartitionSpec as P

ROPE_BASE = 500000.0
EPSILON = 1e-5
MESH = pl.DeviceIdType.MESH
F32 = jnp.float32
BF16 = jnp.bfloat16
CW = 512
G_SLOTS = 5
D_SLOTS = 4
KV_SLOTS = 5
KV_ROWS = 8
ATT_SLOTS = 2
AHEAD_FIRST, AHEAD = 8, 6
STACK = 4
GROUP = 5
O, M = 0, 1
DEC, PRE = 0, 1


def step_kernel(dims, lens, x_in, freq, gain_a, gain_m, wq, wk, wv, wo, wg, wu, wd, kc, vc, y,
                gbuf, dbuf, abuf, acc, act, pbuf, rbuf, xb_o, xb_m, h_o, h_m, ssq, pre, cos, sin, kbuf, vbuf, kpre, vpre,
                qs, kn, vn,
                q_sem, w_sem, g_sem, d_sem, kv_sem, io_sem, p_ss, p_rs, x_ss, x_rs, h_ss, h_rs):
    dec, chunk = dims
    rows = dec + chunk
    width = x_in.shape[1]
    layers, o_depth = wo.shape[0], wo.shape[1]
    ff = wg.shape[2]
    q_cols, k_cols = wq.shape[2], wk.shape[2]
    n_qkv = q_cols + 2 * k_cols
    seq, hd = kc.shape[3], kc.shape[4]
    heads, kv_heads = q_cols // hd, k_cols // hd
    group = heads // kv_heads
    n_chunks = width // CW
    o_per_slot = ff // o_depth
    scale_qk = hd ** -0.5
    base = (0, dec)
    size = (dec, chunk)
    half = (dec // 2, chunk // 2)
    rbase = (0, dec // 2)

    dp_me = lax.axis_index('dp')
    me = lax.axis_index('tp')
    core = lax.rem(me, 2)
    core_peer = (dp_me, me + 1 - 2 * core)
    x_peer = (dp_me, lax.rem(me + 2, 4))

    def own(part):
        return pl.ds(pl.multiple_of(base[part] + core * half[part], 16), half[part])

    def oth(part):
        return pl.ds(pl.multiple_of(base[part] + (1 - core) * half[part], 16), half[part])

    def whole(part):
        return pl.ds(base[part], size[part])

    def landed(part):
        return pl.ds(rbase[part], half[part])

    def cols(j):
        return pl.ds(pl.multiple_of(j * CW, CW), CW)

    att = act.at[:, pl.ds(0, q_cols)]
    kp = act.at[pl.ds(0, chunk), pl.ds(q_cols, k_cols)]
    vp = act.at[pl.ds(0, chunk), pl.ds(q_cols + k_cols, k_cols)]

    def order(l):
        return (PRE, DEC, AHEAD_FIRST) if l == 0 else (DEC, PRE, AHEAD)

    xbs = (xb_o, xb_m)
    hs = (h_o, h_m)

    def x_load(j):
        return pltpu.make_async_copy(x_in.at[:, cols(j)], h_m.at[j], io_sem.at[0])

    def wo_copy(l, j):
        return pltpu.make_async_copy(wo.at[l, :, cols(j)], dbuf.at[j // o_per_slot, pl.ds(pl.multiple_of(lax.rem(j, o_per_slot) * o_depth, 16), o_depth), :], w_sem.at[j])

    def g_copy(l, j, m):
        slot = lax.rem(2 * j + m, G_SLOTS)
        return pltpu.make_async_copy((wg, wu)[m].at[l, cols(j), :], gbuf.at[slot], g_sem.at[slot])

    def d_copy(l, j):
        slot = lax.rem(j, D_SLOTS)
        return pltpu.make_async_copy(wd.at[l, :, cols(j)], dbuf.at[slot], d_sem.at[slot])

    def qkv_place(j):
        return j // 2, (j % 2) * (ff // 2)

    def qkv_copies(l, j):
        slot, left = qkv_place(j)
        dst = gbuf.at[slot]

        def at(off, n):
            return dst.at[:, pl.ds(pl.multiple_of(left + off, 128), n)]

        return (pltpu.make_async_copy(wq.at[l, cols(j), :], at(0, q_cols), q_sem.at[j]),
                pltpu.make_async_copy(wk.at[l, cols(j), :], at(q_cols, k_cols), q_sem.at[j]),
                pltpu.make_async_copy(wv.at[l, cols(j), :], at(q_cols + k_cols, k_cols), q_sem.at[j]))

    def qkv_wait(j):
        slot, left = qkv_place(j)
        dst = gbuf.at[slot, :, pl.ds(pl.multiple_of(left, 128), n_qkv)]
        pltpu.make_async_copy(dst, dst, q_sem.at[j]).wait()

    def kv_copies(l, i):
        slot = lax.rem(i, KV_SLOTS)
        src = pl.ds(i * KV_ROWS, KV_ROWS)
        return (pltpu.make_async_copy(kc.at[l, src], kbuf.at[slot], kv_sem.at[slot, 0]),
                pltpu.make_async_copy(vc.at[l, src], vbuf.at[slot], kv_sem.at[slot, 1]))

    def kv_pre_copies(l):
        return (pltpu.make_async_copy(kc.at[l, dec], kpre, io_sem.at[1]),
                pltpu.make_async_copy(vc.at[l, dec], vpre, io_sem.at[2]))

    def start(copies):
        for c in copies:
            c.start()

    def wait(copies):
        for c in copies:
            c.wait()

    def p_copy(ar, part, j):
        return pltpu.make_async_remote_copy(pbuf.at[j, oth(part), :], rbuf.at[j, landed(part), :], p_ss.at[part, j], p_rs.at[part, j], device_id=core_peer, device_id_type=MESH)

    def x_copy(ar, part, j):
        return pltpu.make_async_remote_copy(pbuf.at[j, own(part), :], xbs[ar].at[j, landed(part), :], x_ss.at[part, j], x_rs.at[ar, part, j], device_id=x_peer, device_id_type=MESH)

    def h_copy(ar, part, j):
        return pltpu.make_async_remote_copy(hs[ar].at[j, own(part), :], hs[ar].at[j, own(part), :], h_ss.at[part, j], h_rs.at[part, j], device_id=core_peer, device_id_type=MESH)

    def h_wait(ar, part, j):
        pltpu.make_async_remote_copy(hs[ar].at[j, oth(part), :], hs[ar].at[j, oth(part), :], h_ss.at[part, j], h_rs.at[part, j], device_id=core_peer, device_id_type=MESH).wait_recv()

    def sent(l, ar, part, j):
        if l > 0 or ar == M:
            p_copy(1 - ar, part, j).wait_send()
            x_copy(1 - ar, part, j).wait_send()

    def pair_sum(ar, part, j):
        p_copy(ar, part, j).wait_recv()
        pbuf[j, own(part), :] = (pbuf[j, own(part), :].astype(F32) + rbuf[j, landed(part), :].astype(F32)).astype(BF16)
        x_copy(ar, part, j).start()

    def finish(l, ar, part, j):
        x_copy(ar, part, j).wait_recv()
        total = pbuf[j, own(part), :].astype(F32) + xbs[ar][j, landed(part), :].astype(F32)
        resid = hs[1 - ar][j, own(part), :].astype(F32)
        if l > 0 or ar == M:
            h_copy(1 - ar, part, j).wait_send()
        hs[ar][j, own(part), :] = (resid + total).astype(BF16)
        h_copy(ar, part, j).start()

    def add_squares(r, vals):
        sq = vals * vals
        ssq[r, :] += sq[:, :128] + sq[:, 128:256] + sq[:, 256:384] + sq[:, 384:]

    def inv_rms(r):
        return lax.rsqrt(jnp.sum(ssq[r, :], axis=-1, keepdims=True) * (1.0 / width) + EPSILON)

    def next_scale(r):
        inv = inv_rms(r)
        scale = inv / pre[r, :1]
        n = ssq[r, :].shape[0]
        pre[r, :] = jnp.broadcast_to(jnp.maximum(inv, 1e-30), (n, 128))
        ssq[r, :] = jnp.zeros((n, 128), F32)
        return scale

    def qkv_block(l, part, pair):
        r = whole(part)
        a = []
        for j in pair:
            if l > 0:
                h_wait(M, part, j)
            vals = h_m[j, r, :].astype(F32)
            add_squares(r, vals)
            a.append((vals * pre[r, :1] * gain_a[l:l + 1, cols(j)].astype(F32)).astype(BF16))
            if part == order(l)[0]:
                qkv_wait(j)
        for n in range(n_qkv // CW):
            total = acc[r, n * CW:(n + 1) * CW]
            for j, a_j in zip(pair, a):
                slot, left = qkv_place(j)
                total += jnp.dot(a_j, gbuf[slot, :, pl.ds(pl.multiple_of(left + n * CW, 128), CW)], preferred_element_type=F32)
            acc[r, n * CW:(n + 1) * CW] = total

    def qkv_begin(part):
        acc[whole(part), :n_qkv] = jnp.zeros((size[part], n_qkv), F32)

    def qkv_lead(l):
        part = order(l)[0]
        qkv_begin(part)
        steps = n_chunks // 2

        def pair(i):
            return 2 * i, 2 * i + 1

        def step(i, c):
            if l > 0:
                for j in pair(i):
                    finish(l - 1, M, part, j)

                @pl.when(i >= 1)
                def _():
                    qkv_block(l, part, pair(i - 1))
            else:
                qkv_block(l, part, pair(i))

                @pl.when(i == 1)
                def _():
                    for j in range(n_chunks):
                        wo_copy(l, j).start()

                @pl.when(i == 3)
                def _():
                    for n in range(KV_SLOTS):
                        start(kv_copies(l, n))
            return c

        lax.fori_loop(0, steps, step, 0)
        if l > 0:
            qkv_block(l, part, pair(steps - 1))
        qkv_end(part)

    def qkv_end(part):
        r = whole(part)
        scale = next_scale(r)
        c_tab, s_tab = cos[r, :], sin[r, :]

        def head(col):
            return (acc[r, col * hd:(col + 1) * hd] * scale).astype(BF16).astype(F32)

        def rope(t):
            return (t * c_tab + pltpu.roll(t, hd // 2, 1) * s_tab).astype(BF16)

        for h in range(heads):
            q = rope(head(h))
            if part == DEC:
                qs[pl.ds(h, dec, stride=heads), :] = q.astype(F32)
            else:
                att[dec:, h * hd:(h + 1) * hd] = q
        for g in range(kv_heads):
            k = rope(head(heads + g))
            v = head(heads + kv_heads + g)
            if part == DEC:
                for h in range(g * group, (g + 1) * group):
                    kn[pl.ds(h, dec, stride=heads), :] = k.astype(F32)
                    vn[pl.ds(h, dec, stride=heads), :] = v
            else:
                kp[:, g * hd:(g + 1) * hd] = k
                vp[:, g * hd:(g + 1) * hd] = v.astype(BF16)

    def decode_attention(l):
        first_rows = lax.broadcasted_iota(jnp.int32, (heads, hd), 0) < group
        places = lax.broadcasted_iota(jnp.int32, (heads, seq), 1)
        n_slots = dec // KV_ROWS
        step_rows = ATT_SLOTS * KV_ROWS

        def block(i, c):
            slots = []
            for t in range(ATT_SLOTS):
                wait(kv_copies(l, ATT_SLOTS * i + t))
                slots.append(lax.rem(ATT_SLOTS * i + t, KV_SLOTS))
            scores = []
            for n in range(step_rows):
                b = i * step_rows + n
                slot, m = slots[n // KV_ROWS], n % KV_ROWS
                q = qs[pl.ds(pl.multiple_of(b * heads, heads), heads), :]
                zero = jnp.zeros_like(q)
                q2 = jnp.concatenate([jnp.where(first_rows, q, zero), jnp.where(first_rows, zero, q)], axis=1).astype(BF16)
                k2 = jnp.concatenate([kbuf[slot, m, 0], kbuf[slot, m, 1]], axis=1)
                s = lax.dot_general(q2, k2, (((1,), (1,)), ((), ())), preferred_element_type=F32) * scale_qk
                scores.append(jnp.where(places < lens[b], s, -jnp.inf))
            r = pl.ds(pl.multiple_of(i * step_rows * heads, step_rows * heads), step_rows * heads)
            s = jnp.concatenate(scores, axis=0)
            s_new = jnp.sum(qs[r, :] * kn[r, :], axis=-1, keepdims=True) * scale_qk
            top = jnp.maximum(jnp.max(s, axis=-1, keepdims=True), s_new)
            e = jnp.exp(s - top)
            e_new = jnp.exp(s_new - top)
            inv = 1.0 / (jnp.sum(e, axis=-1, keepdims=True) + e_new)
            p = (e * inv).astype(BF16)
            p_new = (e_new * inv).astype(BF16).astype(F32)
            outs = []
            for n in range(step_rows):
                slot, m = slots[n // KV_ROWS], n % KV_ROWS
                v2 = jnp.concatenate([vbuf[slot, m, 0], vbuf[slot, m, 1]], axis=1)
                o = jnp.dot(p[n * heads:(n + 1) * heads], v2, preferred_element_type=F32)
                outs.append(jnp.where(first_rows, o[:, :hd], o[:, hd:]))
            qs[r, :] = jnp.concatenate(outs, axis=0) + p_new * vn[r, :]

            for t in range(ATT_SLOTS):
                nxt = ATT_SLOTS * i + t + KV_SLOTS

                @pl.when(nxt < n_slots)
                def _():
                    start(kv_copies(l, nxt))
            return c

        lax.fori_loop(0, n_slots // ATT_SLOTS, block, 0)
        for h in range(heads):
            att[:dec, h * hd:(h + 1) * hd] = qs[pl.ds(h, dec, stride=heads), :].astype(BF16)

    def prefill_attention(l):
        wait(kv_pre_copies(l))
        old = jnp.where(lax.broadcasted_iota(jnp.int32, (1, seq), 1) < lens[dec], 0.0, -jnp.inf)
        causal = jnp.where(lax.broadcasted_iota(jnp.int32, (chunk, chunk), 1) <= lax.broadcasted_iota(jnp.int32, (chunk, chunk), 0), 0.0, -jnp.inf)
        causal = jnp.concatenate([causal] * STACK, axis=0)
        for first in range(0, heads, STACK):
            g = first // group
            cut = [slice((first + i) * hd, (first + i + 1) * hd) for i in range(STACK)]
            q = jnp.concatenate([att[dec:, c] for c in cut], axis=0)
            kv_col = slice(g * hd, (g + 1) * hd)
            s = lax.dot_general(q, kpre[g], (((1,), (1,)), ((), ())), preferred_element_type=F32) * scale_qk + old
            t = lax.dot_general(q, kp[:, kv_col], (((1,), (1,)), ((), ())), preferred_element_type=F32) * scale_qk + causal
            top = jnp.maximum(jnp.max(s, axis=-1, keepdims=True), jnp.max(t, axis=-1, keepdims=True))
            es = jnp.exp(s - top)
            et = jnp.exp(t - top)
            inv = 1.0 / (jnp.sum(es, axis=-1, keepdims=True) + jnp.sum(et, axis=-1, keepdims=True))
            o = jnp.dot((es * inv).astype(BF16), vpre[g], preferred_element_type=F32)
            o += jnp.dot((et * inv).astype(BF16), vp[:, kv_col], preferred_element_type=F32)
            for i in range(STACK):
                att[dec:, cut[i]] = o[i * chunk:(i + 1) * chunk].astype(BF16)

    def o_part(l, part):
        r = whole(part)

        def step(i, c):
            these = tuple(GROUP * i + t for t in range(GROUP))
            for j in these:
                if part == order(l)[0]:
                    wo_copy(l, j).wait()
                sent(l, O, part, j)
            for j in these:
                w = dbuf[j // o_per_slot, pl.ds(pl.multiple_of(lax.rem(j, o_per_slot) * o_depth, 16), o_depth), :]
                pbuf[j, r, :] = jnp.dot(att[r, :], w, preferred_element_type=F32).astype(BF16)
            for j in these:
                p_copy(O, part, j).start()

            @pl.when(i >= 1)
            def _():
                for j in these:
                    pair_sum(O, part, j - GROUP)
            return c

        lax.fori_loop(0, n_chunks // GROUP, step, 0)

    def gate_up(l):
        lead, trail, ahead = order(l)

        def operand(r, j):
            vals = h_o[j, r, :].astype(F32)
            add_squares(r, vals)
            return (vals * pre[r, :1] * gain_m[l:l + 1, cols(j)].astype(F32)).astype(BF16)

        def release(j, m):
            nxt = j + (G_SLOTS + m) // 2

            @pl.when(nxt < n_chunks)
            def _():
                g_copy(l, nxt, (G_SLOTS + m) % 2).start()

        def make_ahead(j):
            abuf[j % 2] = operand(pl.ds(0, rows), j)

        def first_block(part):
            r = whole(part)
            a = operand(r, 0)
            for m in range(2):
                if part == lead:
                    g_copy(l, 0, m).wait()
                elif m == 1:
                    h_wait(O, DEC, 1)
                    h_wait(O, PRE, 1)
                    make_ahead(1)
                for n in range(ff // CW):
                    acc[r, m * ff + n * CW:m * ff + (n + 1) * CW] = jnp.dot(a, gbuf[m, :, n * CW:(n + 1) * CW], preferred_element_type=F32)
                if part == trail:
                    g_copy(l, (G_SLOTS + m) // 2, (G_SLOTS + m) % 2).start()

        def block(j, more):
            for m in range(2):
                g_copy(l, j, m).wait()
                slot = lax.rem(2 * j + m, G_SLOTS)
                if m == 1 and more:
                    h_wait(O, DEC, j + 1)
                    h_wait(O, PRE, j + 1)
                    make_ahead(j + 1)
                a = abuf[j % 2]
                for n in range(ff // CW):
                    acc[:, m * ff + n * CW:m * ff + (n + 1) * CW] += jnp.dot(a, gbuf[slot, :, n * CW:(n + 1) * CW], preferred_element_type=F32)
                if more:
                    release(j, m)

            @pl.when(j >= n_chunks - D_SLOTS)
            def _():
                d_copy(l, j - (n_chunks - D_SLOTS)).start()

        def lead_step(j, c):
            finish(l, O, lead, j)
            return c

        lax.fori_loop(0, GROUP, lead_step, 0)
        for j in range(GROUP, n_chunks):
            if j >= ahead:
                pair_sum(O, lead, j)
            pair_sum(O, trail, j)
        lax.fori_loop(GROUP, ahead, lead_step, 0)
        finish(l, O, trail, 0)
        h_wait(O, lead, 0)
        first_block(lead)
        finish(l, O, trail, 1)
        h_wait(O, trail, 0)
        first_block(trail)

        def step(j, c):
            @pl.when(j + 1 >= ahead)
            def _():
                finish(l, O, lead, j + 1)

            finish(l, O, trail, j + 1)
            block(j, True)
            return c

        lax.fori_loop(1, n_chunks - 1, step, 0)
        block(n_chunks - 1, False)
        scale = next_scale(pl.ds(0, rows))

        def act_step(n, c):
            gate = acc[:, cols(n)] * scale
            up = acc[:, pl.ds(pl.multiple_of(ff + n * CW, CW), CW)] * scale
            act[:, cols(n)] = (gate * jax.nn.sigmoid(gate) * up).astype(BF16)
            return c

        lax.fori_loop(0, ff // CW, act_step, 0)

    def down(l):
        def step(j, c):
            d_copy(l, j).wait()
            for part in (DEC, PRE):
                sent(l, M, part, j)
            pbuf[j] = jnp.dot(act[...], dbuf[lax.rem(j, D_SLOTS)], preferred_element_type=F32).astype(BF16)
            for part in (DEC, PRE):
                p_copy(M, part, j).start()

            @pl.when(j + D_SLOTS < n_chunks)
            def _():
                d_copy(l, j + D_SLOTS).start()

            if l + 1 < layers:
                for n in range(3):
                    nxt = 3 * (j - (n_chunks - D_SLOTS)) + n

                    @pl.when((nxt >= 0) & (nxt < n_chunks))
                    def _():
                        start(qkv_copies(l + 1, nxt))

            @pl.when(j >= 1)
            def _():
                pair_sum(M, DEC, j - 1)
            return c

        lax.fori_loop(0, n_chunks, step, 0)
        pair_sum(M, DEC, n_chunks - 1)
        if l + 1 < layers:
            start(kv_pre_copies(l + 1))
            for i in range(KV_SLOTS):
                start(kv_copies(l + 1, i))
            for j in range(n_chunks):
                wo_copy(l + 1, j).start()

        def pre_step(j, c):
            pair_sum(M, PRE, j)
            return c

        lax.fori_loop(0, n_chunks, pre_step, 0)

    for j in range(n_chunks):
        x_load(j).start()
    barrier = pltpu.get_barrier_semaphore()
    for peer in (core_peer, x_peer):
        pl.semaphore_signal(barrier, inc=1, device_id=peer, device_id_type=MESH)
    for j in range(n_chunks):
        start(qkv_copies(0, j))
    start(kv_pre_copies(0))
    ssq[...] = jnp.zeros_like(ssq)

    def place(b, c):
        cos[pl.ds(b, 1), :] = jnp.full((1, hd), lens[b], jnp.int32).astype(F32)
        return c

    lax.fori_loop(0, dec, place, 0, unroll=8)
    cos[pl.ds(dec, chunk), :] = (lax.broadcasted_iota(jnp.int32, (chunk, hd), 0) + lens[dec]).astype(F32)
    angles = cos[...] * freq[...]
    low = lax.broadcasted_iota(jnp.int32, (rows, hd), 1) < hd // 2
    sines = jnp.sin(angles)
    sin[...] = jnp.where(low, -sines, sines)
    cos[...] = jnp.cos(angles)
    pltpu.make_async_copy(h_m, h_m, io_sem.at[0]).wait()

    def sq_step(j, c):
        add_squares(pl.ds(0, rows), h_m[j].astype(F32))
        return c

    lax.fori_loop(0, n_chunks, sq_step, 0)
    pre[...] = jnp.broadcast_to(jnp.maximum(inv_rms(pl.ds(0, rows)), 1e-30), pre.shape)
    ssq[...] = jnp.zeros_like(ssq)

    def finish_pre(l, first, stop):
        if l > 0:
            def pre_step(j, c):
                finish(l - 1, M, PRE, j)
                return c

            lax.fori_loop(first, stop, pre_step, 0)

    for l in range(layers):
        lead, trail, ahead = order(l)
        attend = (decode_attention, prefill_attention)
        qkv_lead(l)
        attend[lead](l)
        if l == 0:
            pl.semaphore_wait(barrier, 2)
        finish_pre(l, 0, 5)
        o_part(l, lead)
        finish_pre(l, 5, 8)
        qkv_begin(trail)
        qkv_block(l, trail, tuple(range(5)))
        for j in range(GROUP, ahead):
            pair_sum(O, lead, j)
        finish_pre(l, 8, 10)
        qkv_block(l, trail, (5, 6, 7))
        qkv_block(l, trail, (8, 9))
        qkv_end(trail)
        if trail == PRE:
            for i in range(G_SLOTS):
                g_copy(l, i // 2, i % 2).start()
        attend[trail](l)
        if trail == DEC:
            for i in range(G_SLOTS):
                g_copy(l, i // 2, i % 2).start()
        o_part(l, trail)
        gate_up(l)
        down(l)

    def out_copy(part, j):
        r = whole(part)
        return pltpu.make_async_copy(h_m.at[j, r, :], y.at[r, cols(j)], io_sem.at[3 + part])

    def out_dec(j, c):
        finish(layers - 1, M, DEC, j)

        @pl.when(j >= 1)
        def _():
            h_wait(M, DEC, j - 1)
            out_copy(DEC, j - 1).start()

        p_copy(M, DEC, j).wait_send()
        p_copy(M, PRE, j).wait_send()
        return c

    lax.fori_loop(0, n_chunks, out_dec, 0)
    h_wait(M, DEC, n_chunks - 1)
    out_copy(DEC, n_chunks - 1).start()

    def out_pre(j, c):
        finish(layers - 1, M, PRE, j)
        x_copy(M, DEC, j).wait_send()
        h_copy(M, DEC, j).wait_send()

        @pl.when(j >= 1)
        def _():
            h_wait(M, PRE, j - 1)
            out_copy(PRE, j - 1).start()
            x_copy(M, PRE, j - 1).wait_send()

        @pl.when(j >= 2)
        def _():
            h_copy(M, PRE, j - 2).wait_send()
        return c

    lax.fori_loop(0, n_chunks, out_pre, 0)
    last = n_chunks - 1
    h_wait(M, PRE, last)
    out_copy(PRE, last).start()
    x_copy(M, PRE, last).wait_send()
    for j in (last - 1, last):
        h_copy(M, PRE, j).wait_send()
    for part in (DEC, PRE):
        done = h_m.at[:, whole(part), :]
        pltpu.make_async_copy(done, done, io_sem.at[3 + part]).wait()


def step_call(lengths, x, freq, attn_gain, mlp_gain, w_q, w_k, w_v, w_o, w_gate, w_up, w_down, k_cache, v_cache):
    rows, width = x.shape
    dec = lengths.shape[0] - 1
    chunk = rows - dec
    ff = w_gate.shape[2]
    n_chunks = width // CW
    q_cols, k_cols = w_q.shape[2], w_k.shape[2]
    kv_heads, seq, hd = k_cache.shape[2:]
    heads = q_cols // hd
    vmem = pl.BlockSpec(memory_space=pltpu.VMEM)
    hbm = pl.BlockSpec(memory_space=pl.ANY)
    smem = pl.BlockSpec(memory_space=pltpu.SMEM)
    sem = pltpu.SemaphoreType.DMA
    buf = pltpu.VMEM
    return pl.pallas_call(
        functools.partial(step_kernel, (dec, chunk)),
        out_shape=jax.ShapeDtypeStruct((rows, width), BF16),
        in_specs=[smem, hbm, vmem, vmem, vmem] + [hbm] * 9,
        out_specs=hbm,
        scratch_shapes=[
            buf((G_SLOTS, CW, ff), BF16),
            buf((D_SLOTS, ff, CW), BF16),
            buf((2, rows, CW), BF16),
            buf((rows, 2 * ff), F32),
            buf((rows, ff), BF16),
            buf((n_chunks, rows, CW), BF16),
            buf((n_chunks, rows // 2, CW), BF16),
            buf((n_chunks, rows // 2, CW), BF16),
            buf((n_chunks, rows // 2, CW), BF16),
            buf((n_chunks, rows, CW), BF16),
            buf((n_chunks, rows, CW), BF16),
            buf((rows, 128), F32),
            buf((rows, 128), F32),
            buf((rows, hd), F32),
            buf((rows, hd), F32),
            buf((KV_SLOTS, KV_ROWS, kv_heads, seq, hd), BF16),
            buf((KV_SLOTS, KV_ROWS, kv_heads, seq, hd), BF16),
            buf((kv_heads, seq, hd), BF16),
            buf((kv_heads, seq, hd), BF16),
            buf((dec * heads, hd), F32),
            buf((dec * heads, hd), F32),
            buf((dec * heads, hd), F32),
            sem((n_chunks,)),
            sem((n_chunks,)),
            sem((G_SLOTS,)),
            sem((D_SLOTS,)),
            sem((KV_SLOTS, 2)),
            sem((5,)),
            sem((2, n_chunks)),
            sem((2, n_chunks)),
            sem((2, n_chunks)),
            sem((2, 2, n_chunks)),
            sem((2, n_chunks)),
            sem((2, n_chunks)),
        ],
        compiler_params=pltpu.CompilerParams(collective_id=0, has_side_effects=True, vmem_limit_bytes=67043328),
        name='decoder_step',
    )(lengths, x, freq, attn_gain, mlp_gain, w_q, w_k, w_v, w_o, w_gate, w_up, w_down, k_cache, v_cache)


def solution(mesh):
    col_spec = P(None, None, 'tp')
    row_spec = P(None, 'tp', None)
    cache_spec = P(None, 'dp', 'tp', None, None)
    in_specs = (P('dp', None), P('dp'), P(), col_spec, col_spec, col_spec, row_spec, P(), col_spec, col_spec, row_spec, cache_spec, cache_spec)

    def body(x, lengths, attn_gain, w_q, w_k, w_v, w_o, mlp_gain, w_gate, w_up, w_down, k_cache, v_cache):
        head_dim = k_cache.shape[-1]
        exps = np.arange(0, head_dim, 2, dtype=np.float32) / np.float32(head_dim)
        freq = np.power(np.float32(ROPE_BASE), -exps).astype(np.float32)
        freq = jnp.asarray(np.concatenate([freq, freq])[None])
        return step_call(lengths, x, freq, attn_gain, mlp_gain, w_q, w_k, w_v, w_o, w_gate, w_up, w_down, k_cache, v_cache)

    return jax.shard_map(body, mesh=mesh, in_specs=in_specs, out_specs=P('dp', None), check_vma=False)
```
